128 devices in a mesh: shard: 8 (over z, x_hi), context: 2 (over x_lo), tensor: 8 (over y, core).
Axes of the slice: x: 4 (x_hi: 2, x_lo: 2; x = x_hi * 2 + x_lo), y: 4, z: 4, core: 2. Of those that a mesh axis runs over, the one named last changes fastest.
Arguments:
- block_in: bfloat16 [8, 1024, 1024], P('shard', 'context'), may hold values from -6 to 6
- qkv_weight: bfloat16 [2, 1024, 3072], P(None, ('shard', 'context'), 'tensor'), may hold values from -0.1875 to 0.1875
- proj_weight: bfloat16 [2, 1024, 1024], P(None, ('shard', 'context'), 'tensor'), may hold values from -0.375 to 0.375
- fc1_weight: bfloat16 [2, 1024, 4096], P(None, ('shard', 'context'), 'tensor'), may hold values from -0.1875 to 0.1875
- fc2_weight: bfloat16 [2, 1024, 4096], P(None, ('shard', 'context'), 'tensor'), may hold values from -0.09375 to 0.09375
- qv_bias: bfloat16 [2, 2048], P(None, 'tensor'), may hold values from -3 to 3
- fc1_bias: bfloat16 [2, 4096], P(None, 'tensor'), may hold values from -3 to 3
- norm_gains: bfloat16 [2, 2, 1024], P(None, None, ('shard', 'context')), may hold values from 0.5 to 1.5
- row_biases: bfloat16 [2, 4, 1024], P(None, None, ('shard', 'context')), may hold values from -3 to 3
- cotangent: bfloat16 [8, 1024, 1024], P('shard', 'context'), may hold values from -6 to 6
Outputs:
- block_out: bfloat16 [8, 1024, 1024], P('shard', 'context')
- input_grad: float32 [8, 1024, 1024], P('shard', 'context')
- qkv_grad: float32 [2, 1024, 3072], P(None, ('shard', 'context'), 'tensor')
- proj_grad: float32 [2, 1024, 1024], P(None, ('shard', 'context'), 'tensor')
- fc1_grad: float32 [2, 1024, 4096], P(None, ('shard', 'context'), 'tensor')
- fc2_grad: float32 [2, 1024, 4096], P(None, ('shard', 'context'), 'tensor')
- qv_bias_grad: float32 [2, 2048], P(None, 'tensor')
- fc1_bias_grad: float32 [2, 4096], P(None, 'tensor')
- gains_grad: float32 [2, 2, 1024], P(None, None, ('shard', 'context'))
- biases_grad: float32 [2, 4, 1024], P(None, None, ('shard', 'context'))
The draws below stay inside these ranges and needn't reach their ends.
All inputs are finite; a program needn't handle non-finite values.
Results may differ from the reference program's by a relative error of at most 0.025.
Values may be sent and summed in bfloat16 or wider, within the bound.
No kernel may reach another device: no remote copies, remote signals or barrier semaphores. Data moves between devices by JAX's collectives and lax.ppermute only.
A program may use at most 128 MiB of HBM per device.

```python
import jax
import jax.numpy as jnp
from jax import lax

D = 1024
HEADS = 16
HD = 64
FF = 4096
LAYERS = 2
LEN = 1024
SEQS = 8
N_TENSOR = 8


def block_scale(rng, extent, shards, least, high):
    factor_of, own = 1.0, jax.random.fold_in(rng, 6)
    for position, blocks in shards:
        steps = jnp.exp(jax.random.uniform(jax.random.fold_in(own, position), (blocks,), jnp.float32, least / len(shards), high / len(shards)))
        factor_of = factor_of * jnp.repeat(steps, extent[position] // blocks).reshape([-1 if axis == position else 1 for axis in range(len(extent))])
    return factor_of


def scatter_about(stream_key, shape, deviation, reach, shards=(), dtype=jnp.bfloat16):
    loudness = block_scale(stream_key, shape, shards, -0.22, 0.18) if shards else 1.0
    values = jax.random.normal(stream_key, shape, jnp.float32) * deviation * loudness
    return jnp.minimum(jnp.maximum(values, -reach), reach).astype(dtype)


def setup_inputs(seed: int = 0) -> dict:
    keys = jax.random.split(jax.random.key(seed), 11)
    return {
        "block_in": scatter_about(keys[0], (SEQS, LEN, D), 1.0, 6.0, ((0, 8), (1, 2))),
        "qkv_weight": scatter_about(keys[1], (LAYERS, D, 3 * D), D ** -0.5, 0.1875, ((1, 16), (2, 8))),
        "proj_weight": scatter_about(keys[2], (LAYERS, D, D), (D // 4) ** -0.5, 0.375, ((1, 16), (2, 8))),
        "fc1_weight": scatter_about(keys[3], (LAYERS, D, FF), D ** -0.5, 0.1875, ((1, 16), (2, 8))),
        "fc2_weight": scatter_about(keys[4], (LAYERS, D, FF), FF ** -0.5, 0.09375, ((1, 16), (2, 8))),
        "qv_bias": scatter_about(keys[5], (LAYERS, 2 * D), 0.5, 3.0, ((1, 8),)),
        "fc1_bias": scatter_about(keys[6], (LAYERS, FF), 0.5, 3.0, ((1, 8),)),
        "norm_gains": jnp.clip(1.0 + 0.1 * jax.random.normal(keys[7], (LAYERS, 2, D), jnp.float32), 0.5, 1.5).astype(jnp.bfloat16),
        "row_biases": scatter_about(keys[8], (LAYERS, 4, D), 0.5, 3.0, ((2, 16),)),
        "cotangent": scatter_about(keys[9], (SEQS, LEN, D), 1.0, 6.0, ((0, 8), (1, 2))),
    }


NORM_EPS = 1e-05
GELU_SCALE = 0.7978845608028654
EXACT = lax.Precision.HIGHEST

@jax.custom_vjp
def low(v):
    return lax.optimization_barrier(v.astype(jnp.bfloat16)).astype(jnp.float32)

@jax.custom_vjp
def low_back(v):
    return v

def low_keep(v):
    return (low(v), None)

def low_pass(kept, grad):
    return (grad,)

def back_keep(v):
    return (v, None)

def back_low(kept, grad):
    return (low(grad),)
low.defvjp(low_keep, low_pass)
low_back.defvjp(back_keep, back_low)

def norm_rows(source, scales, shifts):
    average = lax.optimization_barrier(jnp.mean(source, axis=-1, keepdims=True))
    centred = source - average
    variance = lax.optimization_barrier(jnp.mean(centred * centred, axis=-1, keepdims=True))
    return centred * lax.rsqrt(variance + NORM_EPS) * scales + shifts

def gelu_tanh(source):
    return 0.5 * source * (1.0 + jnp.tanh(GELU_SCALE * (source + 0.044715 * source * source * source)))

def head_slopes():
    head_rank = jnp.arange(1, HEADS + 1).astype(jnp.float32)
    return jnp.exp2(-8.0 * head_rank / HEADS)

def attend_sequence(operands):
    queries, keys_all, values_all = operands
    raw_scores = jnp.einsum('ihd,jhd->hij', queries, keys_all, precision=EXACT)
    raw_scores = low_back(raw_scores * HD ** (-0.5))
    places = jnp.arange(LEN)
    distance = (places[:, None] - places[None, :]).astype(jnp.float32)
    scores = raw_scores - head_slopes()[:, None, None] * distance[None]
    scores = jnp.where(distance[None] >= 0.0, scores, -1e+30)
    highest = lax.optimization_barrier(jnp.max(scores, axis=-1, keepdims=True))
    weights = jnp.exp(scores - highest)
    prob_rows = low(weights / lax.optimization_barrier(jnp.sum(weights, axis=-1, keepdims=True)))
    return jnp.einsum('hij,jhd->ihd', prob_rows, values_all, precision=EXACT)

def grouped_product(left_side, right_side):
    row_count = left_side.shape[0]
    group_width = left_side.shape[1] // N_TENSOR
    left_parts = left_side.reshape(row_count, N_TENSOR, group_width)
    right_parts = right_side.reshape(right_side.shape[0], N_TENSOR, group_width)
    partial_value = jnp.einsum('rgk,dgk->grd', left_parts, right_parts, precision=EXACT)
    return lax.optimization_barrier(jnp.sum(low(low_back(partial_value)), axis=0))

def one_layer(stream, qkv_matrix, proj_matrix, up_matrix, down_matrix, qv_shift, up_shift, norm_scales, row_shifts):
    seq_count = stream.shape[0]
    flat_rows = stream.reshape(seq_count * LEN, D)
    normed = low(norm_rows(flat_rows, norm_scales[0], row_shifts[0]))
    projected = jnp.dot(normed, qkv_matrix, precision=EXACT, preferred_element_type=jnp.float32)
    projected = projected.reshape(seq_count, LEN, HEADS, 3, HD)
    shift_parts = qv_shift.reshape(HEADS, 2, HD)
    queries = low(low_back(projected[:, :, :, 0] + shift_parts[:, 0]))
    keys_all = low(low_back(projected[:, :, :, 1]))
    values_all = low(low_back(projected[:, :, :, 2] + shift_parts[:, 1]))
    attended = lax.map(jax.checkpoint(attend_sequence), (queries, keys_all, values_all))
    attended = low(low_back(attended)).reshape(seq_count * LEN, D)
    middle = flat_rows + grouped_product(attended, proj_matrix) + row_shifts[1]
    normed_two = low(norm_rows(middle, norm_scales[1], row_shifts[2]))
    hidden = low_back(jnp.dot(normed_two, up_matrix, precision=EXACT, preferred_element_type=jnp.float32) + up_shift)
    active = low(gelu_tanh(hidden))
    result = middle + grouped_product(active, down_matrix) + row_shifts[3]
    return result.reshape(stream.shape)

def reference(block_in, qkv_weight, proj_weight, fc1_weight, fc2_weight, qv_bias, fc1_bias, norm_gains, row_biases, cotangent):

    def forward(stream, qkv_all, proj_all, up_all, down_all, qv_all, up_shift_all, gains_all, shifts_all):
        for layer_index in range(LAYERS):
            stream = one_layer(stream, qkv_all[layer_index], proj_all[layer_index], up_all[layer_index], down_all[layer_index], qv_all[layer_index], up_shift_all[layer_index], gains_all[layer_index], shifts_all[layer_index])
        return stream
    result, pullback = jax.vjp(forward, block_in.astype(jnp.float32), qkv_weight.astype(jnp.float32), proj_weight.astype(jnp.float32), fc1_weight.astype(jnp.float32), fc2_weight.astype(jnp.float32), qv_bias.astype(jnp.float32), fc1_bias.astype(jnp.float32), norm_gains.astype(jnp.float32), row_biases.astype(jnp.float32))
    gradients = pullback(cotangent.astype(jnp.float32))
    return (result.astype(jnp.bfloat16), gradients[0], gradients[1], gradients[2], gradients[3], gradients[4], gradients[5], gradients[6], gradients[7], gradients[8])
```

```python
import jax
import jax.numpy as jnp
from jax import lax
from jax.experimental import pallas as pl
from jax.experimental.pallas import tpu as pltpu
from jax.sharding import PartitionSpec as P

HEADS = 16
HD = 64
NORM_EPS = 1e-05
GELU_SCALE = 0.7978845608028654
GELU_CUBE = 0.044715
F32 = jnp.float32
BF = jnp.bfloat16
W = ("shard", "context")
T = "tensor"
ROWS = 512
HALF = 256
PIECE = 64
D = 1024
NEG = -1e30


def spec(shape, index=None):
    place = tuple(index) if index is not None else (0,) * len(shape)
    return pl.BlockSpec(shape, lambda i: place)


def smem():
    return pl.BlockSpec(memory_space=pltpu.SMEM)


def call(body, name, operands, outs):
    in_specs, args = [], []
    for array, shape, index in operands:
        in_specs.append(smem() if shape is None else spec(shape, index))
        args.append(array)
    return pl.pallas_call(
        body,
        grid=(1,),
        in_specs=in_specs,
        out_specs=[spec(o.shape) for o in outs],
        out_shape=outs,
        compiler_params=pltpu.CompilerParams(vmem_limit_bytes=50 << 20),
        name=name,
    )(*args)


def sds(shape, dtype):
    return jax.ShapeDtypeStruct(shape, dtype)


def mm(a, b):
    return lax.dot_general(a, b, (((1,), (0,)), ((), ())), preferred_element_type=F32)


def mm_nt(a, b):
    return lax.dot_general(a, b, (((1,), (1,)), ((), ())), preferred_element_type=F32)


def mm_tn(a, b):
    return lax.dot_general(a, b, (((0,), (0,)), ((), ())), preferred_element_type=F32)


def core_swap(v):
    return lax.ppermute(v, T, [(i, i ^ 1) for i in range(8)])


def along_y(v, step):
    return lax.ppermute(
        v, T, [(2 * y + c, 2 * ((y + step) % 4) + c) for y in range(4) for c in range(2)]
    )


def add_body(pa, got, h0, h1, h2, h3):
    both = pa[...].astype(F32) + got[...].astype(F32)
    h0[...] = both[:PIECE]
    h1[...] = both[PIECE : 2 * PIECE].astype(BF)
    h2[...] = both[2 * PIECE : 3 * PIECE].astype(BF)
    h3[...] = both[3 * PIECE :].astype(BF)


def sum_pieces(keep, send):
    got = core_swap(send)
    h0, h1, h2, h3 = call(
        add_body,
        "pair_add",
        [(keep, (HALF, D), None), (got, (HALF, D), None)],
        [sds((PIECE, D), F32)] + [sds((PIECE, D), BF)] * 3,
    )
    r2 = along_y(h2, -2)
    r1 = along_y(h1, -1)
    r3 = along_y(h3, -3)
    return h0, r1, r2, r3


def gather_rows(own):
    r2 = along_y(own, 2)
    r1 = along_y(own, 1)
    r3 = along_y(own, 3)
    near = jnp.concatenate([own, r1, r2, r3], axis=0)
    far = core_swap(near)
    return near, far


def norm_parts(v):
    mean = jnp.mean(v, axis=-1, keepdims=True)
    centred = v - mean
    var = jnp.mean(centred * centred, axis=-1, keepdims=True)
    s = lax.rsqrt(var + NORM_EPS)
    return centred * s, s


def norm_fwd_body(h0, r1, r2, r3, resid, rows, stream, normed):
    v = (
        h0[...] + r1[...].astype(F32) + r2[...].astype(F32) + r3[...].astype(F32)
    ) + resid[...].astype(F32) + rows[0:1]
    stream[...] = v
    xhat, _ = norm_parts(v)
    normed[...] = (xhat * rows[1:2] + rows[2:3]).astype(BF)


def norm_fwd(pieces, resid, bias, gain, shift):
    h0, r1, r2, r3 = pieces
    rows = jnp.stack([bias, gain, shift])
    b = (PIECE, D)
    return call(
        norm_fwd_body,
        "norm_fwd",
        [(h0, b, None), (r1, b, None), (r2, b, None), (r3, b, None), (resid, b, None), (rows, (3, D), None)],
        [sds(b, F32), sds(b, BF)],
    )


def norm_bwd_body(h0, r1, r2, r3, stream, grad, gain, out, low, sums):
    g = h0[...] + r1[...].astype(F32) + r2[...].astype(F32) + r3[...].astype(F32)
    xhat, s = norm_parts(stream[...].astype(F32))
    gx = g * xhat
    c = g * gain[...]
    cx = c * xhat
    e = grad[...].astype(F32) + s * (
        c
        - jnp.mean(c, axis=-1, keepdims=True)
        - xhat * jnp.mean(cx, axis=-1, keepdims=True)
    )
    out[...] = e
    low[...] = e.astype(BF)
    sums[0:1] = jnp.sum(gx, axis=0, keepdims=True)
    sums[1:2] = jnp.sum(g, axis=0, keepdims=True)
    sums[2:3] = jnp.sum(e, axis=0, keepdims=True)


def norm_bwd(pieces, stream, grad, gain):
    h0, r1, r2, r3 = pieces
    b = (PIECE, D)
    return call(
        norm_bwd_body,
        "norm_bwd",
        [(h0, b, None), (r1, b, None), (r2, b, None), (r3, b, None), (stream, b, None), (grad, b, None), (gain[None], (1, D), None)],
        [sds(b, F32), sds(b, BF), sds((3, D), F32)],
    )


def qkv_first_body(xa, xb, w, rows, bias, na, nb, q, kv):
    for x, n, at in ((xa, na, 0), (xb, nb, HALF)):
        xhat, _ = norm_parts(x[...].astype(F32))
        normed = (xhat * rows[0:1] + rows[1:2]).astype(BF)
        n[...] = normed
        joined = mm(normed, w[...]) + bias[...]
        q[at : at + HALF] = joined[:, :128].astype(BF)
        kv[at : at + HALF] = joined[:, 128:].astype(BF)


def qkv_body(na, nb, w, bias, q, kv):
    for n, at in ((na, 0), (nb, HALF)):
        joined = mm(n[...], w[...]) + bias[...]
        q[at : at + HALF] = joined[:, :128].astype(BF)
        kv[at : at + HALF] = joined[:, 128:].astype(BF)


def places(place, shape, axis):
    r = lax.broadcasted_iota(jnp.int32, shape, axis)
    y, c = place[0], place[1]
    return (
        ((c + (r >> 8)) & 1) * 256 + ((y - ((r >> 6) & 3)) & 3) * 64 + (r & 63)
    )


def key_terms(place, slope):
    pos = places(place, (1, ROWS), 1).astype(F32)
    off = jnp.where(place[2] == 1, 0.0, NEG)
    own = [slope[h] * pos for h in range(2)]
    earlier = [slope[h] * (pos - 512.0) + off for h in range(2)]
    return own, earlier


def attend_body(place, slope, q, kv, kvo, pw, att, lse, pa, pb):
    mask = places(place, (ROWS, 1), 0) >= places(place, (1, ROWS), 1)
    own, earlier = key_terms(place, slope)
    outs, logs = [], []
    for h in range(2):
        lo, hi = h * HD, (h + 1) * HD
        qh = q[:, lo:hi]
        s1 = mm_nt(qh, kv[:, lo:hi]) * 0.125 + own[h]
        s1 = jnp.where(mask, s1, NEG)
        s2 = mm_nt(qh, kvo[:, lo:hi]) * 0.125 + earlier[h]
        top = jnp.maximum(
            jnp.max(s1, axis=-1, keepdims=True), jnp.max(s2, axis=-1, keepdims=True)
        )
        p1 = jnp.exp(s1 - top)
        p2 = jnp.exp(s2 - top)
        total = jnp.sum(p1, axis=-1, keepdims=True) + jnp.sum(p2, axis=-1, keepdims=True)
        o = mm(p1.astype(BF), kv[:, 128 + lo : 128 + hi]) + mm(
            p2.astype(BF), kvo[:, 128 + lo : 128 + hi]
        )
        outs.append(o / total)
        logs.append(jnp.broadcast_to(top + jnp.log(total), (ROWS, HD)))
    attended = jnp.concatenate(outs, axis=1).astype(BF)
    att[...] = attended
    lse[...] = jnp.concatenate(logs, axis=1)
    pa[...] = mm_nt(attended[:HALF], pw[...]).astype(BF)
    pb[...] = mm_nt(attended[HALF:], pw[...]).astype(BF)


def attend_back_body(place, slope, ma, mb, pw, q, kv, kvo, lse, dq, dkv, dkvo):
    mask = places(place, (ROWS, 1), 0) >= places(place, (1, ROWS), 1)
    own, earlier = key_terms(place, slope)
    do = jnp.concatenate([mm(ma[...], pw[...]), mm(mb[...], pw[...])], axis=0).astype(BF)
    dqs, dks, dvs, dkos, dvos = [], [], [], [], []
    for h in range(2):
        lo, hi = h * HD, (h + 1) * HD
        qh, kh, vh = q[:, lo:hi], kv[:, lo:hi], kv[:, 128 + lo : 128 + hi]
        koh, voh = kvo[:, lo:hi], kvo[:, 128 + lo : 128 + hi]
        doh = do[:, lo:hi]
        log = lse[:, lo : lo + 1]
        s1 = mm_nt(qh, kh) * 0.125 + own[h]
        p1 = jnp.exp(jnp.where(mask, s1, NEG) - log)
        p2 = jnp.exp(mm_nt(qh, koh) * 0.125 + earlier[h] - log)
        g1 = p1 * mm_nt(doh, vh)
        g2 = p2 * mm_nt(doh, voh)
        delta = jnp.sum(g1, axis=-1, keepdims=True) + jnp.sum(g2, axis=-1, keepdims=True)
        d1 = (g1 - p1 * delta).astype(BF)
        d2 = (g2 - p2 * delta).astype(BF)
        dqs.append((mm(d1, kh) + mm(d2, koh)) * 0.125)
        dks.append(mm_tn(d1, qh) * 0.125)
        dkos.append(mm_tn(d2, qh) * 0.125)
        dvs.append(mm_tn(p1.astype(BF), doh))
        dvos.append(mm_tn(p2.astype(BF), doh))
    dq[...] = jnp.concatenate(dqs, axis=1).astype(BF)
    dkv[...] = jnp.concatenate(dks + dvs, axis=1)
    dkvo[...] = jnp.concatenate(dkos + dvos, axis=1).astype(BF)


def ffn_body(na, nb, w1, w2, bias, act, dgel, pa, pb):
    for n, p, at in ((na, pa, 0), (nb, pb, HALF)):
        v = mm(n[...], w1[...]) + bias[...]
        v2 = v * v
        th = jnp.tanh(GELU_SCALE * (v + GELU_CUBE * (v2 * v)))
        one = 0.5 + 0.5 * th
        a = (v * one).astype(BF)
        act[at : at + HALF] = a
        dgel[at : at + HALF] = (
            one
            + (0.5 * GELU_SCALE) * v * (1.0 - th * th) * (1.0 + (3.0 * GELU_CUBE) * v2)
        ).astype(BF)
        p[...] = mm_nt(a, w2[...]).astype(BF)


def ffn_back_body(ea, eb, w1, w2, dgel, hg, sums, pa, pb):
    total = jnp.zeros((1, 512), F32)
    for e, p, at in ((ea, pa, 0), (eb, pb, HALF)):
        g = (mm(e[...], w2[...]) * dgel[at : at + HALF].astype(F32)).astype(BF)
        hg[at : at + HALF] = g
        total += jnp.sum(g.astype(F32), axis=0, keepdims=True)
        p[...] = mm_nt(g, w1[...]).astype(BF)
    sums[...] = total


def ffn_weights_body(ea, eb, act, na, nb, hg, out):
    out[:, :512] = (mm_tn(na[...], hg[:HALF]) + mm_tn(nb[...], hg[HALF:])).astype(BF)
    out[:, 512:] = (mm_tn(ea[...], act[:HALF]) + mm_tn(eb[...], act[HALF:])).astype(BF)


def proj_weights_body(ma, mb, att, out):
    out[...] = (mm_tn(ma[...], att[:HALF]) + mm_tn(mb[...], att[HALF:])).astype(BF)


def qkv_back_body(dq, dkv, got, w, joined, sums, pa, pb):
    j = jnp.concatenate(
        [dq[...], (dkv[...] + got[...].astype(F32)).astype(BF)], axis=1
    )
    joined[...] = j
    sums[...] = jnp.sum(j.astype(F32), axis=0, keepdims=True)
    pa[...] = mm_nt(j[:HALF], w[...]).astype(BF)
    pb[...] = mm_nt(j[HALF:], w[...]).astype(BF)


def qkv_weights_body(na, nb, joined, out):
    out[...] = (mm_tn(na[...], joined[:HALF]) + mm_tn(nb[...], joined[HALF:])).astype(BF)


def first_sums_body(pa, pb, xa, xb, sums):
    gain = jnp.zeros((1, D), F32)
    shift = jnp.zeros((1, D), F32)
    for p, x in ((pa, xa), (pb, xb)):
        g = p[...].astype(F32)
        xhat, _ = norm_parts(x[...].astype(F32))
        gain += jnp.sum(g * xhat, axis=0, keepdims=True)
        shift += jnp.sum(g, axis=0, keepdims=True)
    sums[0:1] = gain
    sums[1:2] = shift


def to_relative(x, order):
    def body(order_ref, src, dst):
        dst[...] = src[...]

    return pl.pallas_call(
        body,
        grid_spec=pltpu.PrefetchScalarGridSpec(
            num_scalar_prefetch=1,
            grid=(8,),
            in_specs=[pl.BlockSpec((PIECE, D), lambda j, o: (o[j], 0))],
            out_specs=pl.BlockSpec((PIECE, D), lambda j, o: (j, 0)),
        ),
        out_shape=sds((ROWS, D), x.dtype),
        name="to_relative",
    )(order, x)


def to_sequence(near, far, order, dtype):
    def body(order_ref, a, b, dst):
        j = pl.program_id(0)

        @pl.when(j < 4)
        def _():
            dst[...] = a[...].astype(dtype)

        @pl.when(j >= 4)
        def _():
            dst[...] = b[...].astype(dtype)

    return pl.pallas_call(
        body,
        grid_spec=pltpu.PrefetchScalarGridSpec(
            num_scalar_prefetch=1,
            grid=(8,),
            in_specs=[
                pl.BlockSpec((PIECE, D), lambda j, o: (jnp.minimum(j, 3), 0)),
                pl.BlockSpec((PIECE, D), lambda j, o: (jnp.maximum(j - 4, 0), 0)),
            ],
            out_specs=pl.BlockSpec((PIECE, D), lambda j, o: (o[j], 0)),
        ),
        out_shape=sds((ROWS, D), dtype),
        name="to_sequence",
    )(order, near, far)


def per_device(
    block_in, qkv_weight, proj_weight, fc1_weight, fc2_weight,
    qv_bias, fc1_bias, norm_gains, row_biases, cotangent,
):
    t = lax.axis_index(T)
    y, c = t // 2, t % 2
    ctx = lax.axis_index("context")
    place = jnp.stack([y, c, ctx]).astype(jnp.int32)
    slope = jnp.exp2(-8.0 * (2 * t + 1 + jnp.arange(2)).astype(F32) / HEADS)
    j = jnp.arange(8)
    order = (((c + j // 4) % 2) * 4 + (y - j % 4) % 4).astype(jnp.int32)

    qkv_w = qkv_weight.reshape(2, 64, 2, 3, HD).transpose(0, 1, 3, 2, 4).reshape(2, 64, 384)
    small = jnp.concatenate([norm_gains.reshape(4, 64), row_biases.reshape(8, 64)])
    first = jnp.concatenate(
        [qkv_w[0], small.reshape(2, 384), jnp.zeros((6, 384), BF)]
    )
    first_all = lax.all_to_all(jnp.broadcast_to(first[None], (16, 72, 384)), W, 0, 0)
    rest0 = lax.all_gather(
        jnp.concatenate([fc1_weight[0], fc2_weight[0], proj_weight[0]], axis=1), W, axis=0, tiled=True
    )
    rest1 = lax.all_gather(
        jnp.concatenate([fc1_weight[1], fc2_weight[1], proj_weight[1], qkv_w[1]], axis=1),
        W, axis=0, tiled=True,
    )
    qkv0 = first_all[:, :64].reshape(D, 384)
    small_all = first_all[:, 64:66].reshape(16, 12, 64).transpose(1, 0, 2).reshape(12, D).astype(F32)
    gains = small_all[:4].reshape(2, 2, D)
    biases = small_all[4:].reshape(2, 4, D)
    rests = (rest0, rest1)
    qkv_of = ((qkv0, (D, 384), (0, 0)), (rest1, (D, 384), (0, 3)))
    fc1_of = [(r, (D, 512), (0, 0)) for r in rests]
    fc2_of = [(r, (D, 512), (0, 1)) for r in rests]
    proj_of = [(r, (D, 128), (0, 8)) for r in rests]
    qv = qv_bias.astype(F32).reshape(2, 2, 2, HD).transpose(0, 2, 1, 3)
    zero = jnp.zeros((2, 1, 2, HD), F32)
    joined_bias = jnp.concatenate([qv[:, :1], zero, qv[:, 1:]], axis=1).reshape(2, 1, 384)
    up_bias = fc1_bias.astype(F32).reshape(2, 1, 512)

    x = to_relative(block_in.reshape(ROWS, D), order)
    cot = to_relative(cotangent.reshape(ROWS, D), order)
    half = (HALF, D)
    qs, kvs, row = (ROWS, 128), (ROWS, 256), (PIECE, D)

    saved = []
    stream = x
    normed = None
    for l in range(2):
        if l == 0:
            na, nb, q, kv = call(
                qkv_first_body, "qkv_first",
                [(x, half, (0, 0)), (x, half, (1, 0)), qkv_of[0],
                 (jnp.stack([gains[0, 0], biases[0, 0]]), (2, D), None), (joined_bias[0], (1, 384), None)],
                [sds(half, BF), sds(half, BF), sds(qs, BF), sds(kvs, BF)],
            )
        else:
            na, nb = gather_rows(normed)
            q, kv = call(
                qkv_body, "qkv",
                [(na, half, None), (nb, half, None), qkv_of[l], (joined_bias[l], (1, 384), None)],
                [sds(qs, BF), sds(kvs, BF)],
            )
        kvo = lax.ppermute(kv, "context", [(0, 1)])
        att, lse, pa, pb = call(
            attend_body, "attend",
            [(place, None, None), (slope, None, None), (q, qs, None), (kv, kvs, None), (kvo, kvs, None), proj_of[l]],
            [sds(qs, BF), sds(qs, F32), sds(half, BF), sds(half, BF)],
        )
        middle, second = norm_fwd(
            sum_pieces(pa, pb), stream, biases[l, 1], gains[l, 1], biases[l, 2]
        )
        sa, sb = gather_rows(second)
        act, dgel, pa, pb = call(
            ffn_body, "ffn",
            [(sa, half, None), (sb, half, None), fc1_of[l], fc2_of[l], (up_bias[l], (1, 512), None)],
            [sds((ROWS, 512), BF), sds((ROWS, 512), BF), sds(half, BF), sds(half, BF)],
        )
        saved.append((stream, na, nb, q, kv, kvo, att, lse, middle, sa, sb, act, dgel))
        nxt = min(l + 1, 1)
        stream, normed = norm_fwd(
            sum_pieces(pa, pb), middle, biases[l, 3], gains[nxt, 0], biases[nxt, 0]
        )
    oa, ob = gather_rows(stream.astype(BF))
    block_out = to_sequence(oa, ob, order, BF)

    grad = cot
    ea = (cot, half, (0, 0))
    eb = (cot, half, (1, 0))
    own_cot = cot[:PIECE].astype(F32)
    sums = {"b13": jnp.sum(own_cot, axis=0)}
    owned = [None, None]
    for l in (1, 0):
        stream, na, nb, q, kv, kvo, att, lse, middle, sa, sb, act, dgel = saved[l]
        hg, up_sum, pa, pb = call(
            ffn_back_body, "ffn_back",
            [ea, eb, fc1_of[l], fc2_of[l], (dgel, (ROWS, 512), None)],
            [sds((ROWS, 512), BF), sds((1, 512), F32), sds(half, BF), sds(half, BF)],
        )
        (ffn_grad,) = call(
            ffn_weights_body, "ffn_weights",
            [ea, eb, (act, (ROWS, 512), None), (sa, half, None), (sb, half, None), (hg, (ROWS, 512), None)],
            [sds((D, D), BF)],
        )
        ffn_owned = lax.psum_scatter(ffn_grad, W, scatter_dimension=0, tiled=True)
        mid, mid_low, s2 = norm_bwd(sum_pieces(pa, pb), middle, grad, gains[l, 1])
        ma, mb = gather_rows(mid_low)
        dq, dkv, dkvo = call(
            attend_back_body, "attend_back",
            [(place, None, None), (slope, None, None), (ma, half, None), (mb, half, None), proj_of[l],
             (q, qs, None), (kv, kvs, None), (kvo, kvs, None), (lse, qs, None)],
            [sds(qs, BF), sds(kvs, F32), sds(kvs, BF)],
        )
        got = lax.ppermute(dkvo, "context", [(1, 0)])
        (proj_grad,) = call(
            proj_weights_body, "proj_weights",
            [(ma, half, None), (mb, half, None), (att, qs, None)],
            [sds((D, 128), BF)],
        )
        joined, qv_sum, pa, pb = call(
            qkv_back_body, "qkv_back",
            [(dq, qs, None), (dkv, kvs, None), (got, kvs, None), qkv_of[l]],
            [sds((ROWS, 384), BF), sds((1, 384), F32), sds(half, BF), sds(half, BF)],
        )
        (qkv_grad,) = call(
            qkv_weights_body, "qkv_weights",
            [(na, half, None), (nb, half, None), (joined, (ROWS, 384), None)],
            [sds((D, 384), BF)],
        )
        attn_grad = jnp.concatenate([qkv_grad, proj_grad], axis=1)
        sums[f"g{l}1"], sums[f"b{l}2"], sums[f"b{l}1"] = s2[0], s2[1], s2[2]
        sums[f"up{l}"], sums[f"qv{l}"] = up_sum[0], qv_sum[0]
        if l == 1:
            attn_owned = lax.psum_scatter(attn_grad, W, scatter_dimension=0, tiled=True)
            grad, low, s1 = norm_bwd(sum_pieces(pa, pb), stream, mid, gains[l, 0])
            sums["g10"], sums["b10"], sums["b03"] = s1[0], s1[1], s1[2]
            near, far = gather_rows(low)
            ea, eb = (near, half, None), (far, half, None)
            owned[1] = (ffn_owned, attn_owned)
        else:
            (s1,) = call(
                first_sums_body, "first_sums",
                [(pa, half, None), (pb, half, None), (x, half, (0, 0)), (x, half, (1, 0))],
                [sds((2, D), F32)],
            )
            sums["g00"], sums["b00"] = s1[0], s1[1]
            columns = jnp.stack(
                [sums[k] for k in ("g00", "g01", "g10", "g11", "b00", "b01", "b02", "b03", "b10", "b11", "b12", "b13")]
            )
            columns = columns.reshape(12, 16, 64).transpose(1, 0, 2).reshape(16, 768)
            columns = jnp.pad(columns, ((0, 0), (0, 256))).astype(BF).reshape(16, 2, 512)
            line = jnp.concatenate([sums["qv0"], sums["qv1"], sums["up0"], sums["up1"]])
            line = jnp.pad(line, (0, 2048 - line.size))
            high = line.astype(BF)
            rest = (line - high.astype(F32)).astype(BF)
            both = jnp.stack([high, rest]).reshape(1, 8, 512)
            packed = jnp.concatenate(
                [attn_grad.reshape(16, 64, 512), columns, jnp.broadcast_to(both, (16, 8, 512))], axis=1
            )
            pieces = sum_pieces(pa, pb)
            mixed = lax.all_to_all(packed, W, 0, 0)
            mixed = jnp.sum(mixed.astype(F32), axis=0)
            grad, low, _ = norm_bwd(pieces, stream, mid, gains[l, 0])
            own_columns = mixed[64:66].reshape(1024)[:768]
            tail = jnp.pad(own_columns, (0, 256))
            tail_high = tail.astype(BF)
            tail_low = (tail - tail_high.astype(F32)).astype(BF)
            extra = jnp.concatenate(
                [tail_high[None], tail_low[None], jnp.zeros((14, D), BF)]
            )
            own = jnp.concatenate([low, extra])
            r2, r1, r3 = along_y(own, 2), along_y(own, 1), along_y(own, 3)
            all_near = jnp.stack([own, r1, r2, r3])
            all_far = core_swap(all_near)
            near = all_near[:, :PIECE].reshape(HALF, D)
            far = all_far[:, :PIECE].reshape(HALF, D)
            input_grad = to_sequence(near, far, order, F32)
            tails = jnp.sum(
                all_near[:, PIECE : PIECE + 2].astype(F32), axis=(0, 1)
            ) + jnp.sum(all_far[:, PIECE : PIECE + 2].astype(F32), axis=(0, 1))
            tails = tails[:768].reshape(12, 64)
            sums_line = mixed[66:70].reshape(2048) + mixed[70:74].reshape(2048)
            owned[0] = (ffn_owned, mixed[:64])

    def back_order(g):
        return g.reshape(64, 3, 2, HD).transpose(0, 2, 1, 3).reshape(64, 384)

    qv_out, up_out = [], []
    for l in range(2):
        qv_l = sums_line[384 * l : 384 * (l + 1)].reshape(3, 2, HD)
        qv_out.append(jnp.stack([qv_l[0], qv_l[2]], axis=1).reshape(256))
        up_out.append(sums_line[768 + 512 * l : 768 + 512 * (l + 1)])
    return (
        block_out[None],
        input_grad[None],
        jnp.stack([back_order(o[1][:, :384].astype(F32)) for o in owned]),
        jnp.stack([o[1][:, 384:].astype(F32) for o in owned]),
        jnp.stack([o[0][:, :512].astype(F32) for o in owned]),
        jnp.stack([o[0][:, 512:].astype(F32) for o in owned]),
        jnp.stack(qv_out),
        jnp.stack(up_out),
        tails[:4].reshape(2, 2, 64),
        tails[4:].reshape(2, 4, 64),
    )


def solution(mesh):
    return jax.shard_map(
        per_device,
        mesh=mesh,
        in_specs=(
            P("shard", "context", None),
            P(None, W, T),
            P(None, W, T),
            P(None, W, T),
            P(None, W, T),
            P(None, T),
            P(None, T),
            P(None, None, W),
            P(None, None, W),
            P("shard", "context", None),
        ),
        out_specs=(
            P("shard", "context", None),
            P("shard", "context", None),
            P(None, W, T),
            P(None, W, T),
            P(None, W, T),
            P(None, W, T),
            P(None, T),
            P(None, T),
            P(None, None, W),
            P(None, None, W),
        ),
        check_vma=False,
    )
```

```python
import jax
import jax.numpy as jnp
from jax import lax
from jax.experimental import pallas as pl
from jax.experimental.pallas import tpu as pltpu
from jax.sharding import PartitionSpec as P

HEADS = 16
HD = 64
NORM_EPS = 1e-05
GELU_SCALE = 0.7978845608028654
GELU_CUBE = 0.044715
F32 = jnp.float32
BF = jnp.bfloat16
W = ("shard", "context")
T = "tensor"
ROWS = 512
HALF = 256
PIECE = 64
D = 1024
NEG = -1e30


def spec(shape, index=None):
    place = tuple(index) if index is not None else (0,) * len(shape)
    return pl.BlockSpec(shape, lambda i: place)


def smem():
    return pl.BlockSpec(memory_space=pltpu.SMEM)


def call(body, name, operands, outs):
    in_specs, args = [], []
    for array, shape, index in operands:
        in_specs.append(smem() if shape is None else spec(shape, index))
        args.append(array)
    return pl.pallas_call(
        body,
        grid=(1,),
        in_specs=in_specs,
        out_specs=[spec(o.shape) for o in outs],
        out_shape=outs,
        compiler_params=pltpu.CompilerParams(vmem_limit_bytes=50 << 20),
        name=name,
    )(*args)


def sds(shape, dtype):
    return jax.ShapeDtypeStruct(shape, dtype)


def mm(a, b):
    return lax.dot_general(a, b, (((1,), (0,)), ((), ())), preferred_element_type=F32)


def mm_nt(a, b):
    return lax.dot_general(a, b, (((1,), (1,)), ((), ())), preferred_element_type=F32)


def mm_tn(a, b):
    return lax.dot_general(a, b, (((0,), (0,)), ((), ())), preferred_element_type=F32)


def core_swap(v):
    return lax.ppermute(v, T, [(i, i ^ 1) for i in range(8)])


def along_y(v, step):
    return lax.ppermute(
        v, T, [(2 * y + c, 2 * ((y + step) % 4) + c) for y in range(4) for c in range(2)]
    )


def add_body(pa, got, h0, h1, h2, h3):
    both = pa[...].astype(F32) + got[...].astype(F32)
    h0[...] = both[:PIECE]
    h1[...] = both[PIECE : 2 * PIECE].astype(BF)
    h2[...] = both[2 * PIECE : 3 * PIECE].astype(BF)
    h3[...] = both[3 * PIECE :].astype(BF)


def sum_pieces(keep, send):
    got = core_swap(send)
    h0, h1, h2, h3 = call(
        add_body,
        "pair_add",
        [(keep, (HALF, D), None), (got, (HALF, D), None)],
        [sds((PIECE, D), F32)] + [sds((PIECE, D), BF)] * 3,
    )
    r2 = along_y(h2, -2)
    r1 = along_y(h1, -1)
    r3 = along_y(h3, -3)
    return h0, r1, r2, r3


def gather_rows(own):
    r2 = along_y(own, 2)
    r1 = along_y(own, 1)
    r3 = along_y(own, 3)
    near = jnp.concatenate([own, r1, r2, r3], axis=0)
    far = core_swap(near)
    return near, far


def norm_parts(v):
    mean = jnp.mean(v, axis=-1, keepdims=True)
    centred = v - mean
    var = jnp.mean(centred * centred, axis=-1, keepdims=True)
    s = lax.rsqrt(var + NORM_EPS)
    return centred * s, s


def gain_row(table, l, i):
    at = 2 * l + i
    return table[at : at + 1]


def bias_row(table, l, i):
    at = 4 + 4 * l + i
    return table[at : at + 1]


def norm_fwd(pieces, resid, table, bias_at, next_at):
    def body(h0, r1, r2, r3, resid_ref, rows, stream, normed):
        v = (
            h0[...] + r1[...].astype(F32) + r2[...].astype(F32) + r3[...].astype(F32)
        ) + resid_ref[...].astype(F32) + bias_row(rows, *bias_at)
        stream[...] = v
        xhat, _ = norm_parts(v)
        gain, shift = next_at
        normed[...] = (xhat * gain_row(rows, *gain) + bias_row(rows, *shift)).astype(BF)

    b = (PIECE, D)
    return call(
        body,
        "norm_fwd",
        [(p, b, None) for p in (*pieces, resid)] + [(table, (12, D), None)],
        [sds(b, F32), sds(b, BF)],
    )


def norm_bwd(pieces, stream, grad, table, gain_at):
    def body(h0, r1, r2, r3, stream_ref, grad_ref, rows, out, low, sums):
        g = h0[...] + r1[...].astype(F32) + r2[...].astype(F32) + r3[...].astype(F32)
        xhat, s = norm_parts(stream_ref[...].astype(F32))
        gx = g * xhat
        c = g * gain_row(rows, *gain_at)
        cx = c * xhat
        e = grad_ref[...].astype(F32) + s * (
            c
            - jnp.mean(c, axis=-1, keepdims=True)
            - xhat * jnp.mean(cx, axis=-1, keepdims=True)
        )
        out[...] = e
        low[...] = e.astype(BF)
        sums[0:1] = jnp.sum(gx, axis=0, keepdims=True)
        sums[1:2] = jnp.sum(g, axis=0, keepdims=True)
        sums[2:3] = jnp.sum(e, axis=0, keepdims=True)

    b = (PIECE, D)
    return call(
        body,
        "norm_bwd",
        [(p, b, None) for p in (*pieces, stream, grad)] + [(table, (12, D), None)],
        [sds(b, F32), sds(b, BF), sds((3, D), F32)],
    )


def qkv_first_body(xa, xb, first, rows, bias, na, nb, q, kv):
    w = qkv_matrix(first)
    for x, n, at in ((xa, na, 0), (xb, nb, HALF)):
        xhat, _ = norm_parts(x[...].astype(F32))
        normed = (xhat * gain_row(rows, 0, 0) + bias_row(rows, 0, 0)).astype(BF)
        n[...] = normed
        joined = mm(normed, w) + bias[...]
        q[at : at + HALF] = joined[:, :128].astype(BF)
        kv[at : at + HALF] = joined[:, 128:].astype(BF)


def qkv_body(na, nb, w, bias, q, kv):
    for n, at in ((na, 0), (nb, HALF)):
        joined = mm(n[...], w[...]) + bias[...]
        q[at : at + HALF] = joined[:, :128].astype(BF)
        kv[at : at + HALF] = joined[:, 128:].astype(BF)


def proj_matrix(ref):
    return ref[:, :64, 384:].reshape(D, 128) if len(ref.shape) == 3 else ref[...]


def qkv_matrix(ref):
    return ref[:, :64, :384].reshape(D, 384) if len(ref.shape) == 3 else ref[...]


def places(place, shape, axis):
    r = lax.broadcasted_iota(jnp.int32, shape, axis)
    y, c = place[0], place[1]
    return ((y - ((r >> 6) & 3)) & 3) * 128 + ((c + (r >> 8)) & 1) * 64 + (r & 63)


def key_terms(place, slope):
    pos = places(place, (1, ROWS), 1).astype(F32)
    off = jnp.where(place[2] == 1, 0.0, NEG)
    own = [slope[h] * pos for h in range(2)]
    earlier = [slope[h] * (pos - 512.0) + off for h in range(2)]
    return own, earlier


def attend_body(place, slope, q, kv, kvo, pw, att, lse, pa, pb):
    mask = places(place, (ROWS, 1), 0) >= places(place, (1, ROWS), 1)
    own, earlier = key_terms(place, slope)
    outs, logs = [], []
    for h in range(2):
        lo, hi = h * HD, (h + 1) * HD
        qh = q[:, lo:hi]
        s1 = mm_nt(qh, kv[:, lo:hi]) * 0.125 + own[h]
        s1 = jnp.where(mask, s1, NEG)
        s2 = mm_nt(qh, kvo[:, lo:hi]) * 0.125 + earlier[h]
        top = jnp.maximum(
            jnp.max(s1, axis=-1, keepdims=True), jnp.max(s2, axis=-1, keepdims=True)
        )
        p1 = jnp.exp(s1 - top)
        p2 = jnp.exp(s2 - top)
        total = jnp.sum(p1, axis=-1, keepdims=True) + jnp.sum(p2, axis=-1, keepdims=True)
        o = mm(p1.astype(BF), kv[:, 128 + lo : 128 + hi]) + mm(
            p2.astype(BF), kvo[:, 128 + lo : 128 + hi]
        )
        outs.append(o / total)
        logs.append(jnp.broadcast_to(top + jnp.log(total), (ROWS, HD)))
    attended = jnp.concatenate(outs, axis=1).astype(BF)
    att[...] = attended
    lse[...] = jnp.concatenate(logs, axis=1)
    pa[...] = mm_nt(attended[:HALF], proj_matrix(pw)).astype(BF)
    pb[...] = mm_nt(attended[HALF:], proj_matrix(pw)).astype(BF)


def attend_back_body(place, slope, ma, mb, pw, q, kv, kvo, lse, dq, dkv, dkvo):
    mask = places(place, (ROWS, 1), 0) >= places(place, (1, ROWS), 1)
    own, earlier = key_terms(place, slope)
    do = jnp.concatenate([mm(ma[...], proj_matrix(pw)), mm(mb[...], proj_matrix(pw))], axis=0).astype(BF)
    dqs, dks, dvs, dkos, dvos = [], [], [], [], []
    for h in range(2):
        lo, hi = h * HD, (h + 1) * HD
        qh, kh, vh = q[:, lo:hi], kv[:, lo:hi], kv[:, 128 + lo : 128 + hi]
        koh, voh = kvo[:, lo:hi], kvo[:, 128 + lo : 128 + hi]
        doh = do[:, lo:hi]
        log = lse[:, lo : lo + 1]
        s1 = mm_nt(qh, kh) * 0.125 + own[h]
        p1 = jnp.exp(jnp.where(mask, s1, NEG) - log)
        p2 = jnp.exp(mm_nt(qh, koh) * 0.125 + earlier[h] - log)
        g1 = p1 * mm_nt(doh, vh)
        g2 = p2 * mm_nt(doh, voh)
        delta = jnp.sum(g1, axis=-1, keepdims=True) + jnp.sum(g2, axis=-1, keepdims=True)
        d1 = (g1 - p1 * delta).astype(BF)
        d2 = (g2 - p2 * delta).astype(BF)
        dqs.append((mm(d1, kh) + mm(d2, koh)) * 0.125)
        dks.append(mm_tn(d1, qh) * 0.125)
        dkos.append(mm_tn(d2, qh) * 0.125)
        dvs.append(mm_tn(p1.astype(BF), doh))
        dvos.append(mm_tn(p2.astype(BF), doh))
    dq[...] = jnp.concatenate(dqs, axis=1).astype(BF)
    dkv[...] = jnp.concatenate(dks + dvs, axis=1)
    dkvo[...] = jnp.concatenate(dkos + dvos, axis=1).astype(BF)


def ffn_body(na, nb, w1, w2, bias, act, dgel, pa, pb):
    for n, p, at in ((na, pa, 0), (nb, pb, HALF)):
        v = mm(n[...], w1[...]) + bias[...]
        v2 = v * v
        th = jnp.tanh(GELU_SCALE * (v + GELU_CUBE * (v2 * v)))
        one = 0.5 + 0.5 * th
        a = (v * one).astype(BF)
        act[at : at + HALF] = a
        dgel[at : at + HALF] = (
            one
            + (0.5 * GELU_SCALE) * v * (1.0 - th * th) * (1.0 + (3.0 * GELU_CUBE) * v2)
        ).astype(BF)
        p[...] = mm_nt(a, w2[...]).astype(BF)


def ffn_last_body(order, na, nb, w1, w2, bias, act, dgel, out):
    for dc, n in enumerate((na, nb)):
        at = dc * HALF
        v = mm(n[...], w1[...]) + bias[...]
        v2 = v * v
        th = jnp.tanh(GELU_SCALE * (v + GELU_CUBE * (v2 * v)))
        one = 0.5 + 0.5 * th
        a = (v * one).astype(BF)
        act[at : at + HALF] = a
        dgel[at : at + HALF] = (
            one
            + (0.5 * GELU_SCALE) * v * (1.0 - th * th) * (1.0 + (3.0 * GELU_CUBE) * v2)
        ).astype(BF)
        p = mm_nt(a, w2[...]).astype(BF)
        for k in range(4):
            row = pl.multiple_of(order[4 * dc + k] * PIECE, PIECE)
            out[pl.ds(row, PIECE)] = p[k * PIECE : (k + 1) * PIECE]


def ffn_back_body(ea, eb, w1, w2, dgel, hg, sums, pa, pb):
    total = jnp.zeros((1, 512), F32)
    for e, p, at in ((ea, pa, 0), (eb, pb, HALF)):
        g = (mm(e[...], w2[...]) * dgel[at : at + HALF].astype(F32)).astype(BF)
        hg[at : at + HALF] = g
        total += jnp.sum(g.astype(F32), axis=0, keepdims=True)
        p[...] = mm_nt(g, w1[...]).astype(BF)
    sums[...] = total


def ffn_weights_body(ea, eb, act, na, nb, hg, out):
    out[:, :512] = (mm_tn(na[...], hg[:HALF]) + mm_tn(nb[...], hg[HALF:])).astype(BF)
    out[:, 512:] = (mm_tn(ea[...], act[:HALF]) + mm_tn(eb[...], act[HALF:])).astype(BF)


def layer_weights_body(ea, eb, act, sa, sb, hg, na, nb, joined, ma, mb, att, out):
    ffn_weights_body(ea, eb, act, sa, sb, hg, out.at[:, :1024])
    out[:, 1024:1408] = (
        mm_tn(na[...], joined[:HALF]) + mm_tn(nb[...], joined[HALF:])
    ).astype(BF)
    out[:, 1408:] = (mm_tn(ma[...], att[:HALF]) + mm_tn(mb[...], att[HALF:])).astype(BF)


def two_halves(v):
    high = v.astype(BF)
    return high, (v - high.astype(F32)).astype(BF)


def last_pack_body(
    na, nb, joined, ma, mb, att, pa, pb, xa, xb,
    s21, s11, s20, b13, up0, up1, qv0, qv1, out,
):
    g = (mm_tn(na[...], joined[:HALF]) + mm_tn(nb[...], joined[HALF:])).astype(BF)
    out[:, :64, :384] = g.reshape(16, 64, 384)
    g = (mm_tn(ma[...], att[:HALF]) + mm_tn(mb[...], att[HALF:])).astype(BF)
    out[:, :64, 384:] = g.reshape(16, 64, 128)
    gain = jnp.zeros((1, D), F32)
    shift = jnp.zeros((1, D), F32)
    for p, x in ((pa, xa), (pb, xb)):
        g = p[...].astype(F32)
        xhat, _ = norm_parts(x[...].astype(F32))
        gain += jnp.sum(g * xhat, axis=0, keepdims=True)
        shift += jnp.sum(g, axis=0, keepdims=True)
    columns = jnp.concatenate(
        [
            gain, s20[0:1], s11[0:1], s21[0:1],
            shift, s20[2:3], s20[1:2], s11[2:3], s11[1:2], s21[2:3], s21[1:2], b13[...],
        ]
    ).astype(BF)
    q0, q0l = two_halves(qv0[...])
    q1, q1l = two_halves(qv1[...])
    u0, u0l = two_halves(up0[...])
    u1, u1l = two_halves(up1[...])
    none = jnp.zeros((1, 384), BF)
    lines = jnp.concatenate(
        [
            q0, q1, q0l, q1l,
            u0[:, :384], u1[:, :384], u0l[:, :384], u1l[:, :384],
            jnp.concatenate([u0[:, 384:], u1[:, 384:], none[:, :128]], axis=1),
            jnp.concatenate([u0l[:, 384:], u1l[:, 384:], none[:, :128]], axis=1),
            none, none,
        ]
    )
    for w in range(16):
        at = 128 * (w // 2)
        tail = jnp.concatenate([columns[:, at : at + 128], lines], axis=1)
        out[w, 64:80] = jnp.concatenate([tail, jnp.zeros((4, 512), BF)])


def qkv_back_body(dq, dkv, got, w, joined, sums, pa, pb):
    j = jnp.concatenate(
        [dq[...], (dkv[...] + got[...].astype(F32)).astype(BF)], axis=1
    )
    joined[...] = j
    sums[...] = jnp.sum(j.astype(F32), axis=0, keepdims=True)
    m = qkv_matrix(w)
    pa[...] = mm_nt(j[:HALF], m).astype(BF)
    pb[...] = mm_nt(j[HALF:], m).astype(BF)


def pack_first_body(qkv, proj, fc1, fc2, gains, biases, first, rest0, rest1):
    def ordered(m):
        parts = [m[:, i * HD : (i + 1) * HD] for i in range(6)]
        return jnp.concatenate([parts[i] for i in (0, 3, 1, 4, 2, 5)], axis=1)

    small = [gains[l, i : i + 1] for l in range(2) for i in range(2)]
    small += [biases[l, i : i + 1] for l in range(2) for i in range(4)]
    lines = jnp.concatenate(
        [jnp.concatenate([small[2 * i], small[2 * i + 1]], axis=1) for i in range(6)]
        + [jnp.zeros((2, 128), BF)]
    )
    own = jnp.concatenate(
        [
            jnp.concatenate([ordered(qkv[0]), proj[0]], axis=1),
            jnp.concatenate([lines, jnp.zeros((8, 384), BF)], axis=1),
        ]
    )
    for w in range(16):
        first[w] = own
    rest0[:, :512] = fc1[0]
    rest0[:, 512:1024] = fc2[0]
    rest0[:, 1024:1152] = jnp.zeros((64, 128), BF)
    rest0[:, 1152:] = ordered(qkv[1])
    rest1[:, :512] = fc1[1]
    rest1[:, 512:1024] = fc2[1]
    rest1[:, 1024:] = proj[1]


def relative_body(order, x, cot, xr, cr, total):
    for j in range(8):
        row = pl.multiple_of(order[j] * PIECE, PIECE)
        xr[j * PIECE : (j + 1) * PIECE] = x[pl.ds(row, PIECE)]
        cr[j * PIECE : (j + 1) * PIECE] = cot[pl.ds(row, PIECE)]
    total[...] = jnp.sum(cr[:PIECE].astype(F32), axis=0, keepdims=True)


def sequence_body(order, near, far, out):
    for j in range(8):
        row = pl.multiple_of(order[j] * PIECE, PIECE)
        src = near if j < 4 else far
        k = j % 4
        out[pl.ds(row, PIECE)] = src[k * PIECE : (k + 1) * PIECE].astype(F32)


def per_device(
    block_in, qkv_weight, proj_weight, fc1_weight, fc2_weight,
    qv_bias, fc1_bias, norm_gains, row_biases, cotangent,
):
    t = lax.axis_index(T)
    y, c = t // 2, t % 2
    ctx = lax.axis_index("context")
    place = jnp.stack([y, c, ctx]).astype(jnp.int32)
    slope = jnp.exp2(-8.0 * (2 * t + 1 + jnp.arange(2)).astype(F32) / HEADS)
    j = jnp.arange(8)
    order = (2 * ((y - j % 4) % 4) + (c + j // 4) % 2).astype(jnp.int32)
    half = (HALF, D)
    qs, kvs, hs, js = (ROWS, 128), (ROWS, 256), (ROWS, 512), (ROWS, 384)

    first, part0, part1 = call(
        pack_first_body, "pack_first",
        [(v, v.shape, None) for v in (qkv_weight, proj_weight, fc1_weight, fc2_weight, norm_gains, row_biases)],
        [sds((16, 72, 512), BF), sds((64, 1536), BF), sds((64, 1152), BF)],
    )
    first_all = lax.all_to_all(first, W, 0, 0)
    rest0 = lax.all_gather(part0, W, axis=0, tiled=True)
    rest1 = lax.all_gather(part1, W, axis=0, tiled=True)
    table = (
        first_all[:, 64:70, :128].reshape(16, 12, 64).transpose(1, 0, 2).reshape(12, D).astype(F32)
    )
    tab = (table, (12, D), None)
    whole_first = (first_all, (16, 72, 512), None)
    qkv_of = (whole_first, (rest0, (D, 384), (0, 3)))
    proj_of = (whole_first, (rest1, (D, 128), (0, 8)))
    fc1_of = [(r, (D, 512), (0, 0)) for r in (rest0, rest1)]
    fc2_of = [(r, (D, 512), (0, 1)) for r in (rest0, rest1)]
    qv = qv_bias.astype(F32).reshape(2, 2, 2, HD).transpose(0, 2, 1, 3)
    zero = jnp.zeros((2, 1, 2, HD), F32)
    joined_bias = jnp.concatenate([qv[:, :1], zero, qv[:, 1:]], axis=1).reshape(2, 1, 384)
    up_bias = fc1_bias.astype(F32).reshape(2, 1, 512)

    x, cot, b13 = call(
        relative_body, "to_relative",
        [(order, None, None), (block_in.reshape(ROWS, D), (ROWS, D), None), (cotangent.reshape(ROWS, D), (ROWS, D), None)],
        [sds((ROWS, D), BF), sds((ROWS, D), BF), sds((1, D), F32)],
    )

    saved = []
    stream = x
    normed = None
    for l in range(2):
        if l == 0:
            na, nb, q, kv = call(
                qkv_first_body, "qkv_first",
                [(x, half, (0, 0)), (x, half, (1, 0)), whole_first, tab, (joined_bias[0], (1, 384), None)],
                [sds(half, BF), sds(half, BF), sds(qs, BF), sds(kvs, BF)],
            )
        else:
            na, nb = gather_rows(normed)
            q, kv = call(
                qkv_body, "qkv",
                [(na, half, None), (nb, half, None), qkv_of[l], (joined_bias[l], (1, 384), None)],
                [sds(qs, BF), sds(kvs, BF)],
            )
        kvo = lax.ppermute(kv, "context", [(0, 1)])
        att, lse, pa, pb = call(
            attend_body, "attend",
            [(place, None, None), (slope, None, None), (q, qs, None), (kv, kvs, None), (kvo, kvs, None), proj_of[l]],
            [sds(qs, BF), sds(qs, F32), sds(half, BF), sds(half, BF)],
        )
        middle, second = norm_fwd(
            sum_pieces(pa, pb), stream, table, (l, 1), ((l, 1), (l, 2))
        )
        sa, sb = gather_rows(second)
        ffn_in = [(sa, half, None), (sb, half, None), fc1_of[l], fc2_of[l], (up_bias[l], (1, 512), None)]
        if l == 0:
            act, dgel, pa, pb = call(
                ffn_body, "ffn", ffn_in,
                [sds(hs, BF), sds(hs, BF), sds(half, BF), sds(half, BF)],
            )
        else:
            act, dgel, terms = call(
                ffn_last_body, "ffn_last", [(order, None, None)] + ffn_in,
                [sds(hs, BF), sds(hs, BF), sds((ROWS, D), BF)],
            )
        saved.append((stream, na, nb, q, kv, kvo, att, lse, middle, sa, sb, act, dgel))
        if l == 0:
            stream, normed = norm_fwd(
                sum_pieces(pa, pb), middle, table, (0, 3), ((1, 0), (1, 0))
            )
    out_own = lax.psum_scatter(terms, T, scatter_dimension=0, tiled=True)
    out_own = (middle + out_own.astype(F32) + table[11:12]).astype(BF)
    block_out = lax.all_gather(out_own, T, axis=0, tiled=True)

    grad = cot
    ea = (cot, half, (0, 0))
    eb = (cot, half, (1, 0))
    for l in (1, 0):
        stream, na, nb, q, kv, kvo, att, lse, middle, sa, sb, act, dgel = saved[l]
        hg, up_sum, pa, pb = call(
            ffn_back_body, "ffn_back",
            [ea, eb, fc1_of[l], fc2_of[l], (dgel, hs, None)],
            [sds(hs, BF), sds((1, 512), F32), sds(half, BF), sds(half, BF)],
        )
        pieces = sum_pieces(pa, pb)
        ffn_ops = [ea, eb, (act, hs, None), (sa, half, None), (sb, half, None), (hg, hs, None)]
        if l == 0:
            (ffn_grad,) = call(ffn_weights_body, "ffn_weights", ffn_ops, [sds((D, D), BF)])
            pieces, ffn_grad = lax.optimization_barrier((pieces, ffn_grad))
            ffn_pieces = lax.all_to_all(ffn_grad.reshape(16, 64, D), W, 0, 0)
        mid, mid_low, s2 = norm_bwd(pieces, middle, grad, table, (l, 1))
        ma, mb = gather_rows(mid_low)
        dq, dkv, dkvo = call(
            attend_back_body, "attend_back",
            [(place, None, None), (slope, None, None), (ma, half, None), (mb, half, None), proj_of[l],
             (q, qs, None), (kv, kvs, None), (kvo, kvs, None), (lse, qs, None)],
            [sds(qs, BF), sds(kvs, F32), sds(kvs, BF)],
        )
        got = lax.ppermute(dkvo, "context", [(1, 0)])
        joined, qv_sum, pa, pb = call(
            qkv_back_body, "qkv_back",
            [(dq, qs, None), (dkv, kvs, None), (got, kvs, None), qkv_of[l]],
            [sds(js, BF), sds((1, 384), F32), sds(half, BF), sds(half, BF)],
        )
        pieces = sum_pieces(pa, pb)
        attn_ops = [(na, half, None), (nb, half, None), (joined, js, None), (ma, half, None), (mb, half, None), (att, qs, None)]
        if l == 1:
            (layer_grad,) = call(
                layer_weights_body, "layer_weights", ffn_ops + attn_ops, [sds((D, 1536), BF)]
            )
            pieces, layer_grad = lax.optimization_barrier((pieces, layer_grad))
            owned1 = lax.psum_scatter(layer_grad, W, scatter_dimension=0, tiled=True)
            up1, qv1, s21 = up_sum, qv_sum, s2
            grad, low, s11 = norm_bwd(pieces, stream, mid, table, (1, 0))
            near, far = gather_rows(low)
            ea, eb = (near, half, None), (far, half, None)
        else:
            three, one = (3, D), (1, D)
            (packed,) = call(
                last_pack_body, "last_pack",
                attn_ops
                + [(pa, half, None), (pb, half, None), (x, half, (0, 0)), (x, half, (1, 0))]
                + [(s21, three, None), (s11, three, None), (s2, three, None), (b13, one, None)]
                + [(up_sum, (1, 512), None), (up1, (1, 512), None), (qv_sum, (1, 384), None), (qv1, (1, 384), None)],
                [sds((16, 80, 512), BF)],
            )
            pieces, packed = lax.optimization_barrier((pieces, packed))
            mixed = lax.all_to_all(packed, W, 0, 0)
            _, low, _ = norm_bwd(pieces, stream, mid, table, (0, 0))
            near, far = gather_rows(low)
            (input_grad,) = call(
                sequence_body, "to_sequence",
                [(order, None, None), (near, half, None), (far, half, None)],
                [sds((ROWS, D), F32)],
            )
    mixed = jnp.sum(mixed.astype(F32), axis=0)
    ffn0 = jnp.sum(ffn_pieces.astype(F32), axis=0)
    own_w = lax.axis_index(W)
    tails = jnp.where(own_w % 2 == 0, mixed[64:76, :64], mixed[64:76, 64:128])
    for step in (1, 2, 4):
        tails = tails + lax.ppermute(tails, T, [(i, i ^ step) for i in range(8)])
    lines = mixed[64:74, 128:]
    qv_line = lines[0:2] + lines[2:4]
    up_line = jnp.concatenate(
        [lines[4:6] + lines[6:8], (lines[8, :256] + lines[9, :256]).reshape(2, 128)], axis=1
    )

    def back_order(g):
        return g.reshape(64, 3, 2, HD).transpose(0, 2, 1, 3).reshape(64, 384)

    qv3 = qv_line.reshape(2, 3, 2, HD)
    owned1 = owned1.astype(F32)
    return (
        block_out[None],
        input_grad[None],
        jnp.stack([back_order(mixed[:64, :384]), back_order(owned1[:, 1024:1408])]),
        jnp.stack([mixed[:64, 384:], owned1[:, 1408:]]),
        jnp.stack([ffn0[:, :512], owned1[:, :512]]),
        jnp.stack([ffn0[:, 512:], owned1[:, 512:1024]]),
        jnp.stack([qv3[:, 0], qv3[:, 2]], axis=2).reshape(2, 256),
        up_line,
        tails[:4].reshape(2, 2, 64),
        tails[4:].reshape(2, 4, 64),
    )


def solution(mesh):
    return jax.shard_map(
        per_device,
        mesh=mesh,
        in_specs=(
            P("shard", "context", None),
            P(None, W, T),
            P(None, W, T),
            P(None, W, T),
            P(None, W, T),
            P(None, T),
            P(None, T),
            P(None, None, W),
            P(None, None, W),
            P("shard", "context", None),
        ),
        out_specs=(
            P("shard", "context", None),
            P("shard", "context", None),
            P(None, W, T),
            P(None, W, T),
            P(None, W, T),
            P(None, W, T),
            P(None, T),
            P(None, T),
            P(None, None, W),
            P(None, None, W),
        ),
        check_vma=False,
    )
```

```python
import jax
import jax.numpy as jnp
from jax import lax
from jax.experimental import pallas as pl
from jax.experimental.pallas import tpu as pltpu
from jax.sharding import PartitionSpec as P

HEADS = 16
HD = 64
NORM_EPS = 1e-05
GELU_SCALE = 0.7978845608028654
GELU_CUBE = 0.044715
F32 = jnp.float32
BF = jnp.bfloat16
W = ("shard", "context")
T = "tensor"
ROWS = 512
HALF = 256
PIECE = 64
D = 1024
NEG = -1e30


def spec(shape, index=None):
    place = tuple(index) if index is not None else (0,) * len(shape)
    return pl.BlockSpec(shape, lambda i: place)


def smem():
    return pl.BlockSpec(memory_space=pltpu.SMEM)


def call(body, name, operands, outs):
    in_specs, args = [], []
    for array, shape, index in operands:
        in_specs.append(smem() if shape is None else spec(shape, index))
        args.append(array)
    return pl.pallas_call(
        body,
        grid=(1,),
        in_specs=in_specs,
        out_specs=[spec(o.shape) for o in outs],
        out_shape=outs,
        compiler_params=pltpu.CompilerParams(vmem_limit_bytes=50 << 20),
        name=name,
    )(*args)


def sds(shape, dtype):
    return jax.ShapeDtypeStruct(shape, dtype)


def mm(a, b):
    return lax.dot_general(a, b, (((1,), (0,)), ((), ())), preferred_element_type=F32)


def mm_nt(a, b):
    return lax.dot_general(a, b, (((1,), (1,)), ((), ())), preferred_element_type=F32)


def mm_tn(a, b):
    return lax.dot_general(a, b, (((0,), (0,)), ((), ())), preferred_element_type=F32)


def core_swap(v):
    return lax.ppermute(v, T, [(i, i ^ 1) for i in range(8)])


def along_y(v, step):
    return lax.ppermute(
        v, T, [(2 * y + c, 2 * ((y + step) % 4) + c) for y in range(4) for c in range(2)]
    )


def add_body(pa, got, h0, h1, h2, h3):
    both = pa[...].astype(F32) + got[...].astype(F32)
    h0[...] = both[:PIECE]
    h1[...] = both[PIECE : 2 * PIECE].astype(BF)
    h2[...] = both[2 * PIECE : 3 * PIECE].astype(BF)
    h3[...] = both[3 * PIECE :].astype(BF)


def tie(*values):
    return lax.optimization_barrier(values)


def chip_sums(keep, send):
    got = core_swap(send)
    return call(
        add_body,
        "pair_add",
        [(keep, (HALF, D), None), (got, (HALF, D), None)],
        [sds((PIECE, D), F32)] + [sds((PIECE, D), BF)] * 3,
    )


def spread(sums):
    h0, h1, h2, h3 = sums
    r2 = along_y(h2, -2)
    r1 = along_y(h1, -1)
    r3 = along_y(h3, -3)
    return h0, r1, r2, r3


def sum_pieces(keep, send):
    return spread(chip_sums(keep, send))


def gather_rows(own):
    r2 = along_y(own, 2)
    r1 = along_y(own, 1)
    r3 = along_y(own, 3)
    near = jnp.concatenate([own, r1, r2, r3], axis=0)
    far = core_swap(near)
    return near, far


def norm_parts(v):
    mean = jnp.mean(v, axis=-1, keepdims=True)
    centred = v - mean
    var = jnp.mean(centred * centred, axis=-1, keepdims=True)
    s = lax.rsqrt(var + NORM_EPS)
    return centred * s, s


def gain_row(table, l, i):
    at = 2 * l + i
    return table[at : at + 1]


def bias_row(table, l, i):
    at = 4 + 4 * l + i
    return table[at : at + 1]


def norm_fwd(pieces, resid, table, bias_at, next_at):
    def body(h0, r1, r2, r3, resid_ref, rows, stream, normed):
        v = (
            h0[...] + r1[...].astype(F32) + r2[...].astype(F32) + r3[...].astype(F32)
        ) + resid_ref[...].astype(F32) + bias_row(rows, *bias_at)
        stream[...] = v
        xhat, _ = norm_parts(v)
        gain, shift = next_at
        normed[...] = (xhat * gain_row(rows, *gain) + bias_row(rows, *shift)).astype(BF)

    b = (PIECE, D)
    return call(
        body,
        "norm_fwd",
        [(p, b, None) for p in (*pieces, resid)] + [(table, (12, D), None)],
        [sds(b, F32), sds(b, BF)],
    )


def out_rows(pieces, resid, table):
    def body(h0, r1, r2, r3, resid_ref, rows, out):
        out[...] = (
            (h0[...] + r1[...].astype(F32) + r2[...].astype(F32) + r3[...].astype(F32))
            + resid_ref[...]
            + bias_row(rows, 1, 3)
        ).astype(BF)

    b = (PIECE, D)
    return call(
        body,
        "out_rows",
        [(p, b, None) for p in (*pieces, resid)] + [(table, (12, D), None)],
        [sds(b, BF)],
    )[0]


def norm_bwd(pieces, stream, grad, table, gain_at):
    def body(h0, r1, r2, r3, stream_ref, grad_ref, rows, out, low, sums):
        g = h0[...] + r1[...].astype(F32) + r2[...].astype(F32) + r3[...].astype(F32)
        xhat, s = norm_parts(stream_ref[...].astype(F32))
        gx = g * xhat
        c = g * gain_row(rows, *gain_at)
        cx = c * xhat
        e = grad_ref[...].astype(F32) + s * (
            c
            - jnp.mean(c, axis=-1, keepdims=True)
            - xhat * jnp.mean(cx, axis=-1, keepdims=True)
        )
        out[...] = e
        low[...] = e.astype(BF)
        sums[0:1] = jnp.sum(gx, axis=0, keepdims=True)
        sums[1:2] = jnp.sum(g, axis=0, keepdims=True)
        sums[2:3] = jnp.sum(e, axis=0, keepdims=True)

    b = (PIECE, D)
    return call(
        body,
        "norm_bwd",
        [(p, b, None) for p in (*pieces, stream, grad)] + [(table, (12, D), None)],
        [sds(b, F32), sds(b, BF), sds((3, D), F32)],
    )


def kv_first_body(xa, xb, first, rows, bias, na, nb, k, v):
    w = qkv_matrix(first)[:, 128:]
    for x, n, at in ((xa, na, 0), (xb, nb, HALF)):
        xhat, _ = norm_parts(x[...].astype(F32))
        normed = (xhat * gain_row(rows, 0, 0) + bias_row(rows, 0, 0)).astype(BF)
        n[...] = normed
        both = (mm(normed, w) + bias[:, 128:]).astype(BF)
        k[at : at + HALF] = both[:, :128]
        v[at : at + HALF] = both[:, 128:]


def kv_body(na, nb, w, bias, k, v):
    for n, at in ((na, 0), (nb, HALF)):
        both = (mm(n[...], w[:, 128:]) + bias[:, 128:]).astype(BF)
        k[at : at + HALF] = both[:, :128]
        v[at : at + HALF] = both[:, 128:]


def q_body(na, nb, w, bias, q):
    m = qkv_matrix(w)[:, :128]
    for n, at in ((na, 0), (nb, HALF)):
        q[at : at + HALF] = (mm(n[...], m) + bias[:, :128]).astype(BF)


def proj_matrix(ref):
    return ref[:, :64, 384:].reshape(D, 128) if len(ref.shape) == 3 else ref[...]


def qkv_matrix(ref):
    return ref[:, :64, :384].reshape(D, 384) if len(ref.shape) == 3 else ref[...]


def places(place, shape, axis):
    r = lax.broadcasted_iota(jnp.int32, shape, axis)
    y, c = place[0], place[1]
    return ((y - ((r >> 6) & 3)) & 3) * 128 + ((c + (r >> 8)) & 1) * 64 + (r & 63)


def own_scores(place, slope, h, qh, kh, mask):
    pos = places(place, (1, ROWS), 1).astype(F32)
    return jnp.where(mask, mm_nt(qh, kh) * 0.125 + slope[h] * pos, NEG)


def earlier_scores(place, slope, h, qh, kh):
    pos = places(place, (1, ROWS), 1).astype(F32)
    off = jnp.where(place[2] == 1, 0.0, NEG)
    return mm_nt(qh, kh) * 0.125 + (slope[h] * (pos - 512.0) + off)


def own_mask(place):
    return places(place, (ROWS, 1), 0) >= places(place, (1, ROWS), 1)


def attend_own_body(place, slope, q, k, v, out, top, total):
    mask = own_mask(place)
    for h in range(2):
        lo, hi = h * HD, (h + 1) * HD
        s = own_scores(place, slope, h, q[:, lo:hi], k[:, lo:hi], mask)
        m = jnp.max(s, axis=-1, keepdims=True)
        p = jnp.exp(s - m)
        out[:, lo:hi] = mm(p.astype(BF), v[:, lo:hi])
        top[:, lo:hi] = jnp.broadcast_to(m, (ROWS, HD))
        total[:, lo:hi] = jnp.broadcast_to(jnp.sum(p, axis=-1, keepdims=True), (ROWS, HD))


def attend_body(place, slope, q, ko, vo, pw, own, own_top, own_total, att, lse, pa, pb):
    outs, logs = [], []
    for h in range(2):
        lo, hi = h * HD, (h + 1) * HD
        s = earlier_scores(place, slope, h, q[:, lo:hi], ko[:, lo:hi])
        m = own_top[:, lo : lo + 1]
        top = jnp.maximum(m, jnp.max(s, axis=-1, keepdims=True))
        p = jnp.exp(s - top)
        scale = jnp.exp(m - top)
        total = own_total[:, lo : lo + 1] * scale + jnp.sum(p, axis=-1, keepdims=True)
        o = own[:, lo:hi] * scale + mm(p.astype(BF), vo[:, lo:hi])
        outs.append(o / total)
        logs.append(jnp.broadcast_to(top + jnp.log(total), (ROWS, HD)))
    attended = jnp.concatenate(outs, axis=1).astype(BF)
    att[...] = attended
    lse[...] = jnp.concatenate(logs, axis=1)
    w = proj_matrix(pw)
    pa[...] = mm_nt(attended[:HALF], w).astype(BF)
    pb[...] = mm_nt(attended[HALF:], w).astype(BF)


def score_grads(p, doh, vh, atth):
    delta = jnp.sum(doh.astype(F32) * atth.astype(F32), axis=-1, keepdims=True)
    return (p * (mm_nt(doh, vh) - delta)).astype(BF)


def back_earlier_body(place, slope, ma, mb, pw, q, ko, vo, lse, att, do_ref, dq, dko, dvo):
    w = proj_matrix(pw)
    do = jnp.concatenate([mm(ma[...], w), mm(mb[...], w)], axis=0).astype(BF)
    do_ref[...] = do
    dqs, dks, dvs = [], [], []
    for h in range(2):
        lo, hi = h * HD, (h + 1) * HD
        qh, kh, vh, doh = q[:, lo:hi], ko[:, lo:hi], vo[:, lo:hi], do[:, lo:hi]
        p = jnp.exp(earlier_scores(place, slope, h, qh, kh) - lse[:, lo : lo + 1])
        d = score_grads(p, doh, vh, att[:, lo:hi])
        dqs.append(mm(d, kh) * 0.125)
        dks.append(mm_tn(d, qh) * 0.125)
        dvs.append(mm_tn(p.astype(BF), doh))
    dq[...] = jnp.concatenate(dqs, axis=1)
    dko[...] = jnp.concatenate(dks, axis=1).astype(BF)
    dvo[...] = jnp.concatenate(dvs, axis=1).astype(BF)


def back_own_body(place, slope, do, q, k, v, lse, att, dq_part, dq, dkv):
    mask = own_mask(place)
    dqs, dks, dvs = [], [], []
    for h in range(2):
        lo, hi = h * HD, (h + 1) * HD
        qh, kh, vh, doh = q[:, lo:hi], k[:, lo:hi], v[:, lo:hi], do[:, lo:hi]
        p = jnp.exp(own_scores(place, slope, h, qh, kh, mask) - lse[:, lo : lo + 1])
        d = score_grads(p, doh, vh, att[:, lo:hi])
        dqs.append(mm(d, kh) * 0.125)
        dks.append(mm_tn(d, qh) * 0.125)
        dvs.append(mm_tn(p.astype(BF), doh))
    dq[...] = (dq_part[...] + jnp.concatenate(dqs, axis=1)).astype(BF)
    dkv[...] = jnp.concatenate(dks + dvs, axis=1)


def ffn_body(na, nb, w1, w2, bias, act, dgel, pa, pb):
    for n, p, at in ((na, pa, 0), (nb, pb, HALF)):
        v = mm(n[...], w1[...]) + bias[...]
        v2 = v * v
        th = jnp.tanh(GELU_SCALE * (v + GELU_CUBE * (v2 * v)))
        one = 0.5 + 0.5 * th
        a = (v * one).astype(BF)
        act[at : at + HALF] = a
        dgel[at : at + HALF] = (
            one
            + (0.5 * GELU_SCALE) * v * (1.0 - th * th) * (1.0 + (3.0 * GELU_CUBE) * v2)
        ).astype(BF)
        p[...] = mm_nt(a, w2[...]).astype(BF)


def ffn_back_body(ea, eb, w1, w2, dgel, hg, sums, pa, pb):
    total = jnp.zeros((1, 512), F32)
    for e, p, at in ((ea, pa, 0), (eb, pb, HALF)):
        g = (mm(e[...], w2[...]) * dgel[at : at + HALF].astype(F32)).astype(BF)
        hg[at : at + HALF] = g
        total += jnp.sum(g.astype(F32), axis=0, keepdims=True)
        p[...] = mm_nt(g, w1[...]).astype(BF)
    sums[...] = total


def ffn_weights_body(ea, eb, act, na, nb, hg, out):
    out[:, :512] = (mm_tn(na[...], hg[:HALF]) + mm_tn(nb[...], hg[HALF:])).astype(BF)
    out[:, 512:] = (mm_tn(ea[...], act[:HALF]) + mm_tn(eb[...], act[HALF:])).astype(BF)


def attn_weights_body(na, nb, joined, ma, mb, att, out):
    out[:, :384] = (
        mm_tn(na[...], joined[:HALF]) + mm_tn(nb[...], joined[HALF:])
    ).astype(BF)
    out[:, 384:] = (mm_tn(ma[...], att[:HALF]) + mm_tn(mb[...], att[HALF:])).astype(BF)


def two_halves(v):
    high = v.astype(BF)
    return high, (v - high.astype(F32)).astype(BF)


def last_pack_body(
    na, nb, joined, ma, mb, att, pa, pb, xa, xb, s21, s11, s20, b13,
    up0, up1, qv0, qv1, out,
):
    g = (mm_tn(na[...], joined[:HALF]) + mm_tn(nb[...], joined[HALF:])).astype(BF)
    out[:, :64, :384] = g.reshape(16, 64, 384)
    g = (mm_tn(ma[...], att[:HALF]) + mm_tn(mb[...], att[HALF:])).astype(BF)
    out[:, :64, 384:] = g.reshape(16, 64, 128)
    gain = jnp.zeros((1, D), F32)
    shift = jnp.zeros((1, D), F32)
    for p, x in ((pa, xa), (pb, xb)):
        g = p[...].astype(F32)
        xhat, _ = norm_parts(x[...].astype(F32))
        gain += jnp.sum(g * xhat, axis=0, keepdims=True)
        shift += jnp.sum(g, axis=0, keepdims=True)
    columns = jnp.concatenate(
        [
            gain, s20[0:1], s11[0:1], s21[0:1],
            shift, s20[2:3], s20[1:2], s11[2:3], s11[1:2], s21[2:3], s21[1:2], b13[...],
        ]
    ).astype(BF)
    q0, q0l = two_halves(qv0[...])
    q1, q1l = two_halves(qv1[...])
    u0, u0l = two_halves(up0[...])
    u1, u1l = two_halves(up1[...])
    none = jnp.zeros((1, 384), BF)
    lines = jnp.concatenate(
        [
            q0, q1, q0l, q1l,
            u0[:, :384], u1[:, :384], u0l[:, :384], u1l[:, :384],
            jnp.concatenate([u0[:, 384:], u1[:, 384:], none[:, :128]], axis=1),
            jnp.concatenate([u0l[:, 384:], u1l[:, 384:], none[:, :128]], axis=1),
            none, none,
        ]
    )
    for w in range(16):
        at = 128 * (w // 2)
        tail = jnp.concatenate([columns[:, at : at + 128], lines], axis=1)
        out[w, 64:80] = jnp.concatenate([tail, jnp.zeros((4, 512), BF)])


def qkv_back_body(dq, dkv, gotk, gotv, w, joined, sums, pa, pb):
    got = jnp.concatenate([gotk[...], gotv[...]], axis=1).astype(F32)
    j = jnp.concatenate([dq[...], (dkv[...] + got).astype(BF)], axis=1)
    joined[...] = j
    sums[...] = jnp.sum(j.astype(F32), axis=0, keepdims=True)
    m = qkv_matrix(w)
    pa[...] = mm_nt(j[:HALF], m).astype(BF)
    pb[...] = mm_nt(j[HALF:], m).astype(BF)


def by_kind(m):
    parts = [m[:, i * HD : (i + 1) * HD] for i in range(6)]
    return jnp.concatenate([parts[i] for i in (0, 3, 1, 4, 2, 5)], axis=1)


def by_head(m):
    parts = [m[:, i * HD : (i + 1) * HD] for i in range(6)]
    return jnp.concatenate([parts[i] for i in (0, 2, 4, 1, 3, 5)], axis=1)


def pack_first_body(qkv, proj, gains, biases, first):
    small = [gains[l, i : i + 1] for l in range(2) for i in range(2)]
    small += [biases[l, i : i + 1] for l in range(2) for i in range(4)]
    lines = jnp.concatenate(
        [jnp.concatenate([small[2 * i], small[2 * i + 1]], axis=1) for i in range(6)]
        + [jnp.zeros((2, 128), BF)]
    )
    own = jnp.concatenate(
        [
            jnp.concatenate([by_kind(qkv[0]), proj[0]], axis=1),
            jnp.concatenate([lines, jnp.zeros((8, 384), BF)], axis=1),
        ]
    )
    for w in range(16):
        first[w] = own


def pack_rest_body(qkv, proj, fc1, fc2, second, third):
    own = jnp.concatenate([by_kind(qkv[0]), proj[0]], axis=1)
    for w in range(16):
        second[w, :, :512] = fc1[0]
        second[w, :, 512:1024] = fc2[0]
        second[w, :, 1024:] = own
        third[w, :, :512] = fc1[1]
        third[w, :, 512:] = fc2[1]


def sum16(ref, *at):
    total = ref[(0, *at)].astype(F32)
    for w in range(1, 16):
        total += ref[(w, *at)].astype(F32)
    return total


def finish_ffn_body(f0, f1, a1, fc1, fc2, attn1):
    for l, f in enumerate((f0, f1)):
        total = sum16(f)
        fc1[l] = total[:, :512]
        fc2[l] = total[:, 512:]
    attn1[...] = sum16(a1)


def finish_columns_body(odd, mixed, columns):
    own = mixed[0, 64:80, :128].astype(F32)
    for w in range(1, 16):
        own += mixed[w, 64:80, :128].astype(F32)
    columns[...] = jnp.where(odd[0] == 1, own[:12, 64:], own[:12, :64])


def finish_body(mixed, attn1, qkv, proj, qv, up):
    total = sum16(mixed)
    for l, m in enumerate((total[:64], attn1[...])):
        qkv[l] = by_head(m[:, :384])
        proj[l] = m[:, 384:]
    own = total[64:76]
    for l in range(2):
        line = own[l : l + 1, 128:] + own[2 + l : 3 + l, 128:]
        parts = [line[:, i * HD : (i + 1) * HD] for i in (0, 4, 1, 5)]
        qv[l : l + 1] = jnp.concatenate(parts, axis=1)
        near = own[4 + l : 5 + l, 128:] + own[6 + l : 7 + l, 128:]
        at = 128 + 128 * l
        up[l : l + 1] = jnp.concatenate(
            [near, own[8:9, at : at + 128] + own[9:10, at : at + 128]], axis=1
        )


def finish_rows_body(t0, t1, t2, t3, gains, biases):
    total = (t0[...] + t1[...]) + (t2[...] + t3[...])
    for l in range(2):
        gains[l] = total[2 * l : 2 * l + 2]
        biases[l] = total[4 + 4 * l : 8 + 4 * l]


def relative_body(order, x, cot, xr, cr, total):
    for j in range(8):
        row = pl.multiple_of(order[j] * PIECE, PIECE)
        xr[j * PIECE : (j + 1) * PIECE] = x[pl.ds(row, PIECE)]
        cr[j * PIECE : (j + 1) * PIECE] = cot[pl.ds(row, PIECE)]
    total[...] = jnp.sum(cr[:PIECE].astype(F32), axis=0, keepdims=True)


def sequence_body(order, near, far, out):
    for j in range(8):
        row = pl.multiple_of(order[j] * PIECE, PIECE)
        src = near if j < 4 else far
        k = j % 4
        out[pl.ds(row, PIECE)] = src[k * PIECE : (k + 1) * PIECE].astype(out.dtype)


def per_device(
    block_in, qkv_weight, proj_weight, fc1_weight, fc2_weight,
    qv_bias, fc1_bias, norm_gains, row_biases, cotangent,
):
    t = lax.axis_index(T)
    y, c = t // 2, t % 2
    ctx = lax.axis_index("context")
    place = jnp.stack([y, c, ctx]).astype(jnp.int32)
    slope = jnp.exp2(-8.0 * (2 * t + 1 + jnp.arange(2)).astype(F32) / HEADS)
    j = jnp.arange(8)
    order = (2 * ((y - j % 4) % 4) + (c + j // 4) % 2).astype(jnp.int32)
    half = (HALF, D)
    qs, kvs, hs, js = (ROWS, 128), (ROWS, 256), (ROWS, 512), (ROWS, 384)

    layer = (1, 64, 384), (1, 64, 128)
    (first,) = call(
        pack_first_body, "pack_first",
        [(qkv_weight, layer[0], (0, 0, 0)), (proj_weight, layer[1], (0, 0, 0)),
         (norm_gains, (2, 2, 64), None), (row_biases, (2, 4, 64), None)],
        [sds((16, 72, 512), BF)],
    )
    first_all = lax.all_to_all(first, W, 0, 0)
    second_part, third_part = call(
        pack_rest_body, "pack_rest",
        [(qkv_weight, layer[0], (1, 0, 0)), (proj_weight, layer[1], (1, 0, 0)),
         (fc1_weight, (2, 64, 512), None), (fc2_weight, (2, 64, 512), None)],
        [sds((16, 64, 1536), BF), sds((16, 64, D), BF)],
    )
    table = (
        first_all[:, 64:70, :128].reshape(16, 12, 64).transpose(1, 0, 2).reshape(12, D).astype(F32)
    )
    tab = (table, (12, D), None)
    whole_first = (first_all, (16, 72, 512), None)
    qv = qv_bias.astype(F32).reshape(2, 2, 2, HD).transpose(0, 2, 1, 3)
    zero = jnp.zeros((2, 1, 2, HD), F32)
    joined_bias = jnp.concatenate([qv[:, :1], zero, qv[:, 1:]], axis=1).reshape(2, 1, 384)
    up_bias = fc1_bias.astype(F32).reshape(2, 1, 512)

    x, cot, b13 = call(
        relative_body, "to_relative",
        [(order, None, None), (block_in.reshape(ROWS, D), (ROWS, D), None), (cotangent.reshape(ROWS, D), (ROWS, D), None)],
        [sds((ROWS, D), BF), sds((ROWS, D), BF), sds((1, D), F32)],
    )

    saved = []
    stream = x
    qkv_of, proj_of = [whole_first, None], [whole_first, None]
    fc1_of, fc2_of = [None, None], [None, None]

    def set_ffn(l, m):
        fc1_of[l], fc2_of[l] = (m, (D, 512), (0, 0)), (m, (D, 512), (0, 1))

    where = [(place, None, None), (slope, None, None)]
    for l in range(2):
        bias = (joined_bias[l], (1, 384), None)
        if l == 0:
            na, nb, k, v = call(
                kv_first_body, "kv_first",
                [(x, half, (0, 0)), (x, half, (1, 0)), whole_first, tab, bias],
                [sds(half, BF), sds(half, BF), sds(qs, BF), sds(qs, BF)],
            )
        else:
            na, nb = gather_rows(normed)
            k, v = call(
                kv_body, "kv", [(na, half, None), (nb, half, None), qkv_of[l], bias], [sds(qs, BF), sds(qs, BF)]
            )
        ko = lax.ppermute(k, "context", [(0, 1)])
        vo = lax.ppermute(v, "context", [(0, 1)])
        (q,) = call(
            q_body, "q", [(na, half, None), (nb, half, None), qkv_of[l], bias], [sds(qs, BF)]
        )
        own, own_top, own_total = call(
            attend_own_body, "attend_own", where + [(q, qs, None), (k, qs, None), (v, qs, None)], [sds(qs, F32)] * 3
        )
        if l == 0:
            ko, part = tie(ko, second_part)
            arrived = lax.all_to_all(part, W, 0, 0).reshape(D, 1536)
            set_ffn(0, arrived)
            qkv_of[1], proj_of[1] = (arrived[:, 1024:1408], (D, 384), None), (arrived, (D, 128), (0, 11))
        else:
            ko, part = tie(ko, third_part)
            set_ffn(1, lax.all_to_all(part, W, 0, 0).reshape(D, D))
        att, lse, pa, pb = call(
            attend_body, "attend",
            where + [(q, qs, None), (ko, qs, None), (vo, qs, None), proj_of[l]] + [(v, qs, None) for v in (own, own_top, own_total)],
            [sds(qs, BF), sds(qs, F32), sds(half, BF), sds(half, BF)],
        )
        middle, second = norm_fwd(
            sum_pieces(pa, pb), stream, table, (l, 1), ((l, 1), (l, 2))
        )
        sa, sb = gather_rows(second)
        act, dgel, pa, pb = call(
            ffn_body, "ffn",
            [(sa, half, None), (sb, half, None), fc1_of[l], fc2_of[l], (up_bias[l], (1, 512), None)],
            [sds(hs, BF), sds(hs, BF), sds(half, BF), sds(half, BF)],
        )
        saved.append((stream, na, nb, q, k, v, ko, vo, att, lse, middle, sa, sb, act, dgel))
        if l == 0:
            stream, normed = norm_fwd(
                sum_pieces(pa, pb), middle, table, (0, 3), ((1, 0), (1, 0))
            )
    out_own = out_rows(sum_pieces(pa, pb), middle, table)

    grad = cot
    ea = (cot, half, (0, 0))
    eb = (cot, half, (1, 0))
    for l in (1, 0):
        stream, na, nb, q, k, v, ko, vo, att, lse, middle, sa, sb, act, dgel = saved[l]
        hg, up_sum, pa, pb = call(
            ffn_back_body, "ffn_back",
            [ea, eb, fc1_of[l], fc2_of[l], (dgel, hs, None)],
            [sds(hs, BF), sds((1, 512), F32), sds(half, BF), sds(half, BF)],
        )
        pieces = sum_pieces(pa, pb)
        (ffn_grad,) = call(
            ffn_weights_body, "ffn_weights",
            [ea, eb, (act, hs, None), (sa, half, None), (sb, half, None), (hg, hs, None)],
            [sds((D, D), BF)],
        )
        if l == 1:
            pieces, ffn_grad, out_own = tie(pieces, ffn_grad, out_own)
        else:
            pieces, ffn_grad, attn_pieces1 = tie(pieces, ffn_grad, attn_pieces1)
        mid, mid_low, s2 = norm_bwd(pieces, middle, grad, table, (l, 1))
        ma, mb = gather_rows(mid_low)
        do, dq, dko, dvo = call(
            back_earlier_body, "back_earlier",
            where
            + [(ma, half, None), (mb, half, None), proj_of[l], (q, qs, None), (ko, qs, None), (vo, qs, None), (lse, qs, None), (att, qs, None)],
            [sds(qs, BF), sds(qs, F32), sds(qs, BF), sds(qs, BF)],
        )
        gotk = lax.ppermute(dko, "context", [(1, 0)])
        gotv = lax.ppermute(dvo, "context", [(1, 0)])
        dq, dkv = call(
            back_own_body, "back_own",
            where
            + [(do, qs, None), (q, qs, None), (k, qs, None), (v, qs, None), (lse, qs, None), (att, qs, None), (dq, qs, None)],
            [sds(qs, BF), sds(kvs, F32)],
        )
        gotk, ffn_grad = tie(gotk, ffn_grad)
        ffn_pieces = lax.all_to_all(ffn_grad.reshape(16, 64, D), W, 0, 0)
        if l == 1:
            dkv, out_own = tie(dkv, out_own)
            oa, ob = gather_rows(out_own)
        joined, qv_sum, pa, pb = call(
            qkv_back_body, "qkv_back",
            [(dq, qs, None), (dkv, kvs, None), (gotk, qs, None), (gotv, qs, None), qkv_of[l]],
            [sds(js, BF), sds((1, 384), F32), sds(half, BF), sds(half, BF)],
        )
        pieces = sum_pieces(pa, pb)
        attn_ops = [(na, half, None), (nb, half, None), (joined, js, None), (ma, half, None), (mb, half, None), (att, qs, None)]
        if l == 1:
            (attn_grad,) = call(attn_weights_body, "attn_weights", attn_ops, [sds((D, 512), BF)])
            pieces, attn_grad, oa = tie(pieces, attn_grad, oa)
            up1, qv1, s21, ffn_pieces1 = up_sum, qv_sum, s2, ffn_pieces
            grad, low, s11 = norm_bwd(pieces, stream, mid, table, (1, 0))
            near, far = gather_rows(low)
            near, attn_grad, ffn_pieces1 = tie(near, attn_grad, ffn_pieces1)
            attn_pieces1 = lax.all_to_all(attn_grad.reshape(16, 64, 512), W, 0, 0)
            ea, eb = (near, half, None), (far, half, None)
        else:
            three, one = (3, D), (1, D)
            (packed,) = call(
                last_pack_body, "last_pack",
                attn_ops
                + [(pa, half, None), (pb, half, None), (x, half, (0, 0)), (x, half, (1, 0))]
                + [(s21, three, None), (s11, three, None), (s2, three, None), (b13, one, None)]
                + [(up_sum, (1, 512), None), (up1, (1, 512), None), (qv_sum, (1, 384), None), (qv1, (1, 384), None)],
                [sds((16, 80, 512), BF)],
            )
            packed, ffn_pieces = tie(packed, ffn_pieces)
            mixed = lax.all_to_all(packed, W, 0, 0)
            _, low, _ = norm_bwd(pieces, stream, mid, table, (0, 0))
            near, far = gather_rows(low)
            near, f0 = tie(near, ffn_pieces)
            fc1_grad, fc2_grad, attn1_grad = call(
                finish_ffn_body, "finish_ffn",
                [(f0, (16, 64, D), None), (ffn_pieces1, (16, 64, D), None), (attn_pieces1, (16, 64, 512), None)],
                [sds((2, 64, 512), F32), sds((2, 64, 512), F32), sds((64, 512), F32)],
            )
            (block_out,) = call(
                sequence_body, "to_sequence",
                [(order, None, None), (oa, half, None), (ob, half, None)],
                [sds((ROWS, D), BF)],
            )
            (input_grad,) = call(
                sequence_body, "to_sequence",
                [(order, None, None), (near, half, None), (far, half, None)],
                [sds((ROWS, D), F32)],
            )
    odd = ctx.astype(jnp.int32).reshape(1)
    small = (12, 64)
    (tail,) = call(
        finish_columns_body, "finish_columns",
        [(odd, None, None), (mixed, (16, 80, 512), None)],
        [sds(small, F32)],
    )
    tail = tail + core_swap(tail)
    tails = [tail] + [along_y(tail, step) for step in (1, 2, 3)]
    qkv_grad, proj_grad, qv_grad, up_grad = call(
        finish_body, "finish",
        [(mixed, (16, 80, 512), None), (attn1_grad, (64, 512), None)],
        [sds((2, 64, 384), F32), sds((2, 64, 128), F32), sds((2, 256), F32), sds((2, 512), F32)],
    )
    gains_grad, biases_grad = call(
        finish_rows_body, "finish_rows",
        [(v, small, None) for v in tails],
        [sds((2, 2, 64), F32), sds((2, 4, 64), F32)],
    )
    return (
        block_out[None], input_grad[None], qkv_grad, proj_grad, fc1_grad, fc2_grad,
        qv_grad, up_grad, gains_grad, biases_grad,
    )


def solution(mesh):
    return jax.shard_map(
        per_device,
        mesh=mesh,
        in_specs=(
            P("shard", "context", None),
            P(None, W, T),
            P(None, W, T),
            P(None, W, T),
            P(None, W, T),
            P(None, T),
            P(None, T),
            P(None, None, W),
            P(None, None, W),
            P("shard", "context", None),
        ),
        out_specs=(
            P("shard", "context", None),
            P("shard", "context", None),
            P(None, W, T),
            P(None, W, T),
            P(None, W, T),
            P(None, W, T),
            P(None, T),
            P(None, T),
            P(None, None, W),
            P(None, None, W),
        ),
        check_vma=False,
    )
```

```python
import jax
import jax.numpy as jnp
from jax import lax
from jax.experimental import pallas as pl
from jax.experimental.pallas import tpu as pltpu
from jax.sharding import PartitionSpec as P

HEADS = 16
HD = 64
NORM_EPS = 1e-05
GELU_SCALE = 0.7978845608028654
GELU_CUBE = 0.044715
F32 = jnp.float32
BF = jnp.bfloat16
W = ("shard", "context")
T = "tensor"
ROWS = 512
HALF = 256
PIECE = 64
D = 1024
NEG = -1e30


def spec(shape, index=None):
    place = tuple(index) if index is not None else (0,) * len(shape)
    return pl.BlockSpec(shape, lambda i: place)


def smem():
    return pl.BlockSpec(memory_space=pltpu.SMEM)


def call(body, name, operands, outs):
    in_specs, args = [], []
    for array, shape, index in operands:
        in_specs.append(smem() if shape is None else spec(shape, index))
        args.append(array)
    return pl.pallas_call(
        body,
        grid=(1,),
        in_specs=in_specs,
        out_specs=[spec(o.shape) for o in outs],
        out_shape=outs,
        compiler_params=pltpu.CompilerParams(vmem_limit_bytes=50 << 20),
        name=name,
    )(*args)


def sds(shape, dtype):
    return jax.ShapeDtypeStruct(shape, dtype)


def mm(a, b):
    return lax.dot_general(a, b, (((1,), (0,)), ((), ())), preferred_element_type=F32)


def mm_nt(a, b):
    return lax.dot_general(a, b, (((1,), (1,)), ((), ())), preferred_element_type=F32)


def mm_tn(a, b):
    return lax.dot_general(a, b, (((0,), (0,)), ((), ())), preferred_element_type=F32)


def core_swap(v):
    return lax.ppermute(v, T, [(i, i ^ 1) for i in range(8)])


def along_y(v, step):
    return lax.ppermute(
        v, T, [(2 * y + c, 2 * ((y + step) % 4) + c) for y in range(4) for c in range(2)]
    )


def add_body(pa, got, h0, h1, h2, h3):
    both = pa[...].astype(F32) + got[...].astype(F32)
    h0[...] = both[:PIECE]
    h1[...] = both[PIECE : 2 * PIECE].astype(BF)
    h2[...] = both[2 * PIECE : 3 * PIECE].astype(BF)
    h3[...] = both[3 * PIECE :].astype(BF)


def tie(*values):
    return lax.optimization_barrier(values)


def chip_sums(keep, send):
    got = core_swap(send)
    return call(
        add_body,
        "pair_add",
        [(keep, (HALF, D), None), (got, (HALF, D), None)],
        [sds((PIECE, D), F32)] + [sds((PIECE, D), BF)] * 3,
    )


def spread(sums):
    h0, h1, h2, h3 = sums
    r2 = along_y(h2, -2)
    r1 = along_y(h1, -1)
    r3 = along_y(h3, -3)
    return h0, r1, r2, r3


def sum_pieces(keep, send):
    return spread(chip_sums(keep, send))


def gather_rows(own):
    r2 = along_y(own, 2)
    r1 = along_y(own, 1)
    r3 = along_y(own, 3)
    near = jnp.concatenate([own, r1, r2, r3], axis=0)
    far = core_swap(near)
    return near, far


def norm_parts(v):
    mean = jnp.mean(v, axis=-1, keepdims=True)
    centred = v - mean
    var = jnp.mean(centred * centred, axis=-1, keepdims=True)
    s = lax.rsqrt(var + NORM_EPS)
    return centred * s, s


def gain_row(table, l, i):
    at = 2 * l + i
    return table[at : at + 1]


def bias_row(table, l, i):
    at = 4 + 4 * l + i
    return table[at : at + 1]


def norm_fwd(pieces, resid, table, bias_at, next_at):
    def body(h0, r1, r2, r3, resid_ref, rows, stream, normed):
        v = (
            h0[...] + r1[...].astype(F32) + r2[...].astype(F32) + r3[...].astype(F32)
        ) + resid_ref[...].astype(F32) + bias_row(rows, *bias_at)
        stream[...] = v
        xhat, _ = norm_parts(v)
        gain, shift = next_at
        normed[...] = (xhat * gain_row(rows, *gain) + bias_row(rows, *shift)).astype(BF)

    b = (PIECE, D)
    return call(
        body,
        "norm_fwd",
        [(p, b, None) for p in (*pieces, resid)] + [(table, (12, D), None)],
        [sds(b, F32), sds(b, BF)],
    )


def out_rows(pieces, resid, table):
    def body(h0, r1, r2, r3, resid_ref, rows, out):
        out[...] = (
            (h0[...] + r1[...].astype(F32) + r2[...].astype(F32) + r3[...].astype(F32))
            + resid_ref[...]
            + bias_row(rows, 1, 3)
        ).astype(BF)

    b = (PIECE, D)
    return call(
        body,
        "out_rows",
        [(p, b, None) for p in (*pieces, resid)] + [(table, (12, D), None)],
        [sds(b, BF)],
    )[0]


def norm_bwd(pieces, stream, grad, table, gain_at):
    def body(h0, r1, r2, r3, stream_ref, grad_ref, rows, out, low, sums):
        g = h0[...] + r1[...].astype(F32) + r2[...].astype(F32) + r3[...].astype(F32)
        xhat, s = norm_parts(stream_ref[...].astype(F32))
        gx = g * xhat
        c = g * gain_row(rows, *gain_at)
        cx = c * xhat
        e = grad_ref[...].astype(F32) + s * (
            c
            - jnp.mean(c, axis=-1, keepdims=True)
            - xhat * jnp.mean(cx, axis=-1, keepdims=True)
        )
        out[...] = e
        low[...] = e.astype(BF)
        sums[0:1] = jnp.sum(gx, axis=0, keepdims=True)
        sums[1:2] = jnp.sum(g, axis=0, keepdims=True)
        sums[2:3] = jnp.sum(e, axis=0, keepdims=True)

    b = (PIECE, D)
    return call(
        body,
        "norm_bwd",
        [(p, b, None) for p in (*pieces, stream, grad)] + [(table, (12, D), None)],
        [sds(b, F32), sds(b, BF), sds((3, D), F32)],
    )


def kv_first_body(xa, xb, first, rows, bias, na, nb, kv):
    w = qkv_matrix(first)[:, 128:]
    for x, n, at in ((xa, na, 0), (xb, nb, HALF)):
        xhat, _ = norm_parts(x[...].astype(F32))
        normed = (xhat * gain_row(rows, 0, 0) + bias_row(rows, 0, 0)).astype(BF)
        n[...] = normed
        kv[at : at + HALF] = (mm(normed, w) + bias[:, 128:]).astype(BF)


def kv_body(na, nb, w, bias, kv):
    for n, at in ((na, 0), (nb, HALF)):
        kv[at : at + HALF] = (mm(n[...], w[:, 128:]) + bias[:, 128:]).astype(BF)


def q_body(na, nb, w, bias, q):
    m = qkv_matrix(w)[:, :128]
    for n, at in ((na, 0), (nb, HALF)):
        q[at : at + HALF] = (mm(n[...], m) + bias[:, :128]).astype(BF)


def proj_matrix(ref):
    return ref[:, :64, 384:].reshape(D, 128) if len(ref.shape) == 3 else ref[...]


def qkv_matrix(ref):
    return ref[:, :64, :384].reshape(D, 384) if len(ref.shape) == 3 else ref[...]


def places(place, shape, axis):
    r = lax.broadcasted_iota(jnp.int32, shape, axis)
    y, c = place[0], place[1]
    return ((y - ((r >> 6) & 3)) & 3) * 128 + ((c + (r >> 8)) & 1) * 64 + (r & 63)


def own_scores(place, slope, h, qh, kh, mask):
    pos = places(place, (1, ROWS), 1).astype(F32)
    return jnp.where(mask, mm_nt(qh, kh) * 0.125 + slope[h] * pos, NEG)


def earlier_scores(place, slope, h, qh, kh):
    pos = places(place, (1, ROWS), 1).astype(F32)
    off = jnp.where(place[2] == 1, 0.0, NEG)
    return mm_nt(qh, kh) * 0.125 + (slope[h] * (pos - 512.0) + off)


def own_mask(place):
    return places(place, (ROWS, 1), 0) >= places(place, (1, ROWS), 1)


def attend_own_body(place, slope, q, kv, out, top, total):
    mask = own_mask(place)
    for h in range(2):
        lo, hi = h * HD, (h + 1) * HD
        s = own_scores(place, slope, h, q[:, lo:hi], kv[:, lo:hi], mask)
        m = jnp.max(s, axis=-1, keepdims=True)
        p = jnp.exp(s - m)
        out[:, lo:hi] = mm(p.astype(BF), kv[:, 128 + lo : 128 + hi])
        top[:, lo:hi] = jnp.broadcast_to(m, (ROWS, HD))
        total[:, lo:hi] = jnp.broadcast_to(jnp.sum(p, axis=-1, keepdims=True), (ROWS, HD))


def attend_body(place, slope, q, kvo, pw, own, own_top, own_total, att, lse, pa, pb):
    outs, logs = [], []
    for h in range(2):
        lo, hi = h * HD, (h + 1) * HD
        s = earlier_scores(place, slope, h, q[:, lo:hi], kvo[:, lo:hi])
        m = own_top[:, lo : lo + 1]
        top = jnp.maximum(m, jnp.max(s, axis=-1, keepdims=True))
        p = jnp.exp(s - top)
        scale = jnp.exp(m - top)
        total = own_total[:, lo : lo + 1] * scale + jnp.sum(p, axis=-1, keepdims=True)
        o = own[:, lo:hi] * scale + mm(p.astype(BF), kvo[:, 128 + lo : 128 + hi])
        outs.append(o / total)
        logs.append(jnp.broadcast_to(top + jnp.log(total), (ROWS, HD)))
    attended = jnp.concatenate(outs, axis=1).astype(BF)
    att[...] = attended
    lse[...] = jnp.concatenate(logs, axis=1)
    w = proj_matrix(pw)
    pa[...] = mm_nt(attended[:HALF], w).astype(BF)
    pb[...] = mm_nt(attended[HALF:], w).astype(BF)


def score_grads(p, doh, vh, atth):
    delta = jnp.sum(doh.astype(F32) * atth.astype(F32), axis=-1, keepdims=True)
    return (p * (mm_nt(doh, vh) - delta)).astype(BF)


def back_earlier_body(place, slope, ma, mb, pw, q, kvo, lse, att, do_ref, dq, dkvo):
    w = proj_matrix(pw)
    do = jnp.concatenate([mm(ma[...], w), mm(mb[...], w)], axis=0).astype(BF)
    do_ref[...] = do
    dqs, dks, dvs = [], [], []
    for h in range(2):
        lo, hi = h * HD, (h + 1) * HD
        qh, kh, vh, doh = q[:, lo:hi], kvo[:, lo:hi], kvo[:, 128 + lo : 128 + hi], do[:, lo:hi]
        p = jnp.exp(earlier_scores(place, slope, h, qh, kh) - lse[:, lo : lo + 1])
        d = score_grads(p, doh, vh, att[:, lo:hi])
        dqs.append(mm(d, kh) * 0.125)
        dks.append(mm_tn(d, qh) * 0.125)
        dvs.append(mm_tn(p.astype(BF), doh))
    dq[...] = jnp.concatenate(dqs, axis=1)
    dkvo[...] = jnp.concatenate(dks + dvs, axis=1).astype(BF)


def back_own_body(place, slope, do, q, kv, lse, att, dq_part, dq, dkv):
    mask = own_mask(place)
    dqs, dks, dvs = [], [], []
    for h in range(2):
        lo, hi = h * HD, (h + 1) * HD
        qh, kh, vh, doh = q[:, lo:hi], kv[:, lo:hi], kv[:, 128 + lo : 128 + hi], do[:, lo:hi]
        p = jnp.exp(own_scores(place, slope, h, qh, kh, mask) - lse[:, lo : lo + 1])
        d = score_grads(p, doh, vh, att[:, lo:hi])
        dqs.append(mm(d, kh) * 0.125)
        dks.append(mm_tn(d, qh) * 0.125)
        dvs.append(mm_tn(p.astype(BF), doh))
    dq[...] = (dq_part[...] + jnp.concatenate(dqs, axis=1)).astype(BF)
    dkv[...] = jnp.concatenate(dks + dvs, axis=1)


def ffn_body(na, nb, w1, w2, bias, act, dgel, pa, pb):
    for n, p, at in ((na, pa, 0), (nb, pb, HALF)):
        v = mm(n[...], w1[...]) + bias[...]
        v2 = v * v
        th = jnp.tanh(GELU_SCALE * (v + GELU_CUBE * (v2 * v)))
        one = 0.5 + 0.5 * th
        a = (v * one).astype(BF)
        act[at : at + HALF] = a
        dgel[at : at + HALF] = (
            one
            + (0.5 * GELU_SCALE) * v * (1.0 - th * th) * (1.0 + (3.0 * GELU_CUBE) * v2)
        ).astype(BF)
        p[...] = mm_nt(a, w2[...]).astype(BF)


def ffn_back_body(ea, eb, w1, w2, dgel, hg, sums, pa, pb):
    total = jnp.zeros((1, 512), F32)
    for e, p, at in ((ea, pa, 0), (eb, pb, HALF)):
        g = (mm(e[...], w2[...]) * dgel[at : at + HALF].astype(F32)).astype(BF)
        hg[at : at + HALF] = g
        total += jnp.sum(g.astype(F32), axis=0, keepdims=True)
        p[...] = mm_nt(g, w1[...]).astype(BF)
    sums[...] = total


def ffn_weights_body(ea, eb, act, na, nb, hg, out):
    out[:, :512] = (mm_tn(na[...], hg[:HALF]) + mm_tn(nb[...], hg[HALF:])).astype(BF)
    out[:, 512:] = (mm_tn(ea[...], act[:HALF]) + mm_tn(eb[...], act[HALF:])).astype(BF)


def attn_weights_body(na, nb, joined, ma, mb, att, out):
    out[:, :384] = (
        mm_tn(na[...], joined[:HALF]) + mm_tn(nb[...], joined[HALF:])
    ).astype(BF)
    out[:, 384:] = (mm_tn(ma[...], att[:HALF]) + mm_tn(mb[...], att[HALF:])).astype(BF)


def mixed_weights_body(ea, eb, act, sa, sb, hg, na, nb, joined, ma, mb, att, out):
    ffn_weights_body(ea, eb, act, sa, sb, hg, out.at[:, :1024])
    attn_weights_body(na, nb, joined, ma, mb, att, out.at[:, 1024:])


def two_halves(v):
    high = v.astype(BF)
    return high, (v - high.astype(F32)).astype(BF)


def last_pack_body(
    na, nb, joined, ma, mb, att, pa, pb, xa, xb, s21, s11, s20, b13,
    up0, up1, qv0, qv1, out,
):
    g = (mm_tn(na[...], joined[:HALF]) + mm_tn(nb[...], joined[HALF:])).astype(BF)
    out[:, :64, :384] = g.reshape(16, 64, 384)
    g = (mm_tn(ma[...], att[:HALF]) + mm_tn(mb[...], att[HALF:])).astype(BF)
    out[:, :64, 384:] = g.reshape(16, 64, 128)
    gain = jnp.zeros((1, D), F32)
    shift = jnp.zeros((1, D), F32)
    for p, x in ((pa, xa), (pb, xb)):
        g = p[...].astype(F32)
        xhat, _ = norm_parts(x[...].astype(F32))
        gain += jnp.sum(g * xhat, axis=0, keepdims=True)
        shift += jnp.sum(g, axis=0, keepdims=True)
    columns = jnp.concatenate(
        [
            gain, s20[0:1], s11[0:1], s21[0:1],
            shift, s20[2:3], s20[1:2], s11[2:3], s11[1:2], s21[2:3], s21[1:2], b13[...],
        ]
    ).astype(BF)
    q0, q0l = two_halves(qv0[...])
    q1, q1l = two_halves(qv1[...])
    u0, u0l = two_halves(up0[...])
    u1, u1l = two_halves(up1[...])
    none = jnp.zeros((1, 384), BF)
    lines = jnp.concatenate(
        [
            q0, q1, q0l, q1l,
            u0[:, :384], u1[:, :384], u0l[:, :384], u1l[:, :384],
            jnp.concatenate([u0[:, 384:], u1[:, 384:], none[:, :128]], axis=1),
            jnp.concatenate([u0l[:, 384:], u1l[:, 384:], none[:, :128]], axis=1),
            none, none,
        ]
    )
    for w in range(16):
        at = 128 * (w // 2)
        tail = jnp.concatenate([columns[:, at : at + 128], lines], axis=1)
        out[w, 64:80] = jnp.concatenate([tail, jnp.zeros((4, 512), BF)])


def qkv_back_body(dq, dkv, got, w, joined, sums, pa, pb):
    j = jnp.concatenate(
        [dq[...], (dkv[...] + got[...].astype(F32)).astype(BF)], axis=1
    )
    joined[...] = j
    sums[...] = jnp.sum(j.astype(F32), axis=0, keepdims=True)
    m = qkv_matrix(w)
    pa[...] = mm_nt(j[:HALF], m).astype(BF)
    pb[...] = mm_nt(j[HALF:], m).astype(BF)


def by_kind(m):
    parts = [m[:, i * HD : (i + 1) * HD] for i in range(6)]
    return jnp.concatenate([parts[i] for i in (0, 3, 1, 4, 2, 5)], axis=1)


def by_head(m):
    parts = [m[:, i * HD : (i + 1) * HD] for i in range(6)]
    return jnp.concatenate([parts[i] for i in (0, 2, 4, 1, 3, 5)], axis=1)


def pack_first_body(qkv, proj, gains, biases, first):
    small = [gains[l, i : i + 1] for l in range(2) for i in range(2)]
    small += [biases[l, i : i + 1] for l in range(2) for i in range(4)]
    lines = jnp.concatenate(
        [jnp.concatenate([small[2 * i], small[2 * i + 1]], axis=1) for i in range(6)]
        + [jnp.zeros((2, 128), BF)]
    )
    own = jnp.concatenate(
        [
            jnp.concatenate([by_kind(qkv[0]), proj[0]], axis=1),
            jnp.concatenate([lines, jnp.zeros((8, 384), BF)], axis=1),
        ]
    )
    for w in range(16):
        first[w] = own


def pack_rest_body(qkv, proj, fc1, fc2, second, third):
    second[:, :512] = fc1[0]
    second[:, 512:1024] = fc2[0]
    second[:, 1024:1152] = jnp.zeros((64, 128), BF)
    second[:, 1152:] = by_kind(qkv[0])
    third[:, :512] = fc1[1]
    third[:, 512:1024] = fc2[1]
    third[:, 1024:] = proj[0]


def sum16(ref, *at):
    total = ref[(0, *at)].astype(F32)
    for w in range(1, 16):
        total += ref[(w, *at)].astype(F32)
    return total


def finish_ffn_body(f0, f1, fc1, fc2):
    for l, f in enumerate((f0, f1)):
        fc1[l] = f[:, :512].astype(F32)
        fc2[l] = f[:, 512:1024].astype(F32)


def finish_columns_body(odd, mixed, columns):
    own = mixed[0, 64:80, :128].astype(F32)
    for w in range(1, 16):
        own += mixed[w, 64:80, :128].astype(F32)
    columns[...] = jnp.where(odd[0] == 1, own[:12, 64:], own[:12, :64])


def finish_body(mixed, attn1, qkv, proj, qv, up):
    total = sum16(mixed)
    for l, m in enumerate((total[:64], attn1[...].astype(F32))):
        qkv[l] = by_head(m[:, :384])
        proj[l] = m[:, 384:]
    own = total[64:76]
    for l in range(2):
        line = own[l : l + 1, 128:] + own[2 + l : 3 + l, 128:]
        parts = [line[:, i * HD : (i + 1) * HD] for i in (0, 4, 1, 5)]
        qv[l : l + 1] = jnp.concatenate(parts, axis=1)
        near = own[4 + l : 5 + l, 128:] + own[6 + l : 7 + l, 128:]
        at = 128 + 128 * l
        up[l : l + 1] = jnp.concatenate(
            [near, own[8:9, at : at + 128] + own[9:10, at : at + 128]], axis=1
        )


def finish_rows_body(t0, t1, t2, t3, gains, biases):
    total = (t0[...] + t1[...]) + (t2[...] + t3[...])
    for l in range(2):
        gains[l] = total[2 * l : 2 * l + 2]
        biases[l] = total[4 + 4 * l : 8 + 4 * l]


def relative_body(order, x, cot, xr, cr, total):
    for j in range(8):
        row = pl.multiple_of(order[j] * PIECE, PIECE)
        xr[j * PIECE : (j + 1) * PIECE] = x[pl.ds(row, PIECE)]
        cr[j * PIECE : (j + 1) * PIECE] = cot[pl.ds(row, PIECE)]
    total[...] = jnp.sum(cr[:PIECE].astype(F32), axis=0, keepdims=True)


def sequence_body(order, near, far, out):
    for j in range(8):
        row = pl.multiple_of(order[j] * PIECE, PIECE)
        src = near if j < 4 else far
        k = j % 4
        out[pl.ds(row, PIECE)] = src[k * PIECE : (k + 1) * PIECE].astype(out.dtype)


def per_device(
    block_in, qkv_weight, proj_weight, fc1_weight, fc2_weight,
    qv_bias, fc1_bias, norm_gains, row_biases, cotangent,
):
    t = lax.axis_index(T)
    y, c = t // 2, t % 2
    ctx = lax.axis_index("context")
    place = jnp.stack([y, c, ctx]).astype(jnp.int32)
    slope = jnp.exp2(-8.0 * (2 * t + 1 + jnp.arange(2)).astype(F32) / HEADS)
    j = jnp.arange(8)
    order = (2 * ((y - j % 4) % 4) + (c + j // 4) % 2).astype(jnp.int32)
    half = (HALF, D)
    qs, kvs, hs, js = (ROWS, 128), (ROWS, 256), (ROWS, 512), (ROWS, 384)

    layer = (1, 64, 384), (1, 64, 128)
    (first,) = call(
        pack_first_body, "pack_first",
        [(qkv_weight, layer[0], (0, 0, 0)), (proj_weight, layer[1], (0, 0, 0)),
         (norm_gains, (2, 2, 64), None), (row_biases, (2, 4, 64), None)],
        [sds((16, 72, 512), BF)],
    )
    first_all = lax.all_to_all(first, W, 0, 0)
    second_part, third_part = call(
        pack_rest_body, "pack_rest",
        [(qkv_weight, layer[0], (1, 0, 0)), (proj_weight, layer[1], (1, 0, 0)),
         (fc1_weight, (2, 64, 512), None), (fc2_weight, (2, 64, 512), None)],
        [sds((64, 1536), BF), sds((64, 1152), BF)],
    )
    second_all = lax.all_gather(second_part, W, axis=0, tiled=True)
    third_all = lax.all_gather(third_part, W, axis=0, tiled=True)
    table = (
        first_all[:, 64:70, :128].reshape(16, 12, 64).transpose(1, 0, 2).reshape(12, D).astype(F32)
    )
    tab = (table, (12, D), None)
    whole_first = (first_all, (16, 72, 512), None)
    qv = qv_bias.astype(F32).reshape(2, 2, 2, HD).transpose(0, 2, 1, 3)
    zero = jnp.zeros((2, 1, 2, HD), F32)
    joined_bias = jnp.concatenate([qv[:, :1], zero, qv[:, 1:]], axis=1).reshape(2, 1, 384)
    up_bias = fc1_bias.astype(F32).reshape(2, 1, 512)

    x, cot, b13 = call(
        relative_body, "to_relative",
        [(order, None, None), (block_in.reshape(ROWS, D), (ROWS, D), None), (cotangent.reshape(ROWS, D), (ROWS, D), None)],
        [sds((ROWS, D), BF), sds((ROWS, D), BF), sds((1, D), F32)],
    )

    saved = []
    stream = x
    qkv_of = (whole_first, (second_all, (D, 384), (0, 3)))
    proj_of = (whole_first, (third_all, (D, 128), (0, 8)))
    fc1_of = [(m, (D, 512), (0, 0)) for m in (second_all, third_all)]
    fc2_of = [(m, (D, 512), (0, 1)) for m in (second_all, third_all)]

    where = [(place, None, None), (slope, None, None)]
    for l in range(2):
        bias = (joined_bias[l], (1, 384), None)
        if l == 0:
            na, nb, kv = call(
                kv_first_body, "kv_first",
                [(x, half, (0, 0)), (x, half, (1, 0)), whole_first, tab, bias],
                [sds(half, BF), sds(half, BF), sds(kvs, BF)],
            )
        else:
            na, nb = gather_rows(normed)
            (kv,) = call(
                kv_body, "kv", [(na, half, None), (nb, half, None), qkv_of[l], bias], [sds(kvs, BF)]
            )
        kvo = lax.ppermute(kv, "context", [(0, 1)])
        (q,) = call(
            q_body, "q", [(na, half, None), (nb, half, None), qkv_of[l], bias], [sds(qs, BF)]
        )
        own, own_top, own_total = call(
            attend_own_body, "attend_own", where + [(q, qs, None), (kv, kvs, None)], [sds(qs, F32)] * 3
        )
        att, lse, pa, pb = call(
            attend_body, "attend",
            where + [(q, qs, None), (kvo, kvs, None), proj_of[l]] + [(v, qs, None) for v in (own, own_top, own_total)],
            [sds(qs, BF), sds(qs, F32), sds(half, BF), sds(half, BF)],
        )
        middle, second = norm_fwd(
            sum_pieces(pa, pb), stream, table, (l, 1), ((l, 1), (l, 2))
        )
        sa, sb = gather_rows(second)
        act, dgel, pa, pb = call(
            ffn_body, "ffn",
            [(sa, half, None), (sb, half, None), fc1_of[l], fc2_of[l], (up_bias[l], (1, 512), None)],
            [sds(hs, BF), sds(hs, BF), sds(half, BF), sds(half, BF)],
        )
        saved.append((stream, na, nb, q, kv, kvo, att, lse, middle, sa, sb, act, dgel))
        if l == 0:
            stream, normed = norm_fwd(
                sum_pieces(pa, pb), middle, table, (0, 3), ((1, 0), (1, 0))
            )
    out_own = out_rows(sum_pieces(pa, pb), middle, table)

    grad = cot
    ea = (cot, half, (0, 0))
    eb = (cot, half, (1, 0))
    for l in (1, 0):
        stream, na, nb, q, kv, kvo, att, lse, middle, sa, sb, act, dgel = saved[l]
        hg, up_sum, pa, pb = call(
            ffn_back_body, "ffn_back",
            [ea, eb, fc1_of[l], fc2_of[l], (dgel, hs, None)],
            [sds(hs, BF), sds((1, 512), F32), sds(half, BF), sds(half, BF)],
        )
        pieces = sum_pieces(pa, pb)
        ffn_ops = [ea, eb, (act, hs, None), (sa, half, None), (sb, half, None), (hg, hs, None)]
        if l == 1:
            (weights_grad,) = call(ffn_weights_body, "ffn_weights", ffn_ops, [sds((D, D), BF)])
            pieces, weights_grad, out_own = tie(pieces, weights_grad, out_own)
            ffn1_owned = lax.psum_scatter(weights_grad, W, scatter_dimension=0, tiled=True)
        else:
            (weights_grad,) = call(
                mixed_weights_body, "mixed_weights", ffn_ops + attn_ops1, [sds((D, 1536), BF)]
            )
            pieces, weights_grad = tie(pieces, weights_grad)
            mixed_owned = lax.psum_scatter(weights_grad, W, scatter_dimension=0, tiled=True)
        mid, mid_low, s2 = norm_bwd(pieces, middle, grad, table, (l, 1))
        ma, mb = gather_rows(mid_low)
        do, dq, dkvo = call(
            back_earlier_body, "back_earlier",
            where
            + [(ma, half, None), (mb, half, None), proj_of[l], (q, qs, None), (kvo, kvs, None), (lse, qs, None), (att, qs, None)],
            [sds(qs, BF), sds(qs, F32), sds(kvs, BF)],
        )
        got = lax.ppermute(dkvo, "context", [(1, 0)])
        dq, dkv = call(
            back_own_body, "back_own",
            where
            + [(do, qs, None), (q, qs, None), (kv, kvs, None), (lse, qs, None), (att, qs, None), (dq, qs, None)],
            [sds(qs, BF), sds(kvs, F32)],
        )
        if l == 1:
            dkv, out_own = tie(dkv, out_own)
            oa, ob = gather_rows(out_own)
        joined, qv_sum, pa, pb = call(
            qkv_back_body, "qkv_back",
            [(dq, qs, None), (dkv, kvs, None), (got, kvs, None), qkv_of[l]],
            [sds(js, BF), sds((1, 384), F32), sds(half, BF), sds(half, BF)],
        )
        pieces = sum_pieces(pa, pb)
        attn_ops = [(na, half, None), (nb, half, None), (joined, js, None), (ma, half, None), (mb, half, None), (att, qs, None)]
        if l == 1:
            pieces, oa = tie(pieces, oa)
            up1, qv1, s21, attn_ops1 = up_sum, qv_sum, s2, attn_ops
            grad, low, s11 = norm_bwd(pieces, stream, mid, table, (1, 0))
            near, far = gather_rows(low)
            ea, eb = (near, half, None), (far, half, None)
        else:
            three, one = (3, D), (1, D)
            (packed,) = call(
                last_pack_body, "last_pack",
                attn_ops
                + [(pa, half, None), (pb, half, None), (x, half, (0, 0)), (x, half, (1, 0))]
                + [(s21, three, None), (s11, three, None), (s2, three, None), (b13, one, None)]
                + [(up_sum, (1, 512), None), (up1, (1, 512), None), (qv_sum, (1, 384), None), (qv1, (1, 384), None)],
                [sds((16, 80, 512), BF)],
            )
            mixed = lax.all_to_all(packed, W, 0, 0)
            _, low, _ = norm_bwd(pieces, stream, mid, table, (0, 0))
            near, far = gather_rows(low)
            (block_out,) = call(
                sequence_body, "to_sequence",
                [(order, None, None), (oa, half, None), (ob, half, None)],
                [sds((ROWS, D), BF)],
            )
            (input_grad,) = call(
                sequence_body, "to_sequence",
                [(order, None, None), (near, half, None), (far, half, None)],
                [sds((ROWS, D), F32)],
            )
    odd = ctx.astype(jnp.int32).reshape(1)
    small = (12, 64)
    (tail,) = call(
        finish_columns_body, "finish_columns",
        [(odd, None, None), (mixed, (16, 80, 512), None)],
        [sds(small, F32)],
    )
    tail = tail + core_swap(tail)
    tails = [tail] + [along_y(tail, step) for step in (1, 2, 3)]
    fc1_grad, fc2_grad = call(
        finish_ffn_body, "finish_ffn",
        [(mixed_owned, (64, D), (0, 0)), (ffn1_owned, (64, D), None)],
        [sds((2, 64, 512), F32), sds((2, 64, 512), F32)],
    )
    qkv_grad, proj_grad, qv_grad, up_grad = call(
        finish_body, "finish",
        [(mixed, (16, 80, 512), None), (mixed_owned, (64, 512), (0, 2))],
        [sds((2, 64, 384), F32), sds((2, 64, 128), F32), sds((2, 256), F32), sds((2, 512), F32)],
    )
    gains_grad, biases_grad = call(
        finish_rows_body, "finish_rows",
        [(v, small, None) for v in tails],
        [sds((2, 2, 64), F32), sds((2, 4, 64), F32)],
    )
    return (
        block_out[None], input_grad[None], qkv_grad, proj_grad, fc1_grad, fc2_grad,
        qv_grad, up_grad, gains_grad, biases_grad,
    )


def solution(mesh):
    return jax.shard_map(
        per_device,
        mesh=mesh,
        in_specs=(
            P("shard", "context", None),
            P(None, W, T),
            P(None, W, T),
            P(None, W, T),
            P(None, W, T),
            P(None, T),
            P(None, T),
            P(None, None, W),
            P(None, None, W),
            P("shard", "context", None),
        ),
        out_specs=(
            P("shard", "context", None),
            P("shard", "context", None),
            P(None, W, T),
            P(None, W, T),
            P(None, W, T),
            P(None, W, T),
            P(None, T),
            P(None, T),
            P(None, None, W),
            P(None, None, W),
        ),
        check_vma=False,
    )
```

```python
import jax
import jax.numpy as jnp
from jax import lax
from jax.experimental import pallas as pl
from jax.experimental.pallas import tpu as pltpu
from jax.sharding import PartitionSpec as P

HEADS = 16
HD = 64
NORM_EPS = 1e-05
GELU_SCALE = 0.7978845608028654
GELU_CUBE = 0.044715
F32 = jnp.float32
BF = jnp.bfloat16
W = ("shard", "context")
T = "tensor"
ROWS = 512
HALF = 256
PIECE = 64
D = 1024
NEG = -1e30


def window(ref, shape, index):
    if tuple(ref.shape) == tuple(shape):
        return ref
    index = index or (0,) * len(shape)
    return ref.at[tuple(pl.ds(i * n, n) for i, n in zip(index, shape))]


def call(body, name, operands, outs):
    count = len(operands)

    def kernel(*refs):
        given = [
            ref if shape is None else window(ref, shape, index)
            for ref, (_, shape, index) in zip(refs, operands)
        ]
        body(*given, *refs[count:])

    def place(shape):
        return pl.BlockSpec(memory_space=pltpu.SMEM if shape is None else pltpu.VMEM)

    return pl.pallas_call(
        kernel,
        in_specs=[place(shape) for _, shape, _ in operands],
        out_specs=[pl.BlockSpec(memory_space=pltpu.VMEM) for _ in outs],
        out_shape=outs,
        compiler_params=pltpu.CompilerParams(vmem_limit_bytes=50 << 20),
        name=name,
    )(*[array for array, _, _ in operands])


def sds(shape, dtype):
    return jax.ShapeDtypeStruct(shape, dtype)


def mm(a, b):
    return lax.dot_general(a, b, (((1,), (0,)), ((), ())), preferred_element_type=F32)


def mm_nt(a, b):
    return lax.dot_general(a, b, (((1,), (1,)), ((), ())), preferred_element_type=F32)


def mm_tn(a, b):
    return lax.dot_general(a, b, (((0,), (0,)), ((), ())), preferred_element_type=F32)


def core_swap(v):
    return lax.ppermute(v, T, [(i, i ^ 1) for i in range(8)])


def along_y(v, step):
    return lax.ppermute(
        v, T, [(2 * y + c, 2 * ((y + step) % 4) + c) for y in range(4) for c in range(2)]
    )


def add_body(pa, got, h0, h1, h2, h3):
    both = pa[...].astype(F32) + got[...].astype(F32)
    h0[...] = both[:PIECE]
    h1[...] = both[PIECE : 2 * PIECE].astype(BF)
    h2[...] = both[2 * PIECE : 3 * PIECE].astype(BF)
    h3[...] = both[3 * PIECE :].astype(BF)


def tie(*values):
    return lax.optimization_barrier(values)


def chip_sums(keep, send):
    got = core_swap(send)
    return call(
        add_body,
        "pair_add",
        [(keep, (HALF, D), None), (got, (HALF, D), None)],
        [sds((PIECE, D), F32)] + [sds((PIECE, D), BF)] * 3,
    )


def spread(sums):
    h0, h1, h2, h3 = sums
    r2 = along_y(h2, -2)
    r1 = along_y(h1, -1)
    r3 = along_y(h3, -3)
    return h0, r1, r2, r3


def sum_pieces(keep, send):
    return spread(chip_sums(keep, send))


def gather_rows(own):
    r2 = along_y(own, 2)
    r1 = along_y(own, 1)
    r3 = along_y(own, 3)
    near = jnp.concatenate([own, r1, r2, r3], axis=0)
    far = core_swap(near)
    return near, far


def norm_parts(v):
    mean = jnp.mean(v, axis=-1, keepdims=True)
    centred = v - mean
    var = jnp.mean(centred * centred, axis=-1, keepdims=True)
    s = lax.rsqrt(var + NORM_EPS)
    return centred * s, s


def gain_row(table, l, i):
    at = 2 * l + i
    return table[at : at + 1]


def bias_row(table, l, i):
    at = 4 + 4 * l + i
    return table[at : at + 1]


def norm_fwd(pieces, resid, table, bias_at, next_at):
    def body(h0, r1, r2, r3, resid_ref, rows, stream, normed):
        v = (
            h0[...] + r1[...].astype(F32) + r2[...].astype(F32) + r3[...].astype(F32)
        ) + resid_ref[...].astype(F32) + bias_row(rows, *bias_at)
        stream[...] = v
        xhat, _ = norm_parts(v)
        gain, shift = next_at
        normed[...] = (xhat * gain_row(rows, *gain) + bias_row(rows, *shift)).astype(BF)

    b = (PIECE, D)
    return call(
        body,
        "norm_fwd",
        [(p, b, None) for p in (*pieces, resid)] + [(table, (12, D), None)],
        [sds(b, F32), sds(b, BF)],
    )


def out_rows(pieces, resid, table):
    def body(h0, r1, r2, r3, resid_ref, rows, out):
        out[...] = (
            (h0[...] + r1[...].astype(F32) + r2[...].astype(F32) + r3[...].astype(F32))
            + resid_ref[...]
            + bias_row(rows, 1, 3)
        ).astype(BF)

    b = (PIECE, D)
    return call(
        body,
        "out_rows",
        [(p, b, None) for p in (*pieces, resid)] + [(table, (12, D), None)],
        [sds(b, BF)],
    )[0]


def norm_bwd(pieces, stream, grad, table, gain_at):
    def body(h0, r1, r2, r3, stream_ref, grad_ref, rows, out, low, sums):
        g = h0[...] + r1[...].astype(F32) + r2[...].astype(F32) + r3[...].astype(F32)
        xhat, s = norm_parts(stream_ref[...].astype(F32))
        gx = g * xhat
        c = g * gain_row(rows, *gain_at)
        cx = c * xhat
        e = grad_ref[...].astype(F32) + s * (
            c
            - jnp.mean(c, axis=-1, keepdims=True)
            - xhat * jnp.mean(cx, axis=-1, keepdims=True)
        )
        out[...] = e
        low[...] = e.astype(BF)
        sums[0:1] = jnp.sum(gx, axis=0, keepdims=True)
        sums[1:2] = jnp.sum(g, axis=0, keepdims=True)
        sums[2:3] = jnp.sum(e, axis=0, keepdims=True)

    b = (PIECE, D)
    return call(
        body,
        "norm_bwd",
        [(p, b, None) for p in (*pieces, stream, grad)] + [(table, (12, D), None)],
        [sds(b, F32), sds(b, BF), sds((3, D), F32)],
    )


def kv_first_body(xa, xb, first, rows, bias, na, nb, kv):
    w = qkv_matrix(first)[:, 128:]
    for x, n, at in ((xa, na, 0), (xb, nb, HALF)):
        xhat, _ = norm_parts(x[...].astype(F32))
        normed = (xhat * gain_row(rows, 0, 0) + bias_row(rows, 0, 0)).astype(BF)
        n[...] = normed
        kv[at : at + HALF] = (mm(normed, w) + bias[:, 128:]).astype(BF)


def kv_body(na, nb, w, bias, kv):
    for n, at in ((na, 0), (nb, HALF)):
        kv[at : at + HALF] = (mm(n[...], w[:, 128:]) + bias[:, 128:]).astype(BF)


def q_body(na, nb, w, bias, q):
    m = qkv_matrix(w)[:, :128]
    for n, at in ((na, 0), (nb, HALF)):
        q[at : at + HALF] = (mm(n[...], m) + bias[:, :128]).astype(BF)


def proj_matrix(ref):
    return ref[:, :64, 384:].reshape(D, 128) if len(ref.shape) == 3 else ref[...]


def qkv_matrix(ref):
    return ref[:, :64, :384].reshape(D, 384) if len(ref.shape) == 3 else ref[...]


def places(place, shape, axis):
    r = lax.broadcasted_iota(jnp.int32, shape, axis)
    y, c = place[0], place[1]
    return ((y - ((r >> 6) & 3)) & 3) * 128 + ((c + (r >> 8)) & 1) * 64 + (r & 63)


def own_scores(place, slope, h, qh, kh, mask):
    pos = places(place, (1, ROWS), 1).astype(F32)
    return jnp.where(mask, mm_nt(qh, kh) * 0.125 + slope[h] * pos, NEG)


def earlier_scores(place, slope, h, qh, kh):
    pos = places(place, (1, ROWS), 1).astype(F32)
    off = jnp.where(place[2] == 1, 0.0, NEG)
    return mm_nt(qh, kh) * 0.125 + (slope[h] * (pos - 512.0) + off)


def own_mask(place):
    return places(place, (ROWS, 1), 0) >= places(place, (1, ROWS), 1)


def attend_own_body(place, slope, q, kv, out, top, total):
    mask = own_mask(place)
    for h in range(2):
        lo, hi = h * HD, (h + 1) * HD
        s = own_scores(place, slope, h, q[:, lo:hi], kv[:, lo:hi], mask)
        m = jnp.max(s, axis=-1, keepdims=True)
        p = jnp.exp(s - m)
        out[:, lo:hi] = mm(p.astype(BF), kv[:, 128 + lo : 128 + hi])
        top[:, lo:hi] = jnp.broadcast_to(m, (ROWS, HD))
        total[:, lo:hi] = jnp.broadcast_to(jnp.sum(p, axis=-1, keepdims=True), (ROWS, HD))


def attend_body(place, slope, q, kvo, pw, own, own_top, own_total, att, lse, pa, pb):
    outs, logs = [], []
    for h in range(2):
        lo, hi = h * HD, (h + 1) * HD
        s = earlier_scores(place, slope, h, q[:, lo:hi], kvo[:, lo:hi])
        m = own_top[:, lo : lo + 1]
        top = jnp.maximum(m, jnp.max(s, axis=-1, keepdims=True))
        p = jnp.exp(s - top)
        scale = jnp.exp(m - top)
        total = own_total[:, lo : lo + 1] * scale + jnp.sum(p, axis=-1, keepdims=True)
        o = own[:, lo:hi] * scale + mm(p.astype(BF), kvo[:, 128 + lo : 128 + hi])
        outs.append(o / total)
        logs.append(jnp.broadcast_to(top + jnp.log(total), (ROWS, HD)))
    attended = jnp.concatenate(outs, axis=1).astype(BF)
    att[...] = attended
    lse[...] = jnp.concatenate(logs, axis=1)
    w = proj_matrix(pw)
    pa[...] = mm_nt(attended[:HALF], w).astype(BF)
    pb[...] = mm_nt(attended[HALF:], w).astype(BF)


def score_grads(p, doh, vh, atth):
    delta = jnp.sum(doh.astype(F32) * atth.astype(F32), axis=-1, keepdims=True)
    return (p * (mm_nt(doh, vh) - delta)).astype(BF)


def back_earlier_body(place, slope, ma, mb, pw, q, kvo, lse, att, do_ref, dq, dkvo):
    w = proj_matrix(pw)
    do = jnp.concatenate([mm(ma[...], w), mm(mb[...], w)], axis=0).astype(BF)
    do_ref[...] = do
    dqs, dks, dvs = [], [], []
    for h in range(2):
        lo, hi = h * HD, (h + 1) * HD
        qh, kh, vh, doh = q[:, lo:hi], kvo[:, lo:hi], kvo[:, 128 + lo : 128 + hi], do[:, lo:hi]
        p = jnp.exp(earlier_scores(place, slope, h, qh, kh) - lse[:, lo : lo + 1])
        d = score_grads(p, doh, vh, att[:, lo:hi])
        dqs.append(mm(d, kh) * 0.125)
        dks.append(mm_tn(d, qh) * 0.125)
        dvs.append(mm_tn(p.astype(BF), doh))
    dq[...] = jnp.concatenate(dqs, axis=1)
    dkvo[...] = jnp.concatenate(dks + dvs, axis=1).astype(BF)


def back_own_body(place, slope, do, q, kv, lse, att, dq_part, dq, dkv):
    mask = own_mask(place)
    dqs, dks, dvs = [], [], []
    for h in range(2):
        lo, hi = h * HD, (h + 1) * HD
        qh, kh, vh, doh = q[:, lo:hi], kv[:, lo:hi], kv[:, 128 + lo : 128 + hi], do[:, lo:hi]
        p = jnp.exp(own_scores(place, slope, h, qh, kh, mask) - lse[:, lo : lo + 1])
        d = score_grads(p, doh, vh, att[:, lo:hi])
        dqs.append(mm(d, kh) * 0.125)
        dks.append(mm_tn(d, qh) * 0.125)
        dvs.append(mm_tn(p.astype(BF), doh))
    dq[...] = (dq_part[...] + jnp.concatenate(dqs, axis=1)).astype(BF)
    dkv[...] = jnp.concatenate(dks + dvs, axis=1)


def ffn_body(na, nb, w1, w2, bias, act, dgel, pa, pb):
    for n, p, at in ((na, pa, 0), (nb, pb, HALF)):
        v = mm(n[...], w1[...]) + bias[...]
        v2 = v * v
        th = jnp.tanh(GELU_SCALE * (v + GELU_CUBE * (v2 * v)))
        one = 0.5 + 0.5 * th
        a = (v * one).astype(BF)
        act[at : at + HALF] = a
        dgel[at : at + HALF] = (
            one
            + (0.5 * GELU_SCALE) * v * (1.0 - th * th) * (1.0 + (3.0 * GELU_CUBE) * v2)
        ).astype(BF)
        p[...] = mm_nt(a, w2[...]).astype(BF)


def ffn_back_body(ea, eb, w1, w2, dgel, hg, sums, pa, pb):
    total = jnp.zeros((1, 512), F32)
    for e, p, at in ((ea, pa, 0), (eb, pb, HALF)):
        g = (mm(e[...], w2[...]) * dgel[at : at + HALF].astype(F32)).astype(BF)
        hg[at : at + HALF] = g
        total += jnp.sum(g.astype(F32), axis=0, keepdims=True)
        p[...] = mm_nt(g, w1[...]).astype(BF)
    sums[...] = total


def ffn_weights_body(ea, eb, act, na, nb, hg, out):
    out[:, :512] = (mm_tn(na[...], hg[:HALF]) + mm_tn(nb[...], hg[HALF:])).astype(BF)
    out[:, 512:] = (mm_tn(ea[...], act[:HALF]) + mm_tn(eb[...], act[HALF:])).astype(BF)


def attn_weights_body(na, nb, joined, ma, mb, att, out):
    out[:, :384] = (
        mm_tn(na[...], joined[:HALF]) + mm_tn(nb[...], joined[HALF:])
    ).astype(BF)
    out[:, 384:] = (mm_tn(ma[...], att[:HALF]) + mm_tn(mb[...], att[HALF:])).astype(BF)


def mixed_weights_body(ea, eb, act, sa, sb, hg, na, nb, joined, ma, mb, att, out):
    ffn_weights_body(ea, eb, act, sa, sb, hg, out.at[:, :1024])
    attn_weights_body(na, nb, joined, ma, mb, att, out.at[:, 1024:])


def two_halves(v):
    high = v.astype(BF)
    return high, (v - high.astype(F32)).astype(BF)


def last_pack_body(
    na, nb, joined, ma, mb, att, pa, pb, xa, xb, s21, s11, s20, b13,
    up0, up1, qv0, qv1, out,
):
    g = (mm_tn(na[...], joined[:HALF]) + mm_tn(nb[...], joined[HALF:])).astype(BF)
    out[:, :64, :384] = g.reshape(16, 64, 384)
    g = (mm_tn(ma[...], att[:HALF]) + mm_tn(mb[...], att[HALF:])).astype(BF)
    out[:, :64, 384:] = g.reshape(16, 64, 128)
    gain = jnp.zeros((1, D), F32)
    shift = jnp.zeros((1, D), F32)
    for p, x in ((pa, xa), (pb, xb)):
        g = p[...].astype(F32)
        xhat, _ = norm_parts(x[...].astype(F32))
        gain += jnp.sum(g * xhat, axis=0, keepdims=True)
        shift += jnp.sum(g, axis=0, keepdims=True)
    columns = jnp.concatenate(
        [
            gain, s20[0:1], s11[0:1], s21[0:1],
            shift, s20[2:3], s20[1:2], s11[2:3], s11[1:2], s21[2:3], s21[1:2], b13[...],
        ]
    ).astype(BF)
    q0, q0l = two_halves(qv0[...])
    q1, q1l = two_halves(qv1[...])
    u0, u0l = two_halves(up0[...])
    u1, u1l = two_halves(up1[...])
    none = jnp.zeros((1, 384), BF)
    lines = jnp.concatenate(
        [
            q0, q1, q0l, q1l,
            u0[:, :384], u1[:, :384], u0l[:, :384], u1l[:, :384],
            jnp.concatenate([u0[:, 384:], u1[:, 384:], none[:, :128]], axis=1),
            jnp.concatenate([u0l[:, 384:], u1l[:, 384:], none[:, :128]], axis=1),
            none, none,
        ]
    )
    for w in range(16):
        at = 128 * (w // 2)
        tail = jnp.concatenate([columns[:, at : at + 128], lines], axis=1)
        out[w, 64:80] = jnp.concatenate([tail, jnp.zeros((4, 512), BF)])


def qkv_back_body(dq, dkv, got, w, joined, sums, pa, pb):
    j = jnp.concatenate(
        [dq[...], (dkv[...] + got[...].astype(F32)).astype(BF)], axis=1
    )
    joined[...] = j
    sums[...] = jnp.sum(j.astype(F32), axis=0, keepdims=True)
    m = qkv_matrix(w)
    pa[...] = mm_nt(j[:HALF], m).astype(BF)
    pb[...] = mm_nt(j[HALF:], m).astype(BF)


def by_kind(m):
    parts = [m[:, i * HD : (i + 1) * HD] for i in range(6)]
    return jnp.concatenate([parts[i] for i in (0, 3, 1, 4, 2, 5)], axis=1)


def by_head(m):
    parts = [m[:, i * HD : (i + 1) * HD] for i in range(6)]
    return jnp.concatenate([parts[i] for i in (0, 2, 4, 1, 3, 5)], axis=1)


def pack_first_body(qkv, proj, gains, biases, first):
    small = [gains[l, i : i + 1] for l in range(2) for i in range(2)]
    small += [biases[l, i : i + 1] for l in range(2) for i in range(4)]
    lines = jnp.concatenate(
        [jnp.concatenate([small[2 * i], small[2 * i + 1]], axis=1) for i in range(6)]
        + [jnp.zeros((2, 128), BF)]
    )
    own = jnp.concatenate(
        [
            jnp.concatenate([by_kind(qkv[0]), proj[0]], axis=1),
            jnp.concatenate([lines, jnp.zeros((8, 384), BF)], axis=1),
        ]
    )
    for w in range(16):
        first[w] = own


def pack_rest_body(qkv, proj, fc1, fc2, second, third):
    second[:, :512] = fc1[0]
    second[:, 512:1024] = fc2[0]
    second[:, 1024:1152] = jnp.zeros((64, 128), BF)
    second[:, 1152:] = by_kind(qkv[0])
    third[:, :512] = fc1[1]
    third[:, 512:1024] = fc2[1]
    third[:, 1024:] = proj[0]


def sum16(ref, *at):
    total = ref[(0, *at)].astype(F32)
    for w in range(1, 16):
        total += ref[(w, *at)].astype(F32)
    return total


def finish_ffn_body(f0, f1, fc1, fc2):
    for l, f in enumerate((f0, f1)):
        fc1[l] = f[:, :512].astype(F32)
        fc2[l] = f[:, 512:1024].astype(F32)


def finish_columns_body(odd, mixed, columns):
    own = mixed[0, 64:80, :128].astype(F32)
    for w in range(1, 16):
        own += mixed[w, 64:80, :128].astype(F32)
    columns[...] = jnp.where(odd[0] == 1, own[:12, 64:], own[:12, :64])


def finish_body(mixed, attn1, qkv, proj, qv, up):
    total = sum16(mixed)
    for l, m in enumerate((total[:64], attn1[...].astype(F32))):
        qkv[l] = by_head(m[:, :384])
        proj[l] = m[:, 384:]
    own = total[64:76]
    for l in range(2):
        line = own[l : l + 1, 128:] + own[2 + l : 3 + l, 128:]
        parts = [line[:, i * HD : (i + 1) * HD] for i in (0, 4, 1, 5)]
        qv[l : l + 1] = jnp.concatenate(parts, axis=1)
        near = own[4 + l : 5 + l, 128:] + own[6 + l : 7 + l, 128:]
        at = 128 + 128 * l
        up[l : l + 1] = jnp.concatenate(
            [near, own[8:9, at : at + 128] + own[9:10, at : at + 128]], axis=1
        )


def finish_rows_body(t0, t1, t2, t3, gains, biases):
    total = (t0[...] + t1[...]) + (t2[...] + t3[...])
    for l in range(2):
        gains[l] = total[2 * l : 2 * l + 2]
        biases[l] = total[4 + 4 * l : 8 + 4 * l]


def relative_body(order, x, cot, xr, cr, total):
    for j in range(8):
        row = pl.multiple_of(order[j] * PIECE, PIECE)
        xr[j * PIECE : (j + 1) * PIECE] = x[pl.ds(row, PIECE)]
        cr[j * PIECE : (j + 1) * PIECE] = cot[pl.ds(row, PIECE)]
    total[...] = jnp.sum(cr[:PIECE].astype(F32), axis=0, keepdims=True)


def sequence_body(order, near, far, out):
    for j in range(8):
        row = pl.multiple_of(order[j] * PIECE, PIECE)
        src = near if j < 4 else far
        k = j % 4
        out[pl.ds(row, PIECE)] = src[k * PIECE : (k + 1) * PIECE].astype(out.dtype)


def per_device(
    block_in, qkv_weight, proj_weight, fc1_weight, fc2_weight,
    qv_bias, fc1_bias, norm_gains, row_biases, cotangent,
):
    t = lax.axis_index(T)
    y, c = t // 2, t % 2
    ctx = lax.axis_index("context")
    place = jnp.stack([y, c, ctx]).astype(jnp.int32)
    slope = jnp.exp2(-8.0 * (2 * t + 1 + jnp.arange(2)).astype(F32) / HEADS)
    j = jnp.arange(8)
    order = (2 * ((y - j % 4) % 4) + (c + j // 4) % 2).astype(jnp.int32)
    half = (HALF, D)
    qs, kvs, hs, js = (ROWS, 128), (ROWS, 256), (ROWS, 512), (ROWS, 384)

    layer = (1, 64, 384), (1, 64, 128)
    (first,) = call(
        pack_first_body, "pack_first",
        [(qkv_weight, layer[0], (0, 0, 0)), (proj_weight, layer[1], (0, 0, 0)),
         (norm_gains, (2, 2, 64), None), (row_biases, (2, 4, 64), None)],
        [sds((16, 72, 512), BF)],
    )
    first_all = lax.all_to_all(first, W, 0, 0)
    second_part, third_part = call(
        pack_rest_body, "pack_rest",
        [(qkv_weight, layer[0], (1, 0, 0)), (proj_weight, layer[1], (1, 0, 0)),
         (fc1_weight, (2, 64, 512), None), (fc2_weight, (2, 64, 512), None)],
        [sds((64, 1536), BF), sds((64, 1152), BF)],
    )
    second_all = lax.all_gather(second_part, W, axis=0, tiled=True)
    third_all = lax.all_gather(third_part, W, axis=0, tiled=True)
    table = (
        first_all[:, 64:70, :128].reshape(16, 12, 64).transpose(1, 0, 2).reshape(12, D).astype(F32)
    )
    tab = (table, (12, D), None)
    whole_first = (first_all, (16, 72, 512), None)
    qv = qv_bias.astype(F32).reshape(2, 2, 2, HD).transpose(0, 2, 1, 3)
    zero = jnp.zeros((2, 1, 2, HD), F32)
    joined_bias = jnp.concatenate([qv[:, :1], zero, qv[:, 1:]], axis=1).reshape(2, 1, 384)
    up_bias = fc1_bias.astype(F32).reshape(2, 1, 512)

    x, cot, b13 = call(
        relative_body, "to_relative",
        [(order, None, None), (block_in.reshape(ROWS, D), (ROWS, D), None), (cotangent.reshape(ROWS, D), (ROWS, D), None)],
        [sds((ROWS, D), BF), sds((ROWS, D), BF), sds((1, D), F32)],
    )

    saved = []
    stream = x
    qkv_of = (whole_first, (second_all, (D, 384), (0, 3)))
    proj_of = (whole_first, (third_all, (D, 128), (0, 8)))
    fc1_of = [(m, (D, 512), (0, 0)) for m in (second_all, third_all)]
    fc2_of = [(m, (D, 512), (0, 1)) for m in (second_all, third_all)]

    where = [(place, None, None), (slope, None, None)]
    for l in range(2):
        bias = (joined_bias[l], (1, 384), None)
        if l == 0:
            na, nb, kv = call(
                kv_first_body, "kv_first",
                [(x, half, (0, 0)), (x, half, (1, 0)), whole_first, tab, bias],
                [sds(half, BF), sds(half, BF), sds(kvs, BF)],
            )
        else:
            na, nb = gather_rows(normed)
            (kv,) = call(
                kv_body, "kv", [(na, half, None), (nb, half, None), qkv_of[l], bias], [sds(kvs, BF)]
            )
        kvo = lax.ppermute(kv, "context", [(0, 1)])
        (q,) = call(
            q_body, "q", [(na, half, None), (nb, half, None), qkv_of[l], bias], [sds(qs, BF)]
        )
        own, own_top, own_total = call(
            attend_own_body, "attend_own", where + [(q, qs, None), (kv, kvs, None)], [sds(qs, F32)] * 3
        )
        att, lse, pa, pb = call(
            attend_body, "attend",
            where + [(q, qs, None), (kvo, kvs, None), proj_of[l]] + [(v, qs, None) for v in (own, own_top, own_total)],
            [sds(qs, BF), sds(qs, F32), sds(half, BF), sds(half, BF)],
        )
        middle, second = norm_fwd(
            sum_pieces(pa, pb), stream, table, (l, 1), ((l, 1), (l, 2))
        )
        sa, sb = gather_rows(second)
        act, dgel, pa, pb = call(
            ffn_body, "ffn",
            [(sa, half, None), (sb, half, None), fc1_of[l], fc2_of[l], (up_bias[l], (1, 512), None)],
            [sds(hs, BF), sds(hs, BF), sds(half, BF), sds(half, BF)],
        )
        saved.append((stream, na, nb, q, kv, kvo, att, lse, middle, sa, sb, act, dgel))
        if l == 0:
            stream, normed = norm_fwd(
                sum_pieces(pa, pb), middle, table, (0, 3), ((1, 0), (1, 0))
            )
    out_own = out_rows(sum_pieces(pa, pb), middle, table)

    grad = cot
    ea = (cot, half, (0, 0))
    eb = (cot, half, (1, 0))
    for l in (1, 0):
        stream, na, nb, q, kv, kvo, att, lse, middle, sa, sb, act, dgel = saved[l]
        hg, up_sum, pa, pb = call(
            ffn_back_body, "ffn_back",
            [ea, eb, fc1_of[l], fc2_of[l], (dgel, hs, None)],
            [sds(hs, BF), sds((1, 512), F32), sds(half, BF), sds(half, BF)],
        )
        pieces = sum_pieces(pa, pb)
        ffn_ops = [ea, eb, (act, hs, None), (sa, half, None), (sb, half, None), (hg, hs, None)]
        if l == 1:
            (weights_grad,) = call(ffn_weights_body, "ffn_weights", ffn_ops, [sds((D, D), BF)])
            pieces, weights_grad, out_own = tie(pieces, weights_grad, out_own)
            ffn1_owned = lax.psum_scatter(weights_grad, W, scatter_dimension=0, tiled=True)
        else:
            (weights_grad,) = call(
                mixed_weights_body, "mixed_weights", ffn_ops + attn_ops1, [sds((D, 1536), BF)]
            )
            pieces, weights_grad, ffn1_owned = tie(pieces, weights_grad, ffn1_owned)
            mixed_owned = lax.psum_scatter(weights_grad, W, scatter_dimension=0, tiled=True)
        mid, mid_low, s2 = norm_bwd(pieces, middle, grad, table, (l, 1))
        ma, mb = gather_rows(mid_low)
        do, dq, dkvo = call(
            back_earlier_body, "back_earlier",
            where
            + [(ma, half, None), (mb, half, None), proj_of[l], (q, qs, None), (kvo, kvs, None), (lse, qs, None), (att, qs, None)],
            [sds(qs, BF), sds(qs, F32), sds(kvs, BF)],
        )
        got = lax.ppermute(dkvo, "context", [(1, 0)])
        dq, dkv = call(
            back_own_body, "back_own",
            where
            + [(do, qs, None), (q, qs, None), (kv, kvs, None), (lse, qs, None), (att, qs, None), (dq, qs, None)],
            [sds(qs, BF), sds(kvs, F32)],
        )
        if l == 1:
            dkv, out_own = tie(dkv, out_own)
            oa, ob = gather_rows(out_own)
        joined, qv_sum, pa, pb = call(
            qkv_back_body, "qkv_back",
            [(dq, qs, None), (dkv, kvs, None), (got, kvs, None), qkv_of[l]],
            [sds(js, BF), sds((1, 384), F32), sds(half, BF), sds(half, BF)],
        )
        pieces = sum_pieces(pa, pb)
        attn_ops = [(na, half, None), (nb, half, None), (joined, js, None), (ma, half, None), (mb, half, None), (att, qs, None)]
        if l == 1:
            pieces, oa = tie(pieces, oa)
            up1, qv1, s21, attn_ops1 = up_sum, qv_sum, s2, attn_ops
            grad, low, s11 = norm_bwd(pieces, stream, mid, table, (1, 0))
            near, far = gather_rows(low)
            ea, eb = (near, half, None), (far, half, None)
        else:
            three, one = (3, D), (1, D)
            (packed,) = call(
                last_pack_body, "last_pack",
                attn_ops
                + [(pa, half, None), (pb, half, None), (x, half, (0, 0)), (x, half, (1, 0))]
                + [(s21, three, None), (s11, three, None), (s2, three, None), (b13, one, None)]
                + [(up_sum, (1, 512), None), (up1, (1, 512), None), (qv_sum, (1, 384), None), (qv1, (1, 384), None)],
                [sds((16, 80, 512), BF)],
            )
            mixed = lax.all_to_all(packed, W, 0, 0)
            _, low, _ = norm_bwd(pieces, stream, mid, table, (0, 0))
            near, far = gather_rows(low)
            (block_out,) = call(
                sequence_body, "to_sequence",
                [(order, None, None), (oa, half, None), (ob, half, None)],
                [sds((ROWS, D), BF)],
            )
            (input_grad,) = call(
                sequence_body, "to_sequence",
                [(order, None, None), (near, half, None), (far, half, None)],
                [sds((ROWS, D), F32)],
            )
    odd = ctx.astype(jnp.int32).reshape(1)
    small = (12, 64)
    (tail,) = call(
        finish_columns_body, "finish_columns",
        [(odd, None, None), (mixed, (16, 80, 512), None)],
        [sds(small, F32)],
    )
    tail = tail + core_swap(tail)
    tails = [tail] + [along_y(tail, step) for step in (1, 2, 3)]
    fc1_grad, fc2_grad = call(
        finish_ffn_body, "finish_ffn",
        [(mixed_owned, (64, D), (0, 0)), (ffn1_owned, (64, D), None)],
        [sds((2, 64, 512), F32), sds((2, 64, 512), F32)],
    )
    qkv_grad, proj_grad, qv_grad, up_grad = call(
        finish_body, "finish",
        [(mixed, (16, 80, 512), None), (mixed_owned, (64, 512), (0, 2))],
        [sds((2, 64, 384), F32), sds((2, 64, 128), F32), sds((2, 256), F32), sds((2, 512), F32)],
    )
    gains_grad, biases_grad = call(
        finish_rows_body, "finish_rows",
        [(v, small, None) for v in tails],
        [sds((2, 2, 64), F32), sds((2, 4, 64), F32)],
    )
    return (
        block_out[None], input_grad[None], qkv_grad, proj_grad, fc1_grad, fc2_grad,
        qv_grad, up_grad, gains_grad, biases_grad,
    )


def solution(mesh):
    return jax.shard_map(
        per_device,
        mesh=mesh,
        in_specs=(
            P("shard", "context", None),
            P(None, W, T),
            P(None, W, T),
            P(None, W, T),
            P(None, W, T),
            P(None, T),
            P(None, T),
            P(None, None, W),
            P(None, None, W),
            P("shard", "context", None),
        ),
        out_specs=(
            P("shard", "context", None),
            P("shard", "context", None),
            P(None, W, T),
            P(None, W, T),
            P(None, W, T),
            P(None, W, T),
            P(None, T),
            P(None, T),
            P(None, None, W),
            P(None, None, W),
        ),
        check_vma=False,
    )
```

```python
import jax
import jax.numpy as jnp
from jax import lax
from jax.experimental import pallas as pl
from jax.experimental.pallas import tpu as pltpu
from jax.sharding import PartitionSpec as P

HEADS = 16
HD = 64
NORM_EPS = 1e-05
GELU_SCALE = 0.7978845608028654
GELU_CUBE = 0.044715
F32 = jnp.float32
BF = jnp.bfloat16
W = ("shard", "context")
T = "tensor"
ROWS = 512
HALF = 256
PIECE = 64
D = 1024
NEG = -1e30


def spec(shape, index=None):
    place = tuple(index) if index is not None else (0,) * len(shape)
    return pl.BlockSpec(shape, lambda i: place)


def smem():
    return pl.BlockSpec(memory_space=pltpu.SMEM)


def call(body, name, operands, outs):
    in_specs, args = [], []
    for array, shape, index in operands:
        in_specs.append(smem() if shape is None else spec(shape, index))
        args.append(array)
    return pl.pallas_call(
        body,
        grid=(1,),
        in_specs=in_specs,
        out_specs=[spec(o.shape) for o in outs],
        out_shape=outs,
        compiler_params=pltpu.CompilerParams(vmem_limit_bytes=50 << 20),
        name=name,
    )(*args)


def sds(shape, dtype):
    return jax.ShapeDtypeStruct(shape, dtype)


def mm(a, b):
    return lax.dot_general(a, b, (((1,), (0,)), ((), ())), preferred_element_type=F32)


def mm_nt(a, b):
    return lax.dot_general(a, b, (((1,), (1,)), ((), ())), preferred_element_type=F32)


def mm_tn(a, b):
    return lax.dot_general(a, b, (((0,), (0,)), ((), ())), preferred_element_type=F32)


def core_swap(v):
    return lax.ppermute(v, T, [(i, i ^ 1) for i in range(8)])


def along_y(v, step):
    return lax.ppermute(
        v, T, [(2 * y + c, 2 * ((y + step) % 4) + c) for y in range(4) for c in range(2)]
    )


def add_body(pa, got, h0, h1, h2, h3):
    both = pa[...].astype(F32) + got[...].astype(F32)
    h0[...] = both[:PIECE]
    h1[...] = both[PIECE : 2 * PIECE].astype(BF)
    h2[...] = both[2 * PIECE : 3 * PIECE].astype(BF)
    h3[...] = both[3 * PIECE :].astype(BF)


def tie(*values):
    return lax.optimization_barrier(values)


def chip_sums(keep, send):
    got = core_swap(send)
    return call(
        add_body,
        "pair_add",
        [(keep, (HALF, D), None), (got, (HALF, D), None)],
        [sds((PIECE, D), F32)] + [sds((PIECE, D), BF)] * 3,
    )


def spread(sums):
    h0, h1, h2, h3 = sums
    r2 = along_y(h2, -2)
    r1 = along_y(h1, -1)
    r3 = along_y(h3, -3)
    return h0, r1, r2, r3


def sum_pieces(keep, send):
    return spread(chip_sums(keep, send))


def gather_rows(own):
    r2 = along_y(own, 2)
    r1 = along_y(own, 1)
    r3 = along_y(own, 3)
    near = jnp.concatenate([own, r1, r2, r3], axis=0)
    far = core_swap(near)
    return near, far


def norm_parts(v):
    mean = jnp.mean(v, axis=-1, keepdims=True)
    centred = v - mean
    var = jnp.mean(centred * centred, axis=-1, keepdims=True)
    s = lax.rsqrt(var + NORM_EPS)
    return centred * s, s


def gain_row(table, l, i):
    at = 2 * l + i
    return table[at : at + 1]


def bias_row(table, l, i):
    at = 4 + 4 * l + i
    return table[at : at + 1]


def norm_fwd(pieces, resid, table, bias_at, next_at):
    def body(h0, r1, r2, r3, resid_ref, rows, stream, normed):
        v = (
            h0[...] + r1[...].astype(F32) + r2[...].astype(F32) + r3[...].astype(F32)
        ) + resid_ref[...].astype(F32) + bias_row(rows, *bias_at)
        stream[...] = v
        xhat, _ = norm_parts(v)
        gain, shift = next_at
        normed[...] = (xhat * gain_row(rows, *gain) + bias_row(rows, *shift)).astype(BF)

    b = (PIECE, D)
    return call(
        body,
        "norm_fwd",
        [(p, b, None) for p in (*pieces, resid)] + [(table, (12, D), None)],
        [sds(b, F32), sds(b, BF)],
    )


def out_rows(pieces, resid, table):
    def body(h0, r1, r2, r3, resid_ref, rows, out):
        out[...] = (
            (h0[...] + r1[...].astype(F32) + r2[...].astype(F32) + r3[...].astype(F32))
            + resid_ref[...]
            + bias_row(rows, 1, 3)
        ).astype(BF)

    b = (PIECE, D)
    return call(
        body,
        "out_rows",
        [(p, b, None) for p in (*pieces, resid)] + [(table, (12, D), None)],
        [sds(b, BF)],
    )[0]


def norm_bwd(pieces, stream, grad, table, gain_at):
    def body(h0, r1, r2, r3, stream_ref, grad_ref, rows, out, low, sums):
        g = h0[...] + r1[...].astype(F32) + r2[...].astype(F32) + r3[...].astype(F32)
        xhat, s = norm_parts(stream_ref[...].astype(F32))
        gx = g * xhat
        c = g * gain_row(rows, *gain_at)
        cx = c * xhat
        e = grad_ref[...].astype(F32) + s * (
            c
            - jnp.mean(c, axis=-1, keepdims=True)
            - xhat * jnp.mean(cx, axis=-1, keepdims=True)
        )
        out[...] = e
        low[...] = e.astype(BF)
        sums[0:1] = jnp.sum(gx, axis=0, keepdims=True)
        sums[1:2] = jnp.sum(g, axis=0, keepdims=True)
        sums[2:3] = jnp.sum(e, axis=0, keepdims=True)

    b = (PIECE, D)
    return call(
        body,
        "norm_bwd",
        [(p, b, None) for p in (*pieces, stream, grad)] + [(table, (12, D), None)],
        [sds(b, F32), sds(b, BF), sds((3, D), F32)],
    )


def kv_first_body(xa, xb, first, rows, bias, na, nb, kv):
    w = qkv_matrix(first)[:, 128:]
    for x, n, at in ((xa, na, 0), (xb, nb, HALF)):
        xhat, _ = norm_parts(x[...].astype(F32))
        normed = (xhat * gain_row(rows, 0, 0) + bias_row(rows, 0, 0)).astype(BF)
        n[...] = normed
        kv[at : at + HALF] = (mm(normed, w) + bias[:, 128:]).astype(BF)


def kv_body(na, nb, w, bias, kv):
    for n, at in ((na, 0), (nb, HALF)):
        kv[at : at + HALF] = (mm(n[...], w[:, 128:]) + bias[:, 128:]).astype(BF)


def q_body(na, nb, w, bias, q):
    m = qkv_matrix(w)[:, :128]
    for n, at in ((na, 0), (nb, HALF)):
        q[at : at + HALF] = (mm(n[...], m) + bias[:, :128]).astype(BF)


def proj_matrix(ref):
    return ref[:, :64, 384:].reshape(D, 128) if len(ref.shape) == 3 else ref[...]


def qkv_matrix(ref):
    return ref[:, :64, :384].reshape(D, 384) if len(ref.shape) == 3 else ref[...]


def places(place, shape, axis):
    r = lax.broadcasted_iota(jnp.int32, shape, axis)
    y, c = place[0], place[1]
    return ((y - ((r >> 6) & 3)) & 3) * 128 + ((c + (r >> 8)) & 1) * 64 + (r & 63)


def own_scores(place, slope, h, qh, kh, mask):
    pos = places(place, (1, ROWS), 1).astype(F32)
    return jnp.where(mask, mm_nt(qh, kh) * 0.125 + slope[h] * pos, NEG)


def earlier_scores(place, slope, h, qh, kh):
    pos = places(place, (1, ROWS), 1).astype(F32)
    off = jnp.where(place[2] == 1, 0.0, NEG)
    return mm_nt(qh, kh) * 0.125 + (slope[h] * (pos - 512.0) + off)


def own_mask(place):
    return places(place, (ROWS, 1), 0) >= places(place, (1, ROWS), 1)


def attend_own_body(place, slope, q, kv, out, top, total):
    mask = own_mask(place)
    for h in range(2):
        lo, hi = h * HD, (h + 1) * HD
        s = own_scores(place, slope, h, q[:, lo:hi], kv[:, lo:hi], mask)
        m = jnp.max(s, axis=-1, keepdims=True)
        p = jnp.exp(s - m)
        out[:, lo:hi] = mm(p.astype(BF), kv[:, 128 + lo : 128 + hi])
        top[:, lo:hi] = jnp.broadcast_to(m, (ROWS, HD))
        total[:, lo:hi] = jnp.broadcast_to(jnp.sum(p, axis=-1, keepdims=True), (ROWS, HD))


def attend_body(place, slope, q, kvo, pw, own, own_top, own_total, att, lse, pa, pb):
    outs, logs = [], []
    for h in range(2):
        lo, hi = h * HD, (h + 1) * HD
        s = earlier_scores(place, slope, h, q[:, lo:hi], kvo[:, lo:hi])
        m = own_top[:, lo : lo + 1]
        top = jnp.maximum(m, jnp.max(s, axis=-1, keepdims=True))
        p = jnp.exp(s - top)
        scale = jnp.exp(m - top)
        total = own_total[:, lo : lo + 1] * scale + jnp.sum(p, axis=-1, keepdims=True)
        o = own[:, lo:hi] * scale + mm(p.astype(BF), kvo[:, 128 + lo : 128 + hi])
        outs.append(o / total)
        logs.append(jnp.broadcast_to(top + jnp.log(total), (ROWS, HD)))
    attended = jnp.concatenate(outs, axis=1).astype(BF)
    att[...] = attended
    lse[...] = jnp.concatenate(logs, axis=1)
    w = proj_matrix(pw)
    pa[...] = mm_nt(attended[:HALF], w).astype(BF)
    pb[...] = mm_nt(attended[HALF:], w).astype(BF)


def score_grads(p, doh, vh, atth):
    delta = jnp.sum(doh.astype(F32) * atth.astype(F32), axis=-1, keepdims=True)
    return (p * (mm_nt(doh, vh) - delta)).astype(BF)


def back_earlier_body(place, slope, ma, mb, pw, q, kvo, lse, att, do_ref, dq, dkvo):
    w = proj_matrix(pw)
    do = jnp.concatenate([mm(ma[...], w), mm(mb[...], w)], axis=0).astype(BF)
    do_ref[...] = do
    dqs, dks, dvs = [], [], []
    for h in range(2):
        lo, hi = h * HD, (h + 1) * HD
        qh, kh, vh, doh = q[:, lo:hi], kvo[:, lo:hi], kvo[:, 128 + lo : 128 + hi], do[:, lo:hi]
        p = jnp.exp(earlier_scores(place, slope, h, qh, kh) - lse[:, lo : lo + 1])
        d = score_grads(p, doh, vh, att[:, lo:hi])
        dqs.append(mm(d, kh) * 0.125)
        dks.append(mm_tn(d, qh) * 0.125)
        dvs.append(mm_tn(p.astype(BF), doh))
    dq[...] = jnp.concatenate(dqs, axis=1)
    dkvo[...] = jnp.concatenate(dks + dvs, axis=1).astype(BF)


def back_own_body(place, slope, do, q, kv, lse, att, dq_part, dq, dkv):
    mask = own_mask(place)
    dqs, dks, dvs = [], [], []
    for h in range(2):
        lo, hi = h * HD, (h + 1) * HD
        qh, kh, vh, doh = q[:, lo:hi], kv[:, lo:hi], kv[:, 128 + lo : 128 + hi], do[:, lo:hi]
        p = jnp.exp(own_scores(place, slope, h, qh, kh, mask) - lse[:, lo : lo + 1])
        d = score_grads(p, doh, vh, att[:, lo:hi])
        dqs.append(mm(d, kh) * 0.125)
        dks.append(mm_tn(d, qh) * 0.125)
        dvs.append(mm_tn(p.astype(BF), doh))
    dq[...] = (dq_part[...] + jnp.concatenate(dqs, axis=1)).astype(BF)
    dkv[...] = jnp.concatenate(dks + dvs, axis=1)


def ffn_body(na, nb, w1, w2, bias, act, dgel, pa, pb):
    for n, p, at in ((na, pa, 0), (nb, pb, HALF)):
        v = mm(n[...], w1[...]) + bias[...]
        v2 = v * v
        th = jnp.tanh(GELU_SCALE * (v + GELU_CUBE * (v2 * v)))
        one = 0.5 + 0.5 * th
        a = (v * one).astype(BF)
        act[at : at + HALF] = a
        dgel[at : at + HALF] = (
            one
            + (0.5 * GELU_SCALE) * v * (1.0 - th * th) * (1.0 + (3.0 * GELU_CUBE) * v2)
        ).astype(BF)
        p[...] = mm_nt(a, w2[...]).astype(BF)


def ffn_back_body(ea, eb, w1, w2, dgel, hg, sums, pa, pb):
    total = jnp.zeros((1, 512), F32)
    for e, p, at in ((ea, pa, 0), (eb, pb, HALF)):
        g = (mm(e[...], w2[...]) * dgel[at : at + HALF].astype(F32)).astype(BF)
        hg[at : at + HALF] = g
        total += jnp.sum(g.astype(F32), axis=0, keepdims=True)
        p[...] = mm_nt(g, w1[...]).astype(BF)
    sums[...] = total


def ffn_weights_body(ea, eb, act, na, nb, hg, out):
    out[:, :512] = (mm_tn(na[...], hg[:HALF]) + mm_tn(nb[...], hg[HALF:])).astype(BF)
    out[:, 512:] = (mm_tn(ea[...], act[:HALF]) + mm_tn(eb[...], act[HALF:])).astype(BF)


def attn_weights_body(na, nb, joined, ma, mb, att, out):
    out[:, :384] = (
        mm_tn(na[...], joined[:HALF]) + mm_tn(nb[...], joined[HALF:])
    ).astype(BF)
    out[:, 384:] = (mm_tn(ma[...], att[:HALF]) + mm_tn(mb[...], att[HALF:])).astype(BF)


def layer_weights_body(ea, eb, act, sa, sb, hg, na, nb, joined, ma, mb, att, out):
    ffn_weights_body(ea, eb, act, sa, sb, hg, out.at[:, :1024])
    attn_weights_body(na, nb, joined, ma, mb, att, out.at[:, 1024:])


def two_halves(v):
    high = v.astype(BF)
    return high, (v - high.astype(F32)).astype(BF)


def last_pack_body(
    na, nb, joined, ma, mb, att, pa, pb, xa, xb, s21, s11, s20, b13,
    up0, up1, qv0, qv1, out,
):
    g = (mm_tn(na[...], joined[:HALF]) + mm_tn(nb[...], joined[HALF:])).astype(BF)
    out[:, :64, :384] = g.reshape(16, 64, 384)
    g = (mm_tn(ma[...], att[:HALF]) + mm_tn(mb[...], att[HALF:])).astype(BF)
    out[:, :64, 384:] = g.reshape(16, 64, 128)
    gain = jnp.zeros((1, D), F32)
    shift = jnp.zeros((1, D), F32)
    for p, x in ((pa, xa), (pb, xb)):
        g = p[...].astype(F32)
        xhat, _ = norm_parts(x[...].astype(F32))
        gain += jnp.sum(g * xhat, axis=0, keepdims=True)
        shift += jnp.sum(g, axis=0, keepdims=True)
    columns = jnp.concatenate(
        [
            gain, s20[0:1], s11[0:1], s21[0:1],
            shift, s20[2:3], s20[1:2], s11[2:3], s11[1:2], s21[2:3], s21[1:2], b13[...],
        ]
    ).astype(BF)
    q0, q0l = two_halves(qv0[...])
    q1, q1l = two_halves(qv1[...])
    u0, u0l = two_halves(up0[...])
    u1, u1l = two_halves(up1[...])
    none = jnp.zeros((1, 384), BF)
    lines = jnp.concatenate(
        [
            q0, q1, q0l, q1l,
            u0[:, :384], u1[:, :384], u0l[:, :384], u1l[:, :384],
            jnp.concatenate([u0[:, 384:], u1[:, 384:], none[:, :128]], axis=1),
            jnp.concatenate([u0l[:, 384:], u1l[:, 384:], none[:, :128]], axis=1),
            none, none,
        ]
    )
    for w in range(16):
        at = 128 * (w // 2)
        tail = jnp.concatenate([columns[:, at : at + 128], lines], axis=1)
        out[w, 64:80] = jnp.concatenate([tail, jnp.zeros((4, 512), BF)])


def qkv_back_body(dq, dkv, got, w, joined, sums, pa, pb):
    j = jnp.concatenate(
        [dq[...], (dkv[...] + got[...].astype(F32)).astype(BF)], axis=1
    )
    joined[...] = j
    sums[...] = jnp.sum(j.astype(F32), axis=0, keepdims=True)
    m = qkv_matrix(w)
    pa[...] = mm_nt(j[:HALF], m).astype(BF)
    pb[...] = mm_nt(j[HALF:], m).astype(BF)


def by_kind(m):
    parts = [m[:, i * HD : (i + 1) * HD] for i in range(6)]
    return jnp.concatenate([parts[i] for i in (0, 3, 1, 4, 2, 5)], axis=1)


def by_head(m):
    parts = [m[:, i * HD : (i + 1) * HD] for i in range(6)]
    return jnp.concatenate([parts[i] for i in (0, 2, 4, 1, 3, 5)], axis=1)


def from_hbm(body, name, arrays, outs):
    count = len(arrays)

    def kernel(*refs):
        given, made = refs[:count], refs[count : count + len(outs)]
        held, sems = refs[count + len(outs) : -1], refs[-1]
        copies = [
            pltpu.make_async_copy(src, dst, sems.at[i])
            for i, (src, dst) in enumerate(zip(given, held))
        ]
        for copy in copies:
            copy.start()
        for copy in copies:
            copy.wait()
        body(*held, *made)

    return pl.pallas_call(
        kernel,
        in_specs=[pl.BlockSpec(memory_space=pltpu.HBM) for _ in arrays],
        out_specs=[pl.BlockSpec(memory_space=pltpu.VMEM) for _ in outs],
        out_shape=outs,
        scratch_shapes=[pltpu.VMEM(a.shape, a.dtype) for a in arrays]
        + [pltpu.SemaphoreType.DMA((count,))],
        compiler_params=pltpu.CompilerParams(vmem_limit_bytes=50 << 20),
        name=name,
    )(*arrays)


def pack_first_body(qkv, proj, gains, biases, first):
    small = [gains[l, i : i + 1] for l in range(2) for i in range(2)]
    small += [biases[l, i : i + 1] for l in range(2) for i in range(4)]
    lines = jnp.concatenate(
        [jnp.concatenate([small[2 * i], small[2 * i + 1]], axis=1) for i in range(6)]
        + [jnp.zeros((2, 128), BF)]
    )
    own = jnp.concatenate(
        [
            jnp.concatenate([by_kind(qkv[0]), proj[0]], axis=1),
            jnp.concatenate([lines, jnp.zeros((8, 384), BF)], axis=1),
        ]
    )
    for w in range(16):
        first[w] = own


def pack_rest_body(qkv, proj, fc1, fc2, second, third):
    second[:, :512] = fc1[0]
    second[:, 512:1024] = fc2[0]
    second[:, 1024:1152] = jnp.zeros((64, 128), BF)
    second[:, 1152:] = by_kind(qkv[1])
    third[:, :512] = fc1[1]
    third[:, 512:1024] = fc2[1]
    third[:, 1024:] = proj[1]


def sum16(ref, *at):
    total = ref[(0, *at)].astype(F32)
    for w in range(1, 16):
        total += ref[(w, *at)].astype(F32)
    return total


def finish_ffn_body(f0, f1, fc1, fc2):
    for l, total in enumerate((sum16(f0), f1[...].astype(F32))):
        fc1[l] = total[:, :512]
        fc2[l] = total[:, 512:]


def finish_columns_body(odd, mixed, columns):
    own = mixed[0, 64:80, :128].astype(F32)
    for w in range(1, 16):
        own += mixed[w, 64:80, :128].astype(F32)
    columns[...] = jnp.where(odd[0] == 1, own[:12, 64:], own[:12, :64])


def finish_body(mixed, attn1, qkv, proj, qv, up):
    total = sum16(mixed)
    for l, m in enumerate((total[:64], attn1[...].astype(F32))):
        qkv[l] = by_head(m[:, :384])
        proj[l] = m[:, 384:]
    own = total[64:76]
    for l in range(2):
        line = own[l : l + 1, 128:] + own[2 + l : 3 + l, 128:]
        parts = [line[:, i * HD : (i + 1) * HD] for i in (0, 4, 1, 5)]
        qv[l : l + 1] = jnp.concatenate(parts, axis=1)
        near = own[4 + l : 5 + l, 128:] + own[6 + l : 7 + l, 128:]
        at = 128 + 128 * l
        up[l : l + 1] = jnp.concatenate(
            [near, own[8:9, at : at + 128] + own[9:10, at : at + 128]], axis=1
        )


def finish_rows_body(t0, t1, t2, t3, gains, biases):
    total = (t0[...] + t1[...]) + (t2[...] + t3[...])
    for l in range(2):
        gains[l] = total[2 * l : 2 * l + 2]
        biases[l] = total[4 + 4 * l : 8 + 4 * l]


def relative_body(order, x, cot, xr, cr, total):
    for j in range(8):
        row = pl.multiple_of(order[j] * PIECE, PIECE)
        xr[j * PIECE : (j + 1) * PIECE] = x[pl.ds(row, PIECE)]
        cr[j * PIECE : (j + 1) * PIECE] = cot[pl.ds(row, PIECE)]
    total[...] = jnp.sum(cr[:PIECE].astype(F32), axis=0, keepdims=True)


def sequence_body(order, near, far, out):
    for j in range(8):
        row = pl.multiple_of(order[j] * PIECE, PIECE)
        src = near if j < 4 else far
        k = j % 4
        out[pl.ds(row, PIECE)] = src[k * PIECE : (k + 1) * PIECE].astype(out.dtype)


def per_device(
    block_in, qkv_weight, proj_weight, fc1_weight, fc2_weight,
    qv_bias, fc1_bias, norm_gains, row_biases, cotangent,
):
    t = lax.axis_index(T)
    y, c = t // 2, t % 2
    ctx = lax.axis_index("context")
    place = jnp.stack([y, c, ctx]).astype(jnp.int32)
    slope = jnp.exp2(-8.0 * (2 * t + 1 + jnp.arange(2)).astype(F32) / HEADS)
    j = jnp.arange(8)
    order = (2 * ((y - j % 4) % 4) + (c + j // 4) % 2).astype(jnp.int32)
    half = (HALF, D)
    qs, kvs, hs, js = (ROWS, 128), (ROWS, 256), (ROWS, 512), (ROWS, 384)

    (first,) = from_hbm(
        pack_first_body, "pack_first", [qkv_weight, proj_weight, norm_gains, row_biases],
        [sds((16, 72, 512), BF)],
    )
    first, fc1_weight = tie(first, fc1_weight)
    first_all = lax.all_to_all(first, W, 0, 0)
    second_part, third_part = from_hbm(
        pack_rest_body, "pack_rest", [qkv_weight, proj_weight, fc1_weight, fc2_weight],
        [sds((64, 1536), BF), sds((64, 1152), BF)],
    )
    second_all = lax.all_gather(second_part, W, axis=0, tiled=True)
    third_all = lax.all_gather(third_part, W, axis=0, tiled=True)
    table = (
        first_all[:, 64:70, :128].reshape(16, 12, 64).transpose(1, 0, 2).reshape(12, D).astype(F32)
    )
    tab = (table, (12, D), None)
    whole_first = (first_all, (16, 72, 512), None)
    qv = qv_bias.astype(F32).reshape(2, 2, 2, HD).transpose(0, 2, 1, 3)
    zero = jnp.zeros((2, 1, 2, HD), F32)
    joined_bias = jnp.concatenate([qv[:, :1], zero, qv[:, 1:]], axis=1).reshape(2, 1, 384)
    up_bias = fc1_bias.astype(F32).reshape(2, 1, 512)

    x, cot, b13 = call(
        relative_body, "to_relative",
        [(order, None, None), (block_in.reshape(ROWS, D), (ROWS, D), None), (cotangent.reshape(ROWS, D), (ROWS, D), None)],
        [sds((ROWS, D), BF), sds((ROWS, D), BF), sds((1, D), F32)],
    )

    saved = []
    stream = x
    qkv_of = (whole_first, (second_all, (D, 384), (0, 3)))
    proj_of = (whole_first, (third_all, (D, 128), (0, 8)))
    fc1_of = [(m, (D, 512), (0, 0)) for m in (second_all, third_all)]
    fc2_of = [(m, (D, 512), (0, 1)) for m in (second_all, third_all)]

    where = [(place, None, None), (slope, None, None)]
    for l in range(2):
        bias = (joined_bias[l], (1, 384), None)
        if l == 0:
            na, nb, kv = call(
                kv_first_body, "kv_first",
                [(x, half, (0, 0)), (x, half, (1, 0)), whole_first, tab, bias],
                [sds(half, BF), sds(half, BF), sds(kvs, BF)],
            )
        else:
            na, nb = gather_rows(normed)
            (kv,) = call(
                kv_body, "kv", [(na, half, None), (nb, half, None), qkv_of[l], bias], [sds(kvs, BF)]
            )
        kvo = lax.ppermute(kv, "context", [(0, 1)])
        (q,) = call(
            q_body, "q", [(na, half, None), (nb, half, None), qkv_of[l], bias], [sds(qs, BF)]
        )
        own, own_top, own_total = call(
            attend_own_body, "attend_own", where + [(q, qs, None), (kv, kvs, None)], [sds(qs, F32)] * 3
        )
        att, lse, pa, pb = call(
            attend_body, "attend",
            where + [(q, qs, None), (kvo, kvs, None), proj_of[l]] + [(v, qs, None) for v in (own, own_top, own_total)],
            [sds(qs, BF), sds(qs, F32), sds(half, BF), sds(half, BF)],
        )
        middle, second = norm_fwd(
            sum_pieces(pa, pb), stream, table, (l, 1), ((l, 1), (l, 2))
        )
        sa, sb = gather_rows(second)
        act, dgel, pa, pb = call(
            ffn_body, "ffn",
            [(sa, half, None), (sb, half, None), fc1_of[l], fc2_of[l], (up_bias[l], (1, 512), None)],
            [sds(hs, BF), sds(hs, BF), sds(half, BF), sds(half, BF)],
        )
        saved.append((stream, na, nb, q, kv, kvo, att, lse, middle, sa, sb, act, dgel))
        if l == 0:
            stream, normed = norm_fwd(
                sum_pieces(pa, pb), middle, table, (0, 3), ((1, 0), (1, 0))
            )
    out_own = out_rows(sum_pieces(pa, pb), middle, table)

    grad = cot
    ea = (cot, half, (0, 0))
    eb = (cot, half, (1, 0))
    for l in (1, 0):
        stream, na, nb, q, kv, kvo, att, lse, middle, sa, sb, act, dgel = saved[l]
        hg, up_sum, pa, pb = call(
            ffn_back_body, "ffn_back",
            [ea, eb, fc1_of[l], fc2_of[l], (dgel, hs, None)],
            [sds(hs, BF), sds((1, 512), F32), sds(half, BF), sds(half, BF)],
        )
        pieces = sum_pieces(pa, pb)
        ffn_ops = [ea, eb, (act, hs, None), (sa, half, None), (sb, half, None), (hg, hs, None)]
        if l == 1:
            pieces, out_own = tie(pieces, out_own)
        else:
            (ffn_grad,) = call(ffn_weights_body, "ffn_weights", ffn_ops, [sds((D, D), BF)])
            pieces, ffn_grad = tie(pieces, ffn_grad)
            ffn_pieces = lax.all_to_all(ffn_grad.reshape(16, 64, D), W, 0, 0)
        mid, mid_low, s2 = norm_bwd(pieces, middle, grad, table, (l, 1))
        ma, mb = gather_rows(mid_low)
        do, dq, dkvo = call(
            back_earlier_body, "back_earlier",
            where
            + [(ma, half, None), (mb, half, None), proj_of[l], (q, qs, None), (kvo, kvs, None), (lse, qs, None), (att, qs, None)],
            [sds(qs, BF), sds(qs, F32), sds(kvs, BF)],
        )
        got = lax.ppermute(dkvo, "context", [(1, 0)])
        dq, dkv = call(
            back_own_body, "back_own",
            where
            + [(do, qs, None), (q, qs, None), (kv, kvs, None), (lse, qs, None), (att, qs, None), (dq, qs, None)],
            [sds(qs, BF), sds(kvs, F32)],
        )
        if l == 1:
            dkv, out_own = tie(dkv, out_own)
            oa, ob = gather_rows(out_own)
        else:
            dkv, oa = tie(dkv, oa)
            (block_out,) = call(
                sequence_body, "to_sequence",
                [(order, None, None), (oa, half, None), (ob, half, None)],
                [sds((ROWS, D), BF)],
            )
            got, block_out, ffn_pieces = tie(got, block_out, ffn_pieces)
        joined, qv_sum, pa, pb = call(
            qkv_back_body, "qkv_back",
            [(dq, qs, None), (dkv, kvs, None), (got, kvs, None), qkv_of[l]],
            [sds(js, BF), sds((1, 384), F32), sds(half, BF), sds(half, BF)],
        )
        pieces = sum_pieces(pa, pb)
        attn_ops = [(na, half, None), (nb, half, None), (joined, js, None), (ma, half, None), (mb, half, None), (att, qs, None)]
        if l == 1:
            (weights_grad,) = call(
                layer_weights_body, "layer_weights", ffn_ops + attn_ops, [sds((D, 1536), BF)]
            )
            pieces, oa, weights_grad = tie(pieces, oa, weights_grad)
            owned1 = lax.psum_scatter(weights_grad, W, scatter_dimension=0, tiled=True)
            up1, qv1, s21 = up_sum, qv_sum, s2
            grad, low, s11 = norm_bwd(pieces, stream, mid, table, (1, 0))
            near, far = gather_rows(low)
            ea, eb = (near, half, None), (far, half, None)
        else:
            three, one = (3, D), (1, D)
            (packed,) = call(
                last_pack_body, "last_pack",
                attn_ops
                + [(pa, half, None), (pb, half, None), (x, half, (0, 0)), (x, half, (1, 0))]
                + [(s21, three, None), (s11, three, None), (s2, three, None), (b13, one, None)]
                + [(up_sum, (1, 512), None), (up1, (1, 512), None), (qv_sum, (1, 384), None), (qv1, (1, 384), None)],
                [sds((16, 80, 512), BF)],
            )
            mixed = lax.all_to_all(packed, W, 0, 0)
            _, low, _ = norm_bwd(pieces, stream, mid, table, (0, 0))
            near, far = gather_rows(low)
            near, ffn_pieces = tie(near, ffn_pieces)
            fc1_grad, fc2_grad = call(
                finish_ffn_body, "finish_ffn",
                [(ffn_pieces, (16, 64, D), None), (owned1, (64, D), (0, 0))],
                [sds((2, 64, 512), F32), sds((2, 64, 512), F32)],
            )
            (input_grad,) = call(
                sequence_body, "to_sequence",
                [(order, None, None), (near, half, None), (far, half, None)],
                [sds((ROWS, D), F32)],
            )
    odd = ctx.astype(jnp.int32).reshape(1)
    small = (12, 64)
    (tail,) = call(
        finish_columns_body, "finish_columns",
        [(odd, None, None), (mixed, (16, 80, 512), None)],
        [sds(small, F32)],
    )
    tail = tail + core_swap(tail)
    tails = [tail] + [along_y(tail, step) for step in (1, 2, 3)]
    qkv_grad, proj_grad, qv_grad, up_grad = call(
        finish_body, "finish",
        [(mixed, (16, 80, 512), None), (owned1, (64, 512), (0, 2))],
        [sds((2, 64, 384), F32), sds((2, 64, 128), F32), sds((2, 256), F32), sds((2, 512), F32)],
    )
    gains_grad, biases_grad = call(
        finish_rows_body, "finish_rows",
        [(v, small, None) for v in tails],
        [sds((2, 2, 64), F32), sds((2, 4, 64), F32)],
    )
    return (
        block_out[None], input_grad[None], qkv_grad, proj_grad, fc1_grad, fc2_grad,
        qv_grad, up_grad, gains_grad, biases_grad,
    )


def solution(mesh):
    return jax.shard_map(
        per_device,
        mesh=mesh,
        in_specs=(
            P("shard", "context", None),
            P(None, W, T),
            P(None, W, T),
            P(None, W, T),
            P(None, W, T),
            P(None, T),
            P(None, T),
            P(None, None, W),
            P(None, None, W),
            P("shard", "context", None),
        ),
        out_specs=(
            P("shard", "context", None),
            P("shard", "context", None),
            P(None, W, T),
            P(None, W, T),
            P(None, W, T),
            P(None, W, T),
            P(None, T),
            P(None, T),
            P(None, None, W),
            P(None, None, W),
        ),
        check_vma=False,
    )
```

```python
import jax
import jax.numpy as jnp
from jax import lax
from jax.experimental import pallas as pl
from jax.experimental.pallas import tpu as pltpu
from jax.sharding import PartitionSpec as P

HEADS = 16
HD = 64
NORM_EPS = 1e-05
GELU_SCALE = 0.7978845608028654
GELU_CUBE = 0.044715
F32 = jnp.float32
BF = jnp.bfloat16
W = ("shard", "context")
T = "tensor"
ROWS = 512
HALF = 256
PIECE = 64
D = 1024
NEG = -1e30
ROOM = {
    "kv_first": 10, "kv": 8, "q": 8, "attend_own": 12, "attend": 12, "ffn": 14, "ffn_back": 12,
    "back_earlier": 14, "back_own": 12, "qkv_back": 10, "ffn_weights": 14, "layer_weights": 20,
    "last_pack": 16, "to_relative": 8, "to_sequence": 8, "finish_ffn": 8,
}


def spec(shape, index=None):
    place = tuple(index) if index is not None else (0,) * len(shape)
    return pl.BlockSpec(shape, lambda i: place)


def smem():
    return pl.BlockSpec(memory_space=pltpu.SMEM)


def call(body, name, operands, outs):
    in_specs, args = [], []
    for array, shape, index in operands:
        in_specs.append(smem() if shape is None else spec(shape, index))
        args.append(array)
    return pl.pallas_call(
        body,
        grid=(1,),
        in_specs=in_specs,
        out_specs=[spec(o.shape) for o in outs],
        out_shape=outs,
        compiler_params=pltpu.CompilerParams(vmem_limit_bytes=ROOM.get(name, 6) << 20),
        name=name,
    )(*args)


def sds(shape, dtype):
    return jax.ShapeDtypeStruct(shape, dtype)


def mm(a, b):
    return lax.dot_general(a, b, (((1,), (0,)), ((), ())), preferred_element_type=F32)


def mm_nt(a, b):
    return lax.dot_general(a, b, (((1,), (1,)), ((), ())), preferred_element_type=F32)


def mm_tn(a, b):
    return lax.dot_general(a, b, (((0,), (0,)), ((), ())), preferred_element_type=F32)


def core_swap(v):
    return lax.ppermute(v, T, [(i, i ^ 1) for i in range(8)])


def along_y(v, step):
    return lax.ppermute(
        v, T, [(2 * y + c, 2 * ((y + step) % 4) + c) for y in range(4) for c in range(2)]
    )


def add_body(pa, got, h0, h1, h2, h3):
    both = pa[...].astype(F32) + got[...].astype(F32)
    h0[...] = both[:PIECE]
    h1[...] = both[PIECE : 2 * PIECE].astype(BF)
    h2[...] = both[2 * PIECE : 3 * PIECE].astype(BF)
    h3[...] = both[3 * PIECE :].astype(BF)


def tie(*values):
    return lax.optimization_barrier(values)


def chip_sums(keep, send):
    got = core_swap(send)
    return call(
        add_body,
        "pair_add",
        [(keep, (HALF, D), None), (got, (HALF, D), None)],
        [sds((PIECE, D), F32)] + [sds((PIECE, D), BF)] * 3,
    )


def spread(sums):
    h0, h1, h2, h3 = sums
    r2 = along_y(h2, -2)
    r1 = along_y(h1, -1)
    r3 = along_y(h3, -3)
    return h0, r1, r2, r3


def sum_pieces(keep, send):
    return spread(chip_sums(keep, send))


def gather_rows(own):
    r2 = along_y(own, 2)
    r1 = along_y(own, 1)
    r3 = along_y(own, 3)
    near = jnp.concatenate([own, r1, r2, r3], axis=0)
    far = core_swap(near)
    return near, far


def norm_parts(v):
    mean = jnp.mean(v, axis=-1, keepdims=True)
    centred = v - mean
    var = jnp.mean(centred * centred, axis=-1, keepdims=True)
    s = lax.rsqrt(var + NORM_EPS)
    return centred * s, s


def gain_row(table, l, i):
    at = 2 * l + i
    return table[at : at + 1]


def bias_row(table, l, i):
    at = 4 + 4 * l + i
    return table[at : at + 1]


def norm_fwd(pieces, resid, table, bias_at, next_at):
    def body(h0, r1, r2, r3, resid_ref, rows, stream, normed):
        v = (
            h0[...] + r1[...].astype(F32) + r2[...].astype(F32) + r3[...].astype(F32)
        ) + resid_ref[...].astype(F32) + bias_row(rows, *bias_at)
        stream[...] = v
        xhat, _ = norm_parts(v)
        gain, shift = next_at
        normed[...] = (xhat * gain_row(rows, *gain) + bias_row(rows, *shift)).astype(BF)

    b = (PIECE, D)
    return call(
        body,
        "norm_fwd",
        [(p, b, None) for p in (*pieces, resid)] + [(table, (12, D), None)],
        [sds(b, F32), sds(b, BF)],
    )


def out_rows(pieces, resid, table):
    def body(h0, r1, r2, r3, resid_ref, rows, out):
        out[...] = (
            (h0[...] + r1[...].astype(F32) + r2[...].astype(F32) + r3[...].astype(F32))
            + resid_ref[...]
            + bias_row(rows, 1, 3)
        ).astype(BF)

    b = (PIECE, D)
    return call(
        body,
        "out_rows",
        [(p, b, None) for p in (*pieces, resid)] + [(table, (12, D), None)],
        [sds(b, BF)],
    )[0]


def norm_bwd(pieces, stream, grad, table, gain_at):
    def body(h0, r1, r2, r3, stream_ref, grad_ref, rows, out, low, sums):
        g = h0[...] + r1[...].astype(F32) + r2[...].astype(F32) + r3[...].astype(F32)
        xhat, s = norm_parts(stream_ref[...].astype(F32))
        gx = g * xhat
        c = g * gain_row(rows, *gain_at)
        cx = c * xhat
        e = grad_ref[...].astype(F32) + s * (
            c
            - jnp.mean(c, axis=-1, keepdims=True)
            - xhat * jnp.mean(cx, axis=-1, keepdims=True)
        )
        out[...] = e
        low[...] = e.astype(BF)
        sums[0:1] = jnp.sum(gx, axis=0, keepdims=True)
        sums[1:2] = jnp.sum(g, axis=0, keepdims=True)
        sums[2:3] = jnp.sum(e, axis=0, keepdims=True)

    b = (PIECE, D)
    return call(
        body,
        "norm_bwd",
        [(p, b, None) for p in (*pieces, stream, grad)] + [(table, (12, D), None)],
        [sds(b, F32), sds(b, BF), sds((3, D), F32)],
    )


def kv_first_body(xa, xb, first, rows, bias, na, nb, kv):
    w = qkv_matrix(first)[:, 128:]
    for x, n, at in ((xa, na, 0), (xb, nb, HALF)):
        xhat, _ = norm_parts(x[...].astype(F32))
        normed = (xhat * gain_row(rows, 0, 0) + bias_row(rows, 0, 0)).astype(BF)
        n[...] = normed
        kv[at : at + HALF] = (mm(normed, w) + bias[:, 128:]).astype(BF)


def kv_body(na, nb, w, bias, kv):
    for n, at in ((na, 0), (nb, HALF)):
        kv[at : at + HALF] = (mm(n[...], w[:, 128:]) + bias[:, 128:]).astype(BF)


def q_body(na, nb, w, bias, q):
    m = qkv_matrix(w)[:, :128]
    for n, at in ((na, 0), (nb, HALF)):
        q[at : at + HALF] = (mm(n[...], m) + bias[:, :128]).astype(BF)


def proj_matrix(ref):
    return ref[:, :64, 384:].reshape(D, 128) if len(ref.shape) == 3 else ref[...]


def qkv_matrix(ref):
    return ref[:, :64, :384].reshape(D, 384) if len(ref.shape) == 3 else ref[...]


def places(place, shape, axis):
    r = lax.broadcasted_iota(jnp.int32, shape, axis)
    y, c = place[0], place[1]
    return ((y - ((r >> 6) & 3)) & 3) * 128 + ((c + (r >> 8)) & 1) * 64 + (r & 63)


def own_scores(place, slope, h, qh, kh, mask):
    pos = places(place, (1, ROWS), 1).astype(F32)
    return jnp.where(mask, mm_nt(qh, kh) * 0.125 + slope[h] * pos, NEG)


def earlier_scores(place, slope, h, qh, kh):
    pos = places(place, (1, ROWS), 1).astype(F32)
    off = jnp.where(place[2] == 1, 0.0, NEG)
    return mm_nt(qh, kh) * 0.125 + (slope[h] * (pos - 512.0) + off)


def own_mask(place):
    return places(place, (ROWS, 1), 0) >= places(place, (1, ROWS), 1)


def attend_own_body(place, slope, q, kv, out, top, total):
    mask = own_mask(place)
    for h in range(2):
        lo, hi = h * HD, (h + 1) * HD
        s = own_scores(place, slope, h, q[:, lo:hi], kv[:, lo:hi], mask)
        m = jnp.max(s, axis=-1, keepdims=True)
        p = jnp.exp(s - m)
        out[:, lo:hi] = mm(p.astype(BF), kv[:, 128 + lo : 128 + hi])
        top[:, lo:hi] = jnp.broadcast_to(m, (ROWS, HD))
        total[:, lo:hi] = jnp.broadcast_to(jnp.sum(p, axis=-1, keepdims=True), (ROWS, HD))


def attend_body(place, slope, q, kvo, pw, own, own_top, own_total, att, lse, pa, pb):
    outs, logs = [], []
    for h in range(2):
        lo, hi = h * HD, (h + 1) * HD
        s = earlier_scores(place, slope, h, q[:, lo:hi], kvo[:, lo:hi])
        m = own_top[:, lo : lo + 1]
        top = jnp.maximum(m, jnp.max(s, axis=-1, keepdims=True))
        p = jnp.exp(s - top)
        scale = jnp.exp(m - top)
        total = own_total[:, lo : lo + 1] * scale + jnp.sum(p, axis=-1, keepdims=True)
        o = own[:, lo:hi] * scale + mm(p.astype(BF), kvo[:, 128 + lo : 128 + hi])
        outs.append(o / total)
        logs.append(jnp.broadcast_to(top + jnp.log(total), (ROWS, HD)))
    attended = jnp.concatenate(outs, axis=1).astype(BF)
    att[...] = attended
    lse[...] = jnp.concatenate(logs, axis=1)
    w = proj_matrix(pw)
    pa[...] = mm_nt(attended[:HALF], w).astype(BF)
    pb[...] = mm_nt(attended[HALF:], w).astype(BF)


def score_grads(p, doh, vh, atth):
    delta = jnp.sum(doh.astype(F32) * atth.astype(F32), axis=-1, keepdims=True)
    return (p * (mm_nt(doh, vh) - delta)).astype(BF)


def back_earlier_body(place, slope, ma, mb, pw, q, kvo, lse, att, do_ref, dq, dkvo):
    w = proj_matrix(pw)
    do = jnp.concatenate([mm(ma[...], w), mm(mb[...], w)], axis=0).astype(BF)
    do_ref[...] = do
    dqs, dks, dvs = [], [], []
    for h in range(2):
        lo, hi = h * HD, (h + 1) * HD
        qh, kh, vh, doh = q[:, lo:hi], kvo[:, lo:hi], kvo[:, 128 + lo : 128 + hi], do[:, lo:hi]
        p = jnp.exp(earlier_scores(place, slope, h, qh, kh) - lse[:, lo : lo + 1])
        d = score_grads(p, doh, vh, att[:, lo:hi])
        dqs.append(mm(d, kh) * 0.125)
        dks.append(mm_tn(d, qh) * 0.125)
        dvs.append(mm_tn(p.astype(BF), doh))
    dq[...] = jnp.concatenate(dqs, axis=1)
    dkvo[...] = jnp.concatenate(dks + dvs, axis=1).astype(BF)


def back_own_body(place, slope, do, q, kv, lse, att, dq_part, dq, dkv):
    mask = own_mask(place)
    dqs, dks, dvs = [], [], []
    for h in range(2):
        lo, hi = h * HD, (h + 1) * HD
        qh, kh, vh, doh = q[:, lo:hi], kv[:, lo:hi], kv[:, 128 + lo : 128 + hi], do[:, lo:hi]
        p = jnp.exp(own_scores(place, slope, h, qh, kh, mask) - lse[:, lo : lo + 1])
        d = score_grads(p, doh, vh, att[:, lo:hi])
        dqs.append(mm(d, kh) * 0.125)
        dks.append(mm_tn(d, qh) * 0.125)
        dvs.append(mm_tn(p.astype(BF), doh))
    dq[...] = (dq_part[...] + jnp.concatenate(dqs, axis=1)).astype(BF)
    dkv[...] = jnp.concatenate(dks + dvs, axis=1)


def ffn_body(na, nb, w1, w2, bias, act, dgel, pa, pb):
    for n, p, at in ((na, pa, 0), (nb, pb, HALF)):
        v = mm(n[...], w1[...]) + bias[...]
        v2 = v * v
        th = jnp.tanh(GELU_SCALE * (v + GELU_CUBE * (v2 * v)))
        one = 0.5 + 0.5 * th
        a = (v * one).astype(BF)
        act[at : at + HALF] = a
        dgel[at : at + HALF] = (
            one
            + (0.5 * GELU_SCALE) * v * (1.0 - th * th) * (1.0 + (3.0 * GELU_CUBE) * v2)
        ).astype(BF)
        p[...] = mm_nt(a, w2[...]).astype(BF)


def ffn_back_body(ea, eb, w1, w2, dgel, hg, sums, pa, pb):
    total = jnp.zeros((1, 512), F32)
    for e, p, at in ((ea, pa, 0), (eb, pb, HALF)):
        g = (mm(e[...], w2[...]) * dgel[at : at + HALF].astype(F32)).astype(BF)
        hg[at : at + HALF] = g
        total += jnp.sum(g.astype(F32), axis=0, keepdims=True)
        p[...] = mm_nt(g, w1[...]).astype(BF)
    sums[...] = total


def ffn_weights_body(ea, eb, act, na, nb, hg, out):
    out[:, :512] = (mm_tn(na[...], hg[:HALF]) + mm_tn(nb[...], hg[HALF:])).astype(BF)
    out[:, 512:] = (mm_tn(ea[...], act[:HALF]) + mm_tn(eb[...], act[HALF:])).astype(BF)


def attn_weights_body(na, nb, joined, ma, mb, att, out):
    out[:, :384] = (
        mm_tn(na[...], joined[:HALF]) + mm_tn(nb[...], joined[HALF:])
    ).astype(BF)
    out[:, 384:] = (mm_tn(ma[...], att[:HALF]) + mm_tn(mb[...], att[HALF:])).astype(BF)


def layer_weights_body(ea, eb, act, sa, sb, hg, na, nb, joined, ma, mb, att, out):
    ffn_weights_body(ea, eb, act, sa, sb, hg, out.at[:, :1024])
    attn_weights_body(na, nb, joined, ma, mb, att, out.at[:, 1024:])


def two_halves(v):
    high = v.astype(BF)
    return high, (v - high.astype(F32)).astype(BF)


def last_pack_body(
    na, nb, joined, ma, mb, att, pa, pb, xa, xb, s21, s11, s20, b13,
    up0, up1, qv0, qv1, out,
):
    g = (mm_tn(na[...], joined[:HALF]) + mm_tn(nb[...], joined[HALF:])).astype(BF)
    out[:, :64, :384] = g.reshape(16, 64, 384)
    g = (mm_tn(ma[...], att[:HALF]) + mm_tn(mb[...], att[HALF:])).astype(BF)
    out[:, :64, 384:] = g.reshape(16, 64, 128)
    gain = jnp.zeros((1, D), F32)
    shift = jnp.zeros((1, D), F32)
    for p, x in ((pa, xa), (pb, xb)):
        g = p[...].astype(F32)
        xhat, _ = norm_parts(x[...].astype(F32))
        gain += jnp.sum(g * xhat, axis=0, keepdims=True)
        shift += jnp.sum(g, axis=0, keepdims=True)
    columns = jnp.concatenate(
        [
            gain, s20[0:1], s11[0:1], s21[0:1],
            shift, s20[2:3], s20[1:2], s11[2:3], s11[1:2], s21[2:3], s21[1:2], b13[...],
        ]
    ).astype(BF)
    q0, q0l = two_halves(qv0[...])
    q1, q1l = two_halves(qv1[...])
    u0, u0l = two_halves(up0[...])
    u1, u1l = two_halves(up1[...])
    none = jnp.zeros((1, 384), BF)
    lines = jnp.concatenate(
        [
            q0, q1, q0l, q1l,
            u0[:, :384], u1[:, :384], u0l[:, :384], u1l[:, :384],
            jnp.concatenate([u0[:, 384:], u1[:, 384:], none[:, :128]], axis=1),
            jnp.concatenate([u0l[:, 384:], u1l[:, 384:], none[:, :128]], axis=1),
            none, none,
        ]
    )
    for w in range(16):
        at = 128 * (w // 2)
        tail = jnp.concatenate([columns[:, at : at + 128], lines], axis=1)
        out[w, 64:80] = jnp.concatenate([tail, jnp.zeros((4, 512), BF)])


def qkv_back_body(dq, dkv, got, w, joined, sums, pa, pb):
    j = jnp.concatenate(
        [dq[...], (dkv[...] + got[...].astype(F32)).astype(BF)], axis=1
    )
    joined[...] = j
    sums[...] = jnp.sum(j.astype(F32), axis=0, keepdims=True)
    m = qkv_matrix(w)
    pa[...] = mm_nt(j[:HALF], m).astype(BF)
    pb[...] = mm_nt(j[HALF:], m).astype(BF)


def by_kind(m):
    parts = [m[:, i * HD : (i + 1) * HD] for i in range(6)]
    return jnp.concatenate([parts[i] for i in (0, 3, 1, 4, 2, 5)], axis=1)


def by_head(m):
    parts = [m[:, i * HD : (i + 1) * HD] for i in range(6)]
    return jnp.concatenate([parts[i] for i in (0, 2, 4, 1, 3, 5)], axis=1)


def from_hbm(body, name, arrays, outs):
    count = len(arrays)

    def kernel(*refs):
        given, made = refs[:count], refs[count : count + len(outs)]
        held, sems = refs[count + len(outs) : -1], refs[-1]
        copies = [
            pltpu.make_async_copy(src, dst, sems.at[i])
            for i, (src, dst) in enumerate(zip(given, held))
        ]
        for copy in copies:
            copy.start()
        for copy in copies:
            copy.wait()
        body(*held, *made)

    return pl.pallas_call(
        kernel,
        in_specs=[pl.BlockSpec(memory_space=pltpu.HBM) for _ in arrays],
        out_specs=[pl.BlockSpec(memory_space=pltpu.VMEM) for _ in outs],
        out_shape=outs,
        scratch_shapes=[pltpu.VMEM(a.shape, a.dtype) for a in arrays]
        + [pltpu.SemaphoreType.DMA((count,))],
        compiler_params=pltpu.CompilerParams(vmem_limit_bytes=ROOM.get(name, 6) << 20),
        name=name,
    )(*arrays)


def pack_first_body(qkv, proj, gains, biases, first):
    small = [gains[l, i : i + 1] for l in range(2) for i in range(2)]
    small += [biases[l, i : i + 1] for l in range(2) for i in range(4)]
    lines = jnp.concatenate(
        [jnp.concatenate([small[2 * i], small[2 * i + 1]], axis=1) for i in range(6)]
        + [jnp.zeros((2, 128), BF)]
    )
    own = jnp.concatenate(
        [
            jnp.concatenate([by_kind(qkv[0]), proj[0]], axis=1),
            jnp.concatenate([lines, jnp.zeros((8, 384), BF)], axis=1),
        ]
    )
    for w in range(16):
        first[w] = own


def pack_rest_body(qkv, proj, fc1, fc2, second, third):
    second[:, :512] = fc1[0]
    second[:, 512:1024] = fc2[0]
    second[:, 1024:1152] = jnp.zeros((64, 128), BF)
    second[:, 1152:] = by_kind(qkv[1])
    third[:, :512] = fc1[1]
    third[:, 512:1024] = fc2[1]
    third[:, 1024:] = proj[1]


def sum16(ref, *at):
    total = ref[(0, *at)].astype(F32)
    for w in range(1, 16):
        total += ref[(w, *at)].astype(F32)
    return total


def finish_ffn_body(f0, f1, fc1, fc2):
    for l, total in enumerate((sum16(f0), f1[...].astype(F32))):
        fc1[l] = total[:, :512]
        fc2[l] = total[:, 512:]


def finish_columns_body(odd, mixed, columns):
    own = mixed[0, 64:80, :128].astype(F32)
    for w in range(1, 16):
        own += mixed[w, 64:80, :128].astype(F32)
    columns[...] = jnp.where(odd[0] == 1, own[:12, 64:], own[:12, :64])


def finish_body(mixed, attn1, qkv, proj, qv, up):
    total = sum16(mixed)
    for l, m in enumerate((total[:64], attn1[...].astype(F32))):
        qkv[l] = by_head(m[:, :384])
        proj[l] = m[:, 384:]
    own = total[64:76]
    for l in range(2):
        line = own[l : l + 1, 128:] + own[2 + l : 3 + l, 128:]
        parts = [line[:, i * HD : (i + 1) * HD] for i in (0, 4, 1, 5)]
        qv[l : l + 1] = jnp.concatenate(parts, axis=1)
        near = own[4 + l : 5 + l, 128:] + own[6 + l : 7 + l, 128:]
        at = 128 + 128 * l
        up[l : l + 1] = jnp.concatenate(
            [near, own[8:9, at : at + 128] + own[9:10, at : at + 128]], axis=1
        )


def finish_rows_body(t0, t1, t2, t3, gains, biases):
    total = (t0[...] + t1[...]) + (t2[...] + t3[...])
    for l in range(2):
        gains[l] = total[2 * l : 2 * l + 2]
        biases[l] = total[4 + 4 * l : 8 + 4 * l]


def relative_body(order, x, cot, xr, cr, total):
    for j in range(8):
        row = pl.multiple_of(order[j] * PIECE, PIECE)
        xr[j * PIECE : (j + 1) * PIECE] = x[pl.ds(row, PIECE)]
        cr[j * PIECE : (j + 1) * PIECE] = cot[pl.ds(row, PIECE)]
    total[...] = jnp.sum(cr[:PIECE].astype(F32), axis=0, keepdims=True)


def sequence_body(order, near, far, out):
    for j in range(8):
        row = pl.multiple_of(order[j] * PIECE, PIECE)
        src = near if j < 4 else far
        k = j % 4
        out[pl.ds(row, PIECE)] = src[k * PIECE : (k + 1) * PIECE].astype(out.dtype)


def per_device(
    block_in, qkv_weight, proj_weight, fc1_weight, fc2_weight,
    qv_bias, fc1_bias, norm_gains, row_biases, cotangent,
):
    t = lax.axis_index(T)
    y, c = t // 2, t % 2
    ctx = lax.axis_index("context")
    place = jnp.stack([y, c, ctx]).astype(jnp.int32)
    slope = jnp.exp2(-8.0 * (2 * t + 1 + jnp.arange(2)).astype(F32) / HEADS)
    j = jnp.arange(8)
    order = (2 * ((y - j % 4) % 4) + (c + j // 4) % 2).astype(jnp.int32)
    half = (HALF, D)
    qs, kvs, hs, js = (ROWS, 128), (ROWS, 256), (ROWS, 512), (ROWS, 384)

    (first,) = from_hbm(
        pack_first_body, "pack_first", [qkv_weight, proj_weight, norm_gains, row_biases],
        [sds((16, 72, 512), BF)],
    )
    first, fc1_weight = tie(first, fc1_weight)
    first_all = lax.all_to_all(first, W, 0, 0)
    second_part, third_part = from_hbm(
        pack_rest_body, "pack_rest", [qkv_weight, proj_weight, fc1_weight, fc2_weight],
        [sds((64, 1536), BF), sds((64, 1152), BF)],
    )
    second_all = lax.all_gather(second_part, W, axis=0, tiled=True)
    third_all = lax.all_gather(third_part, W, axis=0, tiled=True)
    table = (
        first_all[:, 64:70, :128].reshape(16, 12, 64).transpose(1, 0, 2).reshape(12, D).astype(F32)
    )
    tab = (table, (12, D), None)
    whole_first = (first_all, (16, 72, 512), None)
    qv = qv_bias.astype(F32).reshape(2, 2, 2, HD).transpose(0, 2, 1, 3)
    zero = jnp.zeros((2, 1, 2, HD), F32)
    joined_bias = jnp.concatenate([qv[:, :1], zero, qv[:, 1:]], axis=1).reshape(2, 1, 384)
    up_bias = fc1_bias.astype(F32).reshape(2, 1, 512)

    x, cot, b13 = call(
        relative_body, "to_relative",
        [(order, None, None), (block_in.reshape(ROWS, D), (ROWS, D), None), (cotangent.reshape(ROWS, D), (ROWS, D), None)],
        [sds((ROWS, D), BF), sds((ROWS, D), BF), sds((1, D), F32)],
    )

    saved = []
    stream = x
    qkv_of = (whole_first, (second_all, (D, 384), (0, 3)))
    proj_of = (whole_first, (third_all, (D, 128), (0, 8)))
    fc1_of = [(m, (D, 512), (0, 0)) for m in (second_all, third_all)]
    fc2_of = [(m, (D, 512), (0, 1)) for m in (second_all, third_all)]

    where = [(place, None, None), (slope, None, None)]
    for l in range(2):
        bias = (joined_bias[l], (1, 384), None)
        if l == 0:
            na, nb, kv = call(
                kv_first_body, "kv_first",
                [(x, half, (0, 0)), (x, half, (1, 0)), whole_first, tab, bias],
                [sds(half, BF), sds(half, BF), sds(kvs, BF)],
            )
        else:
            na, nb = gather_rows(normed)
            (kv,) = call(
                kv_body, "kv", [(na, half, None), (nb, half, None), qkv_of[l], bias], [sds(kvs, BF)]
            )
        kvo = lax.ppermute(kv, "context", [(0, 1)])
        (q,) = call(
            q_body, "q", [(na, half, None), (nb, half, None), qkv_of[l], bias], [sds(qs, BF)]
        )
        own, own_top, own_total = call(
            attend_own_body, "attend_own", where + [(q, qs, None), (kv, kvs, None)], [sds(qs, F32)] * 3
        )
        att, lse, pa, pb = call(
            attend_body, "attend",
            where + [(q, qs, None), (kvo, kvs, None), proj_of[l]] + [(v, qs, None) for v in (own, own_top, own_total)],
            [sds(qs, BF), sds(qs, F32), sds(half, BF), sds(half, BF)],
        )
        middle, second = norm_fwd(
            sum_pieces(pa, pb), stream, table, (l, 1), ((l, 1), (l, 2))
        )
        sa, sb = gather_rows(second)
        act, dgel, pa, pb = call(
            ffn_body, "ffn",
            [(sa, half, None), (sb, half, None), fc1_of[l], fc2_of[l], (up_bias[l], (1, 512), None)],
            [sds(hs, BF), sds(hs, BF), sds(half, BF), sds(half, BF)],
        )
        saved.append((stream, na, nb, q, kv, kvo, att, lse, middle, sa, sb, act, dgel))
        if l == 0:
            stream, normed = norm_fwd(
                sum_pieces(pa, pb), middle, table, (0, 3), ((1, 0), (1, 0))
            )
    out_own = out_rows(sum_pieces(pa, pb), middle, table)

    grad = cot
    ea = (cot, half, (0, 0))
    eb = (cot, half, (1, 0))
    for l in (1, 0):
        stream, na, nb, q, kv, kvo, att, lse, middle, sa, sb, act, dgel = saved[l]
        hg, up_sum, pa, pb = call(
            ffn_back_body, "ffn_back",
            [ea, eb, fc1_of[l], fc2_of[l], (dgel, hs, None)],
            [sds(hs, BF), sds((1, 512), F32), sds(half, BF), sds(half, BF)],
        )
        pieces = sum_pieces(pa, pb)
        ffn_ops = [ea, eb, (act, hs, None), (sa, half, None), (sb, half, None), (hg, hs, None)]
        if l == 1:
            pieces, out_own = tie(pieces, out_own)
        else:
            (ffn_grad,) = call(ffn_weights_body, "ffn_weights", ffn_ops, [sds((D, D), BF)])
            pieces, ffn_grad = tie(pieces, ffn_grad)
            ffn_pieces = lax.all_to_all(ffn_grad.reshape(16, 64, D), W, 0, 0)
        mid, mid_low, s2 = norm_bwd(pieces, middle, grad, table, (l, 1))
        ma, mb = gather_rows(mid_low)
        do, dq, dkvo = call(
            back_earlier_body, "back_earlier",
            where
            + [(ma, half, None), (mb, half, None), proj_of[l], (q, qs, None), (kvo, kvs, None), (lse, qs, None), (att, qs, None)],
            [sds(qs, BF), sds(qs, F32), sds(kvs, BF)],
        )
        got = lax.ppermute(dkvo, "context", [(1, 0)])
        dq, dkv = call(
            back_own_body, "back_own",
            where
            + [(do, qs, None), (q, qs, None), (kv, kvs, None), (lse, qs, None), (att, qs, None), (dq, qs, None)],
            [sds(qs, BF), sds(kvs, F32)],
        )
        if l == 1:
            dkv, out_own = tie(dkv, out_own)
            oa, ob = gather_rows(out_own)
        else:
            dkv, oa = tie(dkv, oa)
            (block_out,) = call(
                sequence_body, "to_sequence",
                [(order, None, None), (oa, half, None), (ob, half, None)],
                [sds((ROWS, D), BF)],
            )
            got, block_out, ffn_pieces = tie(got, block_out, ffn_pieces)
        joined, qv_sum, pa, pb = call(
            qkv_back_body, "qkv_back",
            [(dq, qs, None), (dkv, kvs, None), (got, kvs, None), qkv_of[l]],
            [sds(js, BF), sds((1, 384), F32), sds(half, BF), sds(half, BF)],
        )
        pieces = sum_pieces(pa, pb)
        attn_ops = [(na, half, None), (nb, half, None), (joined, js, None), (ma, half, None), (mb, half, None), (att, qs, None)]
        if l == 1:
            (weights_grad,) = call(
                layer_weights_body, "layer_weights", ffn_ops + attn_ops, [sds((D, 1536), BF)]
            )
            pieces, oa, weights_grad = tie(pieces, oa, weights_grad)
            owned1 = lax.psum_scatter(weights_grad, W, scatter_dimension=0, tiled=True)
            up1, qv1, s21 = up_sum, qv_sum, s2
            grad, low, s11 = norm_bwd(pieces, stream, mid, table, (1, 0))
            near, far = gather_rows(low)
            ea, eb = (near, half, None), (far, half, None)
        else:
            three, one = (3, D), (1, D)
            (packed,) = call(
                last_pack_body, "last_pack",
                attn_ops
                + [(pa, half, None), (pb, half, None), (x, half, (0, 0)), (x, half, (1, 0))]
                + [(s21, three, None), (s11, three, None), (s2, three, None), (b13, one, None)]
                + [(up_sum, (1, 512), None), (up1, (1, 512), None), (qv_sum, (1, 384), None), (qv1, (1, 384), None)],
                [sds((16, 80, 512), BF)],
            )
            mixed = lax.all_to_all(packed, W, 0, 0)
            _, low, _ = norm_bwd(pieces, stream, mid, table, (0, 0))
            near, far = gather_rows(low)
            near, ffn_pieces = tie(near, ffn_pieces)
            fc1_grad, fc2_grad = call(
                finish_ffn_body, "finish_ffn",
                [(ffn_pieces, (16, 64, D), None), (owned1, (64, D), (0, 0))],
                [sds((2, 64, 512), F32), sds((2, 64, 512), F32)],
            )
            near, fc1_grad, fc2_grad = tie(near, fc1_grad, fc2_grad)
            (input_grad,) = call(
                sequence_body, "to_sequence",
                [(order, None, None), (near, half, None), (far, half, None)],
                [sds((ROWS, D), F32)],
            )
    odd = ctx.astype(jnp.int32).reshape(1)
    small = (12, 64)
    (tail,) = call(
        finish_columns_body, "finish_columns",
        [(odd, None, None), (mixed, (16, 80, 512), None)],
        [sds(small, F32)],
    )
    tail = tail + core_swap(tail)
    tails = [tail] + [along_y(tail, step) for step in (1, 2, 3)]
    qkv_grad, proj_grad, qv_grad, up_grad = call(
        finish_body, "finish",
        [(mixed, (16, 80, 512), None), (owned1, (64, 512), (0, 2))],
        [sds((2, 64, 384), F32), sds((2, 64, 128), F32), sds((2, 256), F32), sds((2, 512), F32)],
    )
    tails, input_grad, qkv_grad = tie(tails, input_grad, qkv_grad)
    gains_grad, biases_grad = call(
        finish_rows_body, "finish_rows",
        [(v, small, None) for v in tails],
        [sds((2, 2, 64), F32), sds((2, 4, 64), F32)],
    )
    return (
        block_out[None], input_grad[None], qkv_grad, proj_grad, fc1_grad, fc2_grad,
        qv_grad, up_grad, gains_grad, biases_grad,
    )


def solution(mesh):
    return jax.shard_map(
        per_device,
        mesh=mesh,
        in_specs=(
            P("shard", "context", None),
            P(None, W, T),
            P(None, W, T),
            P(None, W, T),
            P(None, W, T),
            P(None, T),
            P(None, T),
            P(None, None, W),
            P(None, None, W),
            P("shard", "context", None),
        ),
        out_specs=(
            P("shard", "context", None),
            P("shard", "context", None),
            P(None, W, T),
            P(None, W, T),
            P(None, W, T),
            P(None, W, T),
            P(None, T),
            P(None, T),
            P(None, None, W),
            P(None, None, W),
        ),
        check_vma=False,
    )
```

```python
import jax
import jax.numpy as jnp
from jax import lax
from jax.experimental import pallas as pl
from jax.experimental.pallas import tpu as pltpu
from jax.sharding import PartitionSpec as P

HEADS = 16
HD = 64
NORM_EPS = 1e-05
GELU_SCALE = 0.7978845608028654
GELU_CUBE = 0.044715
F32 = jnp.float32
BF = jnp.bfloat16
W = ("shard", "context")
T = "tensor"
ROWS = 512
HALF = 256
PIECE = 64
D = 1024
NEG = -1e30
ROOM = {
    "kv_first": 6, "kv": 5, "q": 5, "attend_own": 8, "attend": 8, "ffn": 8, "ffn_back": 8,
    "back_earlier": 8, "back_own": 8, "qkv_back": 6, "ffn_weights": 8, "attn_weights": 6,
    "last_pack": 8, "to_relative": 5, "to_sequence": 5, "finish_ffn": 5,
}


def spec(shape, index=None):
    place = tuple(index) if index is not None else (0,) * len(shape)
    return pl.BlockSpec(shape, lambda i: place)


def smem():
    return pl.BlockSpec(memory_space=pltpu.SMEM)


def call(body, name, operands, outs):
    in_specs, args = [], []
    for array, shape, index in operands:
        in_specs.append(smem() if shape is None else spec(shape, index))
        args.append(array)
    return pl.pallas_call(
        body,
        grid=(1,),
        in_specs=in_specs,
        out_specs=[spec(o.shape) for o in outs],
        out_shape=outs,
        compiler_params=pltpu.CompilerParams(vmem_limit_bytes=ROOM.get(name, 4) << 20),
        name=name,
    )(*args)


def sds(shape, dtype):
    return jax.ShapeDtypeStruct(shape, dtype)


def mm(a, b):
    return lax.dot_general(a, b, (((1,), (0,)), ((), ())), preferred_element_type=F32)


def mm_nt(a, b):
    return lax.dot_general(a, b, (((1,), (1,)), ((), ())), preferred_element_type=F32)


def mm_tn(a, b):
    return lax.dot_general(a, b, (((0,), (0,)), ((), ())), preferred_element_type=F32)


def core_swap(v):
    return lax.ppermute(v, T, [(i, i ^ 1) for i in range(8)])


def along_y(v, step):
    return lax.ppermute(
        v, T, [(2 * y + c, 2 * ((y + step) % 4) + c) for y in range(4) for c in range(2)]
    )


def add_body(pa, got, h0, h1, h2, h3):
    both = pa[...].astype(F32) + got[...].astype(F32)
    h0[...] = both[:PIECE]
    h1[...] = both[PIECE : 2 * PIECE].astype(BF)
    h2[...] = both[2 * PIECE : 3 * PIECE].astype(BF)
    h3[...] = both[3 * PIECE :].astype(BF)


def tie(*values):
    return lax.optimization_barrier(values)


def chip_sums(keep, send):
    got = core_swap(send)
    return call(
        add_body,
        "pair_add",
        [(keep, (HALF, D), None), (got, (HALF, D), None)],
        [sds((PIECE, D), F32)] + [sds((PIECE, D), BF)] * 3,
    )


def spread(sums):
    h0, h1, h2, h3 = sums
    r2 = along_y(h2, -2)
    r1 = along_y(h1, -1)
    r3 = along_y(h3, -3)
    return h0, r1, r2, r3


def sum_pieces(keep, send):
    return spread(chip_sums(keep, send))


def gather_rows(own):
    r2 = along_y(own, 2)
    r1 = along_y(own, 1)
    r3 = along_y(own, 3)
    near = jnp.concatenate([own, r1, r2, r3], axis=0)
    far = core_swap(near)
    return near, far


def norm_parts(v):
    mean = jnp.mean(v, axis=-1, keepdims=True)
    centred = v - mean
    var = jnp.mean(centred * centred, axis=-1, keepdims=True)
    s = lax.rsqrt(var + NORM_EPS)
    return centred * s, s


def gain_row(table, l, i):
    at = 2 * l + i
    return table[at : at + 1]


def bias_row(table, l, i):
    at = 4 + 4 * l + i
    return table[at : at + 1]


def norm_fwd(pieces, resid, table, bias_at, next_at):
    def body(h0, r1, r2, r3, resid_ref, rows, stream, normed):
        v = (
            h0[...] + r1[...].astype(F32) + r2[...].astype(F32) + r3[...].astype(F32)
        ) + resid_ref[...].astype(F32) + bias_row(rows, *bias_at)
        stream[...] = v
        xhat, _ = norm_parts(v)
        gain, shift = next_at
        normed[...] = (xhat * gain_row(rows, *gain) + bias_row(rows, *shift)).astype(BF)

    b = (PIECE, D)
    return call(
        body,
        "norm_fwd",
        [(p, b, None) for p in (*pieces, resid)] + [(table, (12, D), None)],
        [sds(b, F32), sds(b, BF)],
    )


def out_rows(pieces, resid, table):
    def body(h0, r1, r2, r3, resid_ref, rows, out):
        out[...] = (
            (h0[...] + r1[...].astype(F32) + r2[...].astype(F32) + r3[...].astype(F32))
            + resid_ref[...]
            + bias_row(rows, 1, 3)
        ).astype(BF)

    b = (PIECE, D)
    return call(
        body,
        "out_rows",
        [(p, b, None) for p in (*pieces, resid)] + [(table, (12, D), None)],
        [sds(b, BF)],
    )[0]


def norm_bwd(pieces, stream, grad, table, gain_at):
    def body(h0, r1, r2, r3, stream_ref, grad_ref, rows, out, low, sums):
        g = h0[...] + r1[...].astype(F32) + r2[...].astype(F32) + r3[...].astype(F32)
        xhat, s = norm_parts(stream_ref[...].astype(F32))
        gx = g * xhat
        c = g * gain_row(rows, *gain_at)
        cx = c * xhat
        e = grad_ref[...].astype(F32) + s * (
            c
            - jnp.mean(c, axis=-1, keepdims=True)
            - xhat * jnp.mean(cx, axis=-1, keepdims=True)
        )
        out[...] = e
        low[...] = e.astype(BF)
        sums[0:1] = jnp.sum(gx, axis=0, keepdims=True)
        sums[1:2] = jnp.sum(g, axis=0, keepdims=True)
        sums[2:3] = jnp.sum(e, axis=0, keepdims=True)

    b = (PIECE, D)
    return call(
        body,
        "norm_bwd",
        [(p, b, None) for p in (*pieces, stream, grad)] + [(table, (12, D), None)],
        [sds(b, F32), sds(b, BF), sds((3, D), F32)],
    )


def kv_first_body(xa, xb, first, rows, bias, na, nb, kv):
    w = qkv_matrix(first)[:, 128:]
    for x, n, at in ((xa, na, 0), (xb, nb, HALF)):
        xhat, _ = norm_parts(x[...].astype(F32))
        normed = (xhat * gain_row(rows, 0, 0) + bias_row(rows, 0, 0)).astype(BF)
        n[...] = normed
        kv[at : at + HALF] = (mm(normed, w) + bias[:, 128:]).astype(BF)


def kv_body(na, nb, w, bias, kv):
    for n, at in ((na, 0), (nb, HALF)):
        kv[at : at + HALF] = (mm(n[...], w[:, 128:]) + bias[:, 128:]).astype(BF)


def q_body(na, nb, w, bias, q):
    m = qkv_matrix(w)[:, :128]
    for n, at in ((na, 0), (nb, HALF)):
        q[at : at + HALF] = (mm(n[...], m) + bias[:, :128]).astype(BF)


def proj_matrix(ref):
    return ref[:, :64, 384:].reshape(D, 128) if len(ref.shape) == 3 else ref[...]


def qkv_matrix(ref):
    return ref[:, :64, :384].reshape(D, 384) if len(ref.shape) == 3 else ref[...]


def places(place, shape, axis):
    r = lax.broadcasted_iota(jnp.int32, shape, axis)
    y, c = place[0], place[1]
    return ((y - ((r >> 6) & 3)) & 3) * 128 + ((c + (r >> 8)) & 1) * 64 + (r & 63)


def own_scores(place, slope, h, qh, kh, mask):
    pos = places(place, (1, ROWS), 1).astype(F32)
    return jnp.where(mask, mm_nt(qh, kh) * 0.125 + slope[h] * pos, NEG)


def earlier_scores(place, slope, h, qh, kh):
    pos = places(place, (1, ROWS), 1).astype(F32)
    off = jnp.where(place[2] == 1, 0.0, NEG)
    return mm_nt(qh, kh) * 0.125 + (slope[h] * (pos - 512.0) + off)


def own_mask(place):
    return places(place, (ROWS, 1), 0) >= places(place, (1, ROWS), 1)


def attend_own_body(place, slope, q, kv, out, top, total):
    mask = own_mask(place)
    for h in range(2):
        lo, hi = h * HD, (h + 1) * HD
        s = own_scores(place, slope, h, q[:, lo:hi], kv[:, lo:hi], mask)
        m = jnp.max(s, axis=-1, keepdims=True)
        p = jnp.exp(s - m)
        out[:, lo:hi] = mm(p.astype(BF), kv[:, 128 + lo : 128 + hi])
        top[:, lo:hi] = jnp.broadcast_to(m, (ROWS, HD))
        total[:, lo:hi] = jnp.broadcast_to(jnp.sum(p, axis=-1, keepdims=True), (ROWS, HD))


def attend_body(place, slope, q, kvo, pw, own, own_top, own_total, att, lse, pa, pb):
    outs, logs = [], []
    for h in range(2):
        lo, hi = h * HD, (h + 1) * HD
        s = earlier_scores(place, slope, h, q[:, lo:hi], kvo[:, lo:hi])
        m = own_top[:, lo : lo + 1]
        top = jnp.maximum(m, jnp.max(s, axis=-1, keepdims=True))
        p = jnp.exp(s - top)
        scale = jnp.exp(m - top)
        total = own_total[:, lo : lo + 1] * scale + jnp.sum(p, axis=-1, keepdims=True)
        o = own[:, lo:hi] * scale + mm(p.astype(BF), kvo[:, 128 + lo : 128 + hi])
        outs.append(o / total)
        logs.append(jnp.broadcast_to(top + jnp.log(total), (ROWS, HD)))
    attended = jnp.concatenate(outs, axis=1).astype(BF)
    att[...] = attended
    lse[...] = jnp.concatenate(logs, axis=1)
    w = proj_matrix(pw)
    pa[...] = mm_nt(attended[:HALF], w).astype(BF)
    pb[...] = mm_nt(attended[HALF:], w).astype(BF)


def score_grads(p, doh, vh, atth):
    delta = jnp.sum(doh.astype(F32) * atth.astype(F32), axis=-1, keepdims=True)
    return (p * (mm_nt(doh, vh) - delta)).astype(BF)


def back_earlier_body(place, slope, ma, mb, pw, q, kvo, lse, att, do_ref, dq, dkvo):
    w = proj_matrix(pw)
    do = jnp.concatenate([mm(ma[...], w), mm(mb[...], w)], axis=0).astype(BF)
    do_ref[...] = do
    dqs, dks, dvs = [], [], []
    for h in range(2):
        lo, hi = h * HD, (h + 1) * HD
        qh, kh, vh, doh = q[:, lo:hi], kvo[:, lo:hi], kvo[:, 128 + lo : 128 + hi], do[:, lo:hi]
        p = jnp.exp(earlier_scores(place, slope, h, qh, kh) - lse[:, lo : lo + 1])
        d = score_grads(p, doh, vh, att[:, lo:hi])
        dqs.append(mm(d, kh) * 0.125)
        dks.append(mm_tn(d, qh) * 0.125)
        dvs.append(mm_tn(p.astype(BF), doh))
    dq[...] = jnp.concatenate(dqs, axis=1)
    dkvo[...] = jnp.concatenate(dks + dvs, axis=1).astype(BF)


def back_own_body(place, slope, do, q, kv, lse, att, dq_part, dq, dkv):
    mask = own_mask(place)
    dqs, dks, dvs = [], [], []
    for h in range(2):
        lo, hi = h * HD, (h + 1) * HD
        qh, kh, vh, doh = q[:, lo:hi], kv[:, lo:hi], kv[:, 128 + lo : 128 + hi], do[:, lo:hi]
        p = jnp.exp(own_scores(place, slope, h, qh, kh, mask) - lse[:, lo : lo + 1])
        d = score_grads(p, doh, vh, att[:, lo:hi])
        dqs.append(mm(d, kh) * 0.125)
        dks.append(mm_tn(d, qh) * 0.125)
        dvs.append(mm_tn(p.astype(BF), doh))
    dq[...] = (dq_part[...] + jnp.concatenate(dqs, axis=1)).astype(BF)
    dkv[...] = jnp.concatenate(dks + dvs, axis=1)


def ffn_body(na, nb, w1, w2, bias, act, dgel, pa, pb):
    for n, p, at in ((na, pa, 0), (nb, pb, HALF)):
        v = mm(n[...], w1[...]) + bias[...]
        v2 = v * v
        th = jnp.tanh(GELU_SCALE * (v + GELU_CUBE * (v2 * v)))
        one = 0.5 + 0.5 * th
        a = (v * one).astype(BF)
        act[at : at + HALF] = a
        dgel[at : at + HALF] = (
            one
            + (0.5 * GELU_SCALE) * v * (1.0 - th * th) * (1.0 + (3.0 * GELU_CUBE) * v2)
        ).astype(BF)
        p[...] = mm_nt(a, w2[...]).astype(BF)


def ffn_back_body(ea, eb, w1, w2, dgel, hg, sums, pa, pb):
    total = jnp.zeros((1, 512), F32)
    for e, p, at in ((ea, pa, 0), (eb, pb, HALF)):
        g = (mm(e[...], w2[...]) * dgel[at : at + HALF].astype(F32)).astype(BF)
        hg[at : at + HALF] = g
        total += jnp.sum(g.astype(F32), axis=0, keepdims=True)
        p[...] = mm_nt(g, w1[...]).astype(BF)
    sums[...] = total


def ffn_weights_body(ea, eb, act, na, nb, hg, out):
    out[:, :512] = (mm_tn(na[...], hg[:HALF]) + mm_tn(nb[...], hg[HALF:])).astype(BF)
    out[:, 512:] = (mm_tn(ea[...], act[:HALF]) + mm_tn(eb[...], act[HALF:])).astype(BF)


def attn_weights_body(na, nb, joined, ma, mb, att, out):
    out[:, :384] = (
        mm_tn(na[...], joined[:HALF]) + mm_tn(nb[...], joined[HALF:])
    ).astype(BF)
    out[:, 384:] = (mm_tn(ma[...], att[:HALF]) + mm_tn(mb[...], att[HALF:])).astype(BF)


def two_halves(v):
    high = v.astype(BF)
    return high, (v - high.astype(F32)).astype(BF)


def last_pack_body(
    na, nb, joined, ma, mb, att, pa, pb, xa, xb, s21, s11, s20, b13,
    up0, up1, qv0, qv1, out,
):
    g = (mm_tn(na[...], joined[:HALF]) + mm_tn(nb[...], joined[HALF:])).astype(BF)
    out[:, :64, :384] = g.reshape(16, 64, 384)
    g = (mm_tn(ma[...], att[:HALF]) + mm_tn(mb[...], att[HALF:])).astype(BF)
    out[:, :64, 384:] = g.reshape(16, 64, 128)
    gain = jnp.zeros((1, D), F32)
    shift = jnp.zeros((1, D), F32)
    for p, x in ((pa, xa), (pb, xb)):
        g = p[...].astype(F32)
        xhat, _ = norm_parts(x[...].astype(F32))
        gain += jnp.sum(g * xhat, axis=0, keepdims=True)
        shift += jnp.sum(g, axis=0, keepdims=True)
    columns = jnp.concatenate(
        [
            gain, s20[0:1], s11[0:1], s21[0:1],
            shift, s20[2:3], s20[1:2], s11[2:3], s11[1:2], s21[2:3], s21[1:2], b13[...],
        ]
    ).astype(BF)
    q0, q0l = two_halves(qv0[...])
    q1, q1l = two_halves(qv1[...])
    u0, u0l = two_halves(up0[...])
    u1, u1l = two_halves(up1[...])
    none = jnp.zeros((1, 384), BF)
    lines = jnp.concatenate(
        [
            q0, q1, q0l, q1l,
            u0[:, :384], u1[:, :384], u0l[:, :384], u1l[:, :384],
            jnp.concatenate([u0[:, 384:], u1[:, 384:], none[:, :128]], axis=1),
            jnp.concatenate([u0l[:, 384:], u1l[:, 384:], none[:, :128]], axis=1),
            none, none,
        ]
    )
    for w in range(16):
        at = 128 * (w // 2)
        tail = jnp.concatenate([columns[:, at : at + 128], lines], axis=1)
        out[w, 64:80] = jnp.concatenate([tail, jnp.zeros((4, 512), BF)])


def qkv_back_body(dq, dkv, got, w, joined, sums, pa, pb):
    j = jnp.concatenate(
        [dq[...], (dkv[...] + got[...].astype(F32)).astype(BF)], axis=1
    )
    joined[...] = j
    sums[...] = jnp.sum(j.astype(F32), axis=0, keepdims=True)
    m = qkv_matrix(w)
    pa[...] = mm_nt(j[:HALF], m).astype(BF)
    pb[...] = mm_nt(j[HALF:], m).astype(BF)


def by_kind(m):
    parts = [m[:, i * HD : (i + 1) * HD] for i in range(6)]
    return jnp.concatenate([parts[i] for i in (0, 3, 1, 4, 2, 5)], axis=1)


def by_head(m):
    parts = [m[:, i * HD : (i + 1) * HD] for i in range(6)]
    return jnp.concatenate([parts[i] for i in (0, 2, 4, 1, 3, 5)], axis=1)


def from_hbm(body, name, arrays, outs):
    count = len(arrays)

    def kernel(*refs):
        given, made = refs[:count], refs[count : count + len(outs)]
        held, sems = refs[count + len(outs) : -1], refs[-1]
        copies = [
            pltpu.make_async_copy(src, dst, sems.at[i])
            for i, (src, dst) in enumerate(zip(given, held))
        ]
        for copy in copies:
            copy.start()
        for copy in copies:
            copy.wait()
        body(*held, *made)

    return pl.pallas_call(
        kernel,
        in_specs=[pl.BlockSpec(memory_space=pltpu.HBM) for _ in arrays],
        out_specs=[pl.BlockSpec(memory_space=pltpu.VMEM) for _ in outs],
        out_shape=outs,
        scratch_shapes=[pltpu.VMEM(a.shape, a.dtype) for a in arrays]
        + [pltpu.SemaphoreType.DMA((count,))],
        compiler_params=pltpu.CompilerParams(vmem_limit_bytes=ROOM.get(name, 4) << 20),
        name=name,
    )(*arrays)


def pack_first_body(qkv, proj, gains, biases, first):
    small = [gains[l, i : i + 1] for l in range(2) for i in range(2)]
    small += [biases[l, i : i + 1] for l in range(2) for i in range(4)]
    lines = jnp.concatenate(
        [jnp.concatenate([small[2 * i], small[2 * i + 1]], axis=1) for i in range(6)]
        + [jnp.zeros((2, 128), BF)]
    )
    own = jnp.concatenate(
        [
            jnp.concatenate([by_kind(qkv[0]), proj[0]], axis=1),
            jnp.concatenate([lines, jnp.zeros((8, 384), BF)], axis=1),
        ]
    )
    for w in range(16):
        first[w] = own


def pack_rest_body(qkv, proj, fc1, fc2, second, third):
    second[:, :512] = fc1[0]
    second[:, 512:1024] = fc2[0]
    second[:, 1024:1152] = jnp.zeros((64, 128), BF)
    second[:, 1152:] = by_kind(qkv[1])
    third[:, :512] = fc1[1]
    third[:, 512:1024] = fc2[1]
    third[:, 1024:] = proj[1]


def sum16(ref, *at):
    total = ref[(0, *at)].astype(F32)
    for w in range(1, 16):
        total += ref[(w, *at)].astype(F32)
    return total


def finish_ffn_body(f0, f1, fc1, fc2):
    for l, total in enumerate((sum16(f0), f1[...].astype(F32))):
        fc1[l] = total[:, :512]
        fc2[l] = total[:, 512:]


def finish_columns_body(odd, mixed, columns):
    own = mixed[0, 64:80, :128].astype(F32)
    for w in range(1, 16):
        own += mixed[w, 64:80, :128].astype(F32)
    columns[...] = jnp.where(odd[0] == 1, own[:12, 64:], own[:12, :64])


def finish_body(mixed, attn1, qkv, proj, qv, up):
    total = sum16(mixed)
    for l, m in enumerate((total[:64], attn1[...].astype(F32))):
        qkv[l] = by_head(m[:, :384])
        proj[l] = m[:, 384:]
    own = total[64:76]
    for l in range(2):
        line = own[l : l + 1, 128:] + own[2 + l : 3 + l, 128:]
        parts = [line[:, i * HD : (i + 1) * HD] for i in (0, 4, 1, 5)]
        qv[l : l + 1] = jnp.concatenate(parts, axis=1)
        near = own[4 + l : 5 + l, 128:] + own[6 + l : 7 + l, 128:]
        at = 128 + 128 * l
        up[l : l + 1] = jnp.concatenate(
            [near, own[8:9, at : at + 128] + own[9:10, at : at + 128]], axis=1
        )


def finish_rows_body(t0, t1, t2, t3, gains, biases):
    total = (t0[...] + t1[...]) + (t2[...] + t3[...])
    for l in range(2):
        gains[l] = total[2 * l : 2 * l + 2]
        biases[l] = total[4 + 4 * l : 8 + 4 * l]


def relative_body(order, x, cot, xr, cr, total):
    for j in range(8):
        row = pl.multiple_of(order[j] * PIECE, PIECE)
        xr[j * PIECE : (j + 1) * PIECE] = x[pl.ds(row, PIECE)]
        cr[j * PIECE : (j + 1) * PIECE] = cot[pl.ds(row, PIECE)]
    total[...] = jnp.sum(cr[:PIECE].astype(F32), axis=0, keepdims=True)


def sequence_body(order, near, far, out):
    for j in range(8):
        row = pl.multiple_of(order[j] * PIECE, PIECE)
        src = near if j < 4 else far
        k = j % 4
        out[pl.ds(row, PIECE)] = src[k * PIECE : (k + 1) * PIECE].astype(out.dtype)


def per_device(
    block_in, qkv_weight, proj_weight, fc1_weight, fc2_weight,
    qv_bias, fc1_bias, norm_gains, row_biases, cotangent,
):
    t = lax.axis_index(T)
    y, c = t // 2, t % 2
    ctx = lax.axis_index("context")
    place = jnp.stack([y, c, ctx]).astype(jnp.int32)
    slope = jnp.exp2(-8.0 * (2 * t + 1 + jnp.arange(2)).astype(F32) / HEADS)
    j = jnp.arange(8)
    order = (2 * ((y - j % 4) % 4) + (c + j // 4) % 2).astype(jnp.int32)
    half = (HALF, D)
    qs, kvs, hs, js = (ROWS, 128), (ROWS, 256), (ROWS, 512), (ROWS, 384)

    (first,) = from_hbm(
        pack_first_body, "pack_first", [qkv_weight, proj_weight, norm_gains, row_biases],
        [sds((16, 72, 512), BF)],
    )
    first, fc1_weight = tie(first, fc1_weight)
    first_all = lax.all_to_all(first, W, 0, 0)
    second_part, third_part = from_hbm(
        pack_rest_body, "pack_rest", [qkv_weight, proj_weight, fc1_weight, fc2_weight],
        [sds((64, 1536), BF), sds((64, 1152), BF)],
    )
    second_all = lax.all_gather(second_part, W, axis=0, tiled=True)
    third_all = lax.all_gather(third_part, W, axis=0, tiled=True)
    table = (
        first_all[:, 64:70, :128].reshape(16, 12, 64).transpose(1, 0, 2).reshape(12, D).astype(F32)
    )
    tab = (table, (12, D), None)
    whole_first = (first_all, (16, 72, 512), None)
    qv = qv_bias.astype(F32).reshape(2, 2, 2, HD).transpose(0, 2, 1, 3)
    zero = jnp.zeros((2, 1, 2, HD), F32)
    joined_bias = jnp.concatenate([qv[:, :1], zero, qv[:, 1:]], axis=1).reshape(2, 1, 384)
    up_bias = fc1_bias.astype(F32).reshape(2, 1, 512)

    x, cot, b13 = call(
        relative_body, "to_relative",
        [(order, None, None), (block_in.reshape(ROWS, D), (ROWS, D), None), (cotangent.reshape(ROWS, D), (ROWS, D), None)],
        [sds((ROWS, D), BF), sds((ROWS, D), BF), sds((1, D), F32)],
    )

    saved = []
    stream = x
    qkv_of = (whole_first, (second_all, (D, 384), (0, 3)))
    proj_of = (whole_first, (third_all, (D, 128), (0, 8)))
    fc1_of = [(m, (D, 512), (0, 0)) for m in (second_all, third_all)]
    fc2_of = [(m, (D, 512), (0, 1)) for m in (second_all, third_all)]

    where = [(place, None, None), (slope, None, None)]
    for l in range(2):
        bias = (joined_bias[l], (1, 384), None)
        if l == 0:
            na, nb, kv = call(
                kv_first_body, "kv_first",
                [(x, half, (0, 0)), (x, half, (1, 0)), whole_first, tab, bias],
                [sds(half, BF), sds(half, BF), sds(kvs, BF)],
            )
        else:
            na, nb = gather_rows(normed)
            (kv,) = call(
                kv_body, "kv", [(na, half, None), (nb, half, None), qkv_of[l], bias], [sds(kvs, BF)]
            )
        kvo = lax.ppermute(kv, "context", [(0, 1)])
        (q,) = call(
            q_body, "q", [(na, half, None), (nb, half, None), qkv_of[l], bias], [sds(qs, BF)]
        )
        own, own_top, own_total = call(
            attend_own_body, "attend_own", where + [(q, qs, None), (kv, kvs, None)], [sds(qs, F32)] * 3
        )
        att, lse, pa, pb = call(
            attend_body, "attend",
            where + [(q, qs, None), (kvo, kvs, None), proj_of[l]] + [(v, qs, None) for v in (own, own_top, own_total)],
            [sds(qs, BF), sds(qs, F32), sds(half, BF), sds(half, BF)],
        )
        middle, second = norm_fwd(
            sum_pieces(pa, pb), stream, table, (l, 1), ((l, 1), (l, 2))
        )
        sa, sb = gather_rows(second)
        act, dgel, pa, pb = call(
            ffn_body, "ffn",
            [(sa, half, None), (sb, half, None), fc1_of[l], fc2_of[l], (up_bias[l], (1, 512), None)],
            [sds(hs, BF), sds(hs, BF), sds(half, BF), sds(half, BF)],
        )
        saved.append((stream, na, nb, q, kv, kvo, att, lse, middle, sa, sb, act, dgel))
        if l == 0:
            stream, normed = norm_fwd(
                sum_pieces(pa, pb), middle, table, (0, 3), ((1, 0), (1, 0))
            )
    out_own = out_rows(sum_pieces(pa, pb), middle, table)

    grad = cot
    ea = (cot, half, (0, 0))
    eb = (cot, half, (1, 0))
    for l in (1, 0):
        stream, na, nb, q, kv, kvo, att, lse, middle, sa, sb, act, dgel = saved[l]
        hg, up_sum, pa, pb = call(
            ffn_back_body, "ffn_back",
            [ea, eb, fc1_of[l], fc2_of[l], (dgel, hs, None)],
            [sds(hs, BF), sds((1, 512), F32), sds(half, BF), sds(half, BF)],
        )
        pieces = sum_pieces(pa, pb)
        ffn_ops = [ea, eb, (act, hs, None), (sa, half, None), (sb, half, None), (hg, hs, None)]
        if l == 1:
            (ffn_grad,) = call(ffn_weights_body, "ffn_weights", ffn_ops, [sds((D, D), BF)])
            pieces, out_own, ffn_grad = tie(pieces, out_own, ffn_grad)
            ffn1_owned = lax.psum_scatter(ffn_grad, W, scatter_dimension=0, tiled=True)
        else:
            (ffn_grad,) = call(ffn_weights_body, "ffn_weights", ffn_ops, [sds((D, D), BF)])
            ffn_pieces = lax.all_to_all(ffn_grad.reshape(16, 64, D), W, 0, 0)
        mid, mid_low, s2 = norm_bwd(pieces, middle, grad, table, (l, 1))
        ma, mb = gather_rows(mid_low)
        do, dq, dkvo = call(
            back_earlier_body, "back_earlier",
            where
            + [(ma, half, None), (mb, half, None), proj_of[l], (q, qs, None), (kvo, kvs, None), (lse, qs, None), (att, qs, None)],
            [sds(qs, BF), sds(qs, F32), sds(kvs, BF)],
        )
        got = lax.ppermute(dkvo, "context", [(1, 0)])
        dq, dkv = call(
            back_own_body, "back_own",
            where
            + [(do, qs, None), (q, qs, None), (kv, kvs, None), (lse, qs, None), (att, qs, None), (dq, qs, None)],
            [sds(qs, BF), sds(kvs, F32)],
        )
        if l == 1:
            dkv, out_own = tie(dkv, out_own)
            oa, ob = gather_rows(out_own)
        else:
            dkv, oa = tie(dkv, oa)
            (block_out,) = call(
                sequence_body, "to_sequence",
                [(order, None, None), (oa, half, None), (ob, half, None)],
                [sds((ROWS, D), BF)],
            )
            got, block_out, ffn_pieces = tie(got, block_out, ffn_pieces)
        joined, qv_sum, pa, pb = call(
            qkv_back_body, "qkv_back",
            [(dq, qs, None), (dkv, kvs, None), (got, kvs, None), qkv_of[l]],
            [sds(js, BF), sds((1, 384), F32), sds(half, BF), sds(half, BF)],
        )
        pieces = sum_pieces(pa, pb)
        attn_ops = [(na, half, None), (nb, half, None), (joined, js, None), (ma, half, None), (mb, half, None), (att, qs, None)]
        if l == 1:
            (weights_grad,) = call(
                attn_weights_body, "attn_weights", attn_ops, [sds((D, 512), BF)]
            )
            pieces, oa, weights_grad = tie(pieces, oa, weights_grad)
            weights_grad, ffn1_owned = tie(weights_grad, ffn1_owned)
            owned1 = lax.psum_scatter(weights_grad, W, scatter_dimension=0, tiled=True)
            up1, qv1, s21 = up_sum, qv_sum, s2
            grad, low, s11 = norm_bwd(pieces, stream, mid, table, (1, 0))
            near, far = gather_rows(low)
            ea, eb = (near, half, None), (far, half, None)
        else:
            three, one = (3, D), (1, D)
            (packed,) = call(
                last_pack_body, "last_pack",
                attn_ops
                + [(pa, half, None), (pb, half, None), (x, half, (0, 0)), (x, half, (1, 0))]
                + [(s21, three, None), (s11, three, None), (s2, three, None), (b13, one, None)]
                + [(up_sum, (1, 512), None), (up1, (1, 512), None), (qv_sum, (1, 384), None), (qv1, (1, 384), None)],
                [sds((16, 80, 512), BF)],
            )
            mixed = lax.all_to_all(packed, W, 0, 0)
            _, low, _ = norm_bwd(pieces, stream, mid, table, (0, 0))
            near, far = gather_rows(low)
            near, ffn_pieces = tie(near, ffn_pieces)
            fc1_grad, fc2_grad = call(
                finish_ffn_body, "finish_ffn",
                [(ffn_pieces, (16, 64, D), None), (ffn1_owned, (64, D), None)],
                [sds((2, 64, 512), F32), sds((2, 64, 512), F32)],
            )
            near, fc1_grad, fc2_grad = tie(near, fc1_grad, fc2_grad)
            (input_grad,) = call(
                sequence_body, "to_sequence",
                [(order, None, None), (near, half, None), (far, half, None)],
                [sds((ROWS, D), F32)],
            )
    odd = ctx.astype(jnp.int32).reshape(1)
    small = (12, 64)
    (tail,) = call(
        finish_columns_body, "finish_columns",
        [(odd, None, None), (mixed, (16, 80, 512), None)],
        [sds(small, F32)],
    )
    tail = tail + core_swap(tail)
    tails = [tail] + [along_y(tail, step) for step in (1, 2, 3)]
    qkv_grad, proj_grad, qv_grad, up_grad = call(
        finish_body, "finish",
        [(mixed, (16, 80, 512), None), (owned1, (64, 512), None)],
        [sds((2, 64, 384), F32), sds((2, 64, 128), F32), sds((2, 256), F32), sds((2, 512), F32)],
    )
    tails, input_grad, qkv_grad = tie(tails, input_grad, qkv_grad)
    gains_grad, biases_grad = call(
        finish_rows_body, "finish_rows",
        [(v, small, None) for v in tails],
        [sds((2, 2, 64), F32), sds((2, 4, 64), F32)],
    )
    return (
        block_out[None], input_grad[None], qkv_grad, proj_grad, fc1_grad, fc2_grad,
        qv_grad, up_grad, gains_grad, biases_grad,
    )


def solution(mesh):
    return jax.shard_map(
        per_device,
        mesh=mesh,
        in_specs=(
            P("shard", "context", None),
            P(None, W, T),
            P(None, W, T),
            P(None, W, T),
            P(None, W, T),
            P(None, T),
            P(None, T),
            P(None, None, W),
            P(None, None, W),
            P("shard", "context", None),
        ),
        out_specs=(
            P("shard", "context", None),
            P("shard", "context", None),
            P(None, W, T),
            P(None, W, T),
            P(None, W, T),
            P(None, W, T),
            P(None, T),
            P(None, T),
            P(None, None, W),
            P(None, None, W),
        ),
        check_vma=False,
    )
```

```python
import jax
import jax.numpy as jnp
from jax import lax
from jax.experimental import pallas as pl
from jax.experimental.pallas import tpu as pltpu
from jax.sharding import PartitionSpec as P

HEADS = 16
HD = 64
NORM_EPS = 1e-05
GELU_SCALE = 0.7978845608028654
GELU_CUBE = 0.044715
F32 = jnp.float32
BF = jnp.bfloat16
W = ("shard", "context")
T = "tensor"
ROWS = 512
HALF = 256
PIECE = 64
D = 1024
NEG = -1e30
ROOM = {
    "kv_first": 10, "kv": 8, "q": 8, "attend_own": 12, "attend": 12, "ffn": 14, "ffn_back": 12,
    "back_earlier": 14, "back_own": 12, "qkv_back": 10, "ffn_weights": 14, "layer_weights": 20,
    "last_pack": 16, "to_relative": 8, "to_sequence": 8, "finish_ffn": 8,
}


def spec(shape, index=None):
    place = tuple(index) if index is not None else (0,) * len(shape)
    return pl.BlockSpec(shape, lambda i: place)


def smem():
    return pl.BlockSpec(memory_space=pltpu.SMEM)


def call(body, name, operands, outs):
    in_specs, args = [], []
    for array, shape, index in operands:
        in_specs.append(smem() if shape is None else spec(shape, index))
        args.append(array)
    return pl.pallas_call(
        body,
        grid=(1,),
        in_specs=in_specs,
        out_specs=[spec(o.shape) for o in outs],
        out_shape=outs,
        compiler_params=pltpu.CompilerParams(vmem_limit_bytes=ROOM.get(name, 6) << 20),
        name=name,
    )(*args)


def sds(shape, dtype):
    return jax.ShapeDtypeStruct(shape, dtype)


def mm(a, b):
    return lax.dot_general(a, b, (((1,), (0,)), ((), ())), preferred_element_type=F32)


def mm_nt(a, b):
    return lax.dot_general(a, b, (((1,), (1,)), ((), ())), preferred_element_type=F32)


def mm_tn(a, b):
    return lax.dot_general(a, b, (((0,), (0,)), ((), ())), preferred_element_type=F32)


def core_swap(v):
    return lax.ppermute(v, T, [(i, i ^ 1) for i in range(8)])


def along_y(v, step):
    return lax.ppermute(
        v, T, [(2 * y + c, 2 * ((y + step) % 4) + c) for y in range(4) for c in range(2)]
    )


def add_body(pa, got, h0, h1, h2, h3):
    both = pa[...].astype(F32) + got[...].astype(F32)
    h0[...] = both[:PIECE]
    h1[...] = both[PIECE : 2 * PIECE].astype(BF)
    h2[...] = both[2 * PIECE : 3 * PIECE].astype(BF)
    h3[...] = both[3 * PIECE :].astype(BF)


def tie(*values):
    return lax.optimization_barrier(values)


def chip_sums(keep, send):
    got = core_swap(send)
    return call(
        add_body,
        "pair_add",
        [(keep, (HALF, D), None), (got, (HALF, D), None)],
        [sds((PIECE, D), F32)] + [sds((PIECE, D), BF)] * 3,
    )


def spread(sums):
    h0, h1, h2, h3 = sums
    r2 = along_y(h2, -2)
    r1 = along_y(h1, -1)
    r3 = along_y(h3, -3)
    return h0, r1, r2, r3


def sum_pieces(keep, send):
    return spread(chip_sums(keep, send))


def gather_rows(own):
    r2 = along_y(own, 2)
    r1 = along_y(own, 1)
    r3 = along_y(own, 3)
    near = jnp.concatenate([own, r1, r2, r3], axis=0)
    far = core_swap(near)
    return near, far


def norm_parts(v):
    mean = jnp.mean(v, axis=-1, keepdims=True)
    centred = v - mean
    var = jnp.mean(centred * centred, axis=-1, keepdims=True)
    s = lax.rsqrt(var + NORM_EPS)
    return centred * s, s


def gain_row(table, l, i):
    at = 2 * l + i
    return table[at : at + 1]


def bias_row(table, l, i):
    at = 4 + 4 * l + i
    return table[at : at + 1]


def norm_fwd(pieces, resid, table, bias_at, next_at):
    def body(h0, r1, r2, r3, resid_ref, rows, stream, normed):
        v = (
            h0[...] + r1[...].astype(F32) + r2[...].astype(F32) + r3[...].astype(F32)
        ) + resid_ref[...].astype(F32) + bias_row(rows, *bias_at)
        stream[...] = v
        xhat, _ = norm_parts(v)
        gain, shift = next_at
        normed[...] = (xhat * gain_row(rows, *gain) + bias_row(rows, *shift)).astype(BF)

    b = (PIECE, D)
    return call(
        body,
        "norm_fwd",
        [(p, b, None) for p in (*pieces, resid)] + [(table, (12, D), None)],
        [sds(b, F32), sds(b, BF)],
    )


def out_rows(pieces, resid, table):
    def body(h0, r1, r2, r3, resid_ref, rows, out):
        out[...] = (
            (h0[...] + r1[...].astype(F32) + r2[...].astype(F32) + r3[...].astype(F32))
            + resid_ref[...]
            + bias_row(rows, 1, 3)
        ).astype(BF)

    b = (PIECE, D)
    return call(
        body,
        "out_rows",
        [(p, b, None) for p in (*pieces, resid)] + [(table, (12, D), None)],
        [sds(b, BF)],
    )[0]


def norm_bwd(pieces, stream, grad, table, gain_at):
    def body(h0, r1, r2, r3, stream_ref, grad_ref, rows, out, low, sums):
        g = h0[...] + r1[...].astype(F32) + r2[...].astype(F32) + r3[...].astype(F32)
        xhat, s = norm_parts(stream_ref[...].astype(F32))
        gx = g * xhat
        c = g * gain_row(rows, *gain_at)
        cx = c * xhat
        e = grad_ref[...].astype(F32) + s * (
            c
            - jnp.mean(c, axis=-1, keepdims=True)
            - xhat * jnp.mean(cx, axis=-1, keepdims=True)
        )
        out[...] = e
        low[...] = e.astype(BF)
        sums[0:1] = jnp.sum(gx, axis=0, keepdims=True)
        sums[1:2] = jnp.sum(g, axis=0, keepdims=True)
        sums[2:3] = jnp.sum(e, axis=0, keepdims=True)

    b = (PIECE, D)
    return call(
        body,
        "norm_bwd",
        [(p, b, None) for p in (*pieces, stream, grad)] + [(table, (12, D), None)],
        [sds(b, F32), sds(b, BF), sds((3, D), F32)],
    )


def kv_first_body(xa, xb, first, rows, bias, na, nb, kv):
    w = qkv_matrix(first)[:, 128:]
    for x, n, at in ((xa, na, 0), (xb, nb, HALF)):
        xhat, _ = norm_parts(x[...].astype(F32))
        normed = (xhat * gain_row(rows, 0, 0) + bias_row(rows, 0, 0)).astype(BF)
        n[...] = normed
        kv[at : at + HALF] = (mm(normed, w) + bias[:, 128:]).astype(BF)


def kv_body(na, nb, w, bias, kv):
    for n, at in ((na, 0), (nb, HALF)):
        kv[at : at + HALF] = (mm(n[...], w[:, 128:]) + bias[:, 128:]).astype(BF)


def q_body(na, nb, w, bias, q):
    m = qkv_matrix(w)[:, :128]
    for n, at in ((na, 0), (nb, HALF)):
        q[at : at + HALF] = (mm(n[...], m) + bias[:, :128]).astype(BF)


def proj_matrix(ref):
    return ref[:, :64, 384:].reshape(D, 128) if len(ref.shape) == 3 else ref[...]


def qkv_matrix(ref):
    return ref[:, :64, :384].reshape(D, 384) if len(ref.shape) == 3 else ref[...]


def places(place, shape, axis):
    r = lax.broadcasted_iota(jnp.int32, shape, axis)
    y, c = place[0], place[1]
    return ((y - ((r >> 6) & 3)) & 3) * 128 + ((c + (r >> 8)) & 1) * 64 + (r & 63)


def own_scores(place, slope, h, qh, kh, mask):
    pos = places(place, (1, ROWS), 1).astype(F32)
    return jnp.where(mask, mm_nt(qh, kh) * 0.125 + slope[h] * pos, NEG)


def earlier_scores(place, slope, h, qh, kh):
    pos = places(place, (1, ROWS), 1).astype(F32)
    off = jnp.where(place[2] == 1, 0.0, NEG)
    return mm_nt(qh, kh) * 0.125 + (slope[h] * (pos - 512.0) + off)


def own_mask(place):
    return places(place, (ROWS, 1), 0) >= places(place, (1, ROWS), 1)


def attend_own_body(place, slope, q, kv, own):
    mask = own_mask(place)
    for h in range(2):
        lo, hi = h * HD, (h + 1) * HD
        s = own_scores(place, slope, h, q[:, lo:hi], kv[:, lo:hi], mask)
        m = jnp.max(s, axis=-1, keepdims=True)
        p = jnp.exp(s - m)
        own[:, lo:hi] = mm(p.astype(BF), kv[:, 128 + lo : 128 + hi])
        own[:, 128 + lo : 128 + hi] = jnp.broadcast_to(m, (ROWS, HD))
        own[:, 256 + lo : 256 + hi] = jnp.broadcast_to(jnp.sum(p, axis=-1, keepdims=True), (ROWS, HD))


def attend_body(place, slope, q, kvo, pw, own, att, lse, pa, pb):
    outs, logs = [], []
    for h in range(2):
        lo, hi = h * HD, (h + 1) * HD
        s = earlier_scores(place, slope, h, q[:, lo:hi], kvo[:, lo:hi])
        m = own[:, 128 + lo : 129 + lo]
        top = jnp.maximum(m, jnp.max(s, axis=-1, keepdims=True))
        p = jnp.exp(s - top)
        scale = jnp.exp(m - top)
        total = own[:, 256 + lo : 257 + lo] * scale + jnp.sum(p, axis=-1, keepdims=True)
        o = own[:, lo:hi] * scale + mm(p.astype(BF), kvo[:, 128 + lo : 128 + hi])
        outs.append(o / total)
        logs.append(jnp.broadcast_to(top + jnp.log(total), (ROWS, HD)))
    attended = jnp.concatenate(outs, axis=1).astype(BF)
    att[...] = attended
    lse[...] = jnp.concatenate(logs, axis=1)
    w = proj_matrix(pw)
    pa[...] = mm_nt(attended[:HALF], w).astype(BF)
    pb[...] = mm_nt(attended[HALF:], w).astype(BF)


def score_grads(p, doh, vh, atth):
    delta = jnp.sum(doh.astype(F32) * atth.astype(F32), axis=-1, keepdims=True)
    return (p * (mm_nt(doh, vh) - delta)).astype(BF)


def back_earlier_body(place, slope, ma, mb, pw, q, kvo, lse, att, do_ref, dq, dkvo):
    w = proj_matrix(pw)
    do = jnp.concatenate([mm(ma[...], w), mm(mb[...], w)], axis=0).astype(BF)
    do_ref[...] = do
    dqs, dks, dvs = [], [], []
    for h in range(2):
        lo, hi = h * HD, (h + 1) * HD
        qh, kh, vh, doh = q[:, lo:hi], kvo[:, lo:hi], kvo[:, 128 + lo : 128 + hi], do[:, lo:hi]
        p = jnp.exp(earlier_scores(place, slope, h, qh, kh) - lse[:, lo : lo + 1])
        d = score_grads(p, doh, vh, att[:, lo:hi])
        dqs.append(mm(d, kh) * 0.125)
        dks.append(mm_tn(d, qh) * 0.125)
        dvs.append(mm_tn(p.astype(BF), doh))
    dq[...] = jnp.concatenate(dqs, axis=1)
    dkvo[...] = jnp.concatenate(dks + dvs, axis=1).astype(BF)


def back_own_body(place, slope, do, q, kv, lse, att, dq_part, part):
    mask = own_mask(place)
    dqs, dks, dvs = [], [], []
    for h in range(2):
        lo, hi = h * HD, (h + 1) * HD
        qh, kh, vh, doh = q[:, lo:hi], kv[:, lo:hi], kv[:, 128 + lo : 128 + hi], do[:, lo:hi]
        p = jnp.exp(own_scores(place, slope, h, qh, kh, mask) - lse[:, lo : lo + 1])
        d = score_grads(p, doh, vh, att[:, lo:hi])
        dqs.append(mm(d, kh) * 0.125)
        dks.append(mm_tn(d, qh) * 0.125)
        dvs.append(mm_tn(p.astype(BF), doh))
    part[:, :128] = (dq_part[...] + jnp.concatenate(dqs, axis=1)).astype(BF)
    part[:, 128:] = jnp.concatenate(dks + dvs, axis=1).astype(BF)


def ffn_body(na, nb, w1, w2, bias, act, dgel, pa, pb):
    for n, p, at in ((na, pa, 0), (nb, pb, HALF)):
        v = mm(n[...], w1[...]) + bias[...]
        v2 = v * v
        th = jnp.tanh(GELU_SCALE * (v + GELU_CUBE * (v2 * v)))
        one = 0.5 + 0.5 * th
        a = (v * one).astype(BF)
        act[at : at + HALF] = a
        dgel[at : at + HALF] = (
            one
            + (0.5 * GELU_SCALE) * v * (1.0 - th * th) * (1.0 + (3.0 * GELU_CUBE) * v2)
        ).astype(BF)
        p[...] = mm_nt(a, w2[...]).astype(BF)


def ffn_back_body(ea, eb, w1, w2, dgel, hg, sums, pa, pb):
    total = jnp.zeros((1, 512), F32)
    for e, p, at in ((ea, pa, 0), (eb, pb, HALF)):
        g = (mm(e[...], w2[...]) * dgel[at : at + HALF].astype(F32)).astype(BF)
        hg[at : at + HALF] = g
        total += jnp.sum(g.astype(F32), axis=0, keepdims=True)
        p[...] = mm_nt(g, w1[...]).astype(BF)
    sums[...] = total


def ffn_weights_body(ea, eb, act, na, nb, hg, out):
    out[:, :512] = (mm_tn(na[...], hg[:HALF]) + mm_tn(nb[...], hg[HALF:])).astype(BF)
    out[:, 512:] = (mm_tn(ea[...], act[:HALF]) + mm_tn(eb[...], act[HALF:])).astype(BF)


def attn_weights_body(na, nb, joined, ma, mb, att, out):
    out[:, :384] = (
        mm_tn(na[...], joined[:HALF]) + mm_tn(nb[...], joined[HALF:])
    ).astype(BF)
    out[:, 384:] = (mm_tn(ma[...], att[:HALF]) + mm_tn(mb[...], att[HALF:])).astype(BF)


def layer_weights_body(ea, eb, act, sa, sb, hg, na, nb, joined, ma, mb, att, out):
    ffn_weights_body(ea, eb, act, sa, sb, hg, out.at[:, :1024])
    attn_weights_body(na, nb, joined, ma, mb, att, out.at[:, 1024:])


def two_halves(v):
    high = v.astype(BF)
    return high, (v - high.astype(F32)).astype(BF)


def last_pack_body(
    na, nb, joined, ma, mb, att, pa, pb, xa, xb, s21, s11, s20, b13,
    up0, up1, qv0, qv1, out,
):
    g = (mm_tn(na[...], joined[:HALF]) + mm_tn(nb[...], joined[HALF:])).astype(BF)
    out[:, :64, :384] = g.reshape(16, 64, 384)
    g = (mm_tn(ma[...], att[:HALF]) + mm_tn(mb[...], att[HALF:])).astype(BF)
    out[:, :64, 384:] = g.reshape(16, 64, 128)
    gain = jnp.zeros((1, D), F32)
    shift = jnp.zeros((1, D), F32)
    for p, x in ((pa, xa), (pb, xb)):
        g = p[...].astype(F32)
        xhat, _ = norm_parts(x[...].astype(F32))
        gain += jnp.sum(g * xhat, axis=0, keepdims=True)
        shift += jnp.sum(g, axis=0, keepdims=True)
    columns = jnp.concatenate(
        [
            gain, s20[0:1], s11[0:1], s21[0:1],
            shift, s20[2:3], s20[1:2], s11[2:3], s11[1:2], s21[2:3], s21[1:2], b13[...],
        ]
    ).astype(BF)
    q0, q0l = two_halves(qv0[...])
    q1, q1l = two_halves(qv1[...])
    u0, u0l = two_halves(up0[...])
    u1, u1l = two_halves(up1[...])
    none = jnp.zeros((1, 384), BF)
    lines = jnp.concatenate(
        [
            q0, q1, q0l, q1l,
            u0[:, :384], u1[:, :384], u0l[:, :384], u1l[:, :384],
            jnp.concatenate([u0[:, 384:], u1[:, 384:], none[:, :128]], axis=1),
            jnp.concatenate([u0l[:, 384:], u1l[:, 384:], none[:, :128]], axis=1),
            none, none,
        ]
    )
    for w in range(16):
        at = 128 * (w // 2)
        tail = jnp.concatenate([columns[:, at : at + 128], lines], axis=1)
        out[w, 64:80] = jnp.concatenate([tail, jnp.zeros((4, 512), BF)])


def qkv_back_body(part, got, w, joined, sums, pa, pb):
    both = (part[:, 128:].astype(F32) + got[...].astype(F32)).astype(BF)
    j = jnp.concatenate([part[:, :128], both], axis=1)
    joined[...] = j
    sums[...] = jnp.sum(j.astype(F32), axis=0, keepdims=True)
    m = qkv_matrix(w)
    pa[...] = mm_nt(j[:HALF], m).astype(BF)
    pb[...] = mm_nt(j[HALF:], m).astype(BF)


def by_kind(m):
    parts = [m[:, i * HD : (i + 1) * HD] for i in range(6)]
    return jnp.concatenate([parts[i] for i in (0, 3, 1, 4, 2, 5)], axis=1)


def by_head(m):
    parts = [m[:, i * HD : (i + 1) * HD] for i in range(6)]
    return jnp.concatenate([parts[i] for i in (0, 2, 4, 1, 3, 5)], axis=1)


def from_hbm(body, name, arrays, outs):
    count = len(arrays)

    def kernel(*refs):
        given, made = refs[:count], refs[count : count + len(outs)]
        held, sems = refs[count + len(outs) : -1], refs[-1]
        copies = [
            pltpu.make_async_copy(src, dst, sems.at[i])
            for i, (src, dst) in enumerate(zip(given, held))
        ]
        for copy in copies:
            copy.start()
        for copy in copies:
            copy.wait()
        body(*held, *made)

    return pl.pallas_call(
        kernel,
        in_specs=[pl.BlockSpec(memory_space=pltpu.HBM) for _ in arrays],
        out_specs=[pl.BlockSpec(memory_space=pltpu.VMEM) for _ in outs],
        out_shape=outs,
        scratch_shapes=[pltpu.VMEM(a.shape, a.dtype) for a in arrays]
        + [pltpu.SemaphoreType.DMA((count,))],
        compiler_params=pltpu.CompilerParams(vmem_limit_bytes=ROOM.get(name, 6) << 20),
        name=name,
    )(*arrays)


def pack_first_body(qkv, proj, gains, biases, first):
    small = [gains[l, i : i + 1] for l in range(2) for i in range(2)]
    small += [biases[l, i : i + 1] for l in range(2) for i in range(4)]
    lines = jnp.concatenate(
        [jnp.concatenate([small[2 * i], small[2 * i + 1]], axis=1) for i in range(6)]
        + [jnp.zeros((2, 128), BF)]
    )
    own = jnp.concatenate(
        [
            jnp.concatenate([by_kind(qkv[0]), proj[0]], axis=1),
            jnp.concatenate([lines, jnp.zeros((8, 384), BF)], axis=1),
        ]
    )
    for w in range(16):
        first[w] = own


def pack_rest_body(qkv, proj, fc1, fc2, second, third):
    second[:, :512] = fc1[0]
    second[:, 512:1024] = fc2[0]
    second[:, 1024:1152] = jnp.zeros((64, 128), BF)
    second[:, 1152:] = by_kind(qkv[1])
    third[:, :512] = fc1[1]
    third[:, 512:1024] = fc2[1]
    third[:, 1024:] = proj[1]


def sum16(ref, *at):
    total = ref[(0, *at)].astype(F32)
    for w in range(1, 16):
        total += ref[(w, *at)].astype(F32)
    return total


def finish_ffn_body(f0, f1, fc1, fc2):
    for l, total in enumerate((sum16(f0), f1[...].astype(F32))):
        fc1[l] = total[:, :512]
        fc2[l] = total[:, 512:]


def finish_columns_body(odd, mixed, columns):
    own = mixed[0, 64:80, :128].astype(F32)
    for w in range(1, 16):
        own += mixed[w, 64:80, :128].astype(F32)
    columns[...] = jnp.where(odd[0] == 1, own[:12, 64:], own[:12, :64])


def finish_body(mixed, attn1, qkv, proj, qv, up):
    total = sum16(mixed)
    for l, m in enumerate((total[:64], attn1[...].astype(F32))):
        qkv[l] = by_head(m[:, :384])
        proj[l] = m[:, 384:]
    own = total[64:76]
    for l in range(2):
        line = own[l : l + 1, 128:] + own[2 + l : 3 + l, 128:]
        parts = [line[:, i * HD : (i + 1) * HD] for i in (0, 4, 1, 5)]
        qv[l : l + 1] = jnp.concatenate(parts, axis=1)
        near = own[4 + l : 5 + l, 128:] + own[6 + l : 7 + l, 128:]
        at = 128 + 128 * l
        up[l : l + 1] = jnp.concatenate(
            [near, own[8:9, at : at + 128] + own[9:10, at : at + 128]], axis=1
        )


def finish_rows_body(t0, t1, t2, t3, gains, biases):
    total = (t0[...] + t1[...]) + (t2[...] + t3[...])
    for l in range(2):
        gains[l] = total[2 * l : 2 * l + 2]
        biases[l] = total[4 + 4 * l : 8 + 4 * l]


def relative_body(order, x, cot, xr, cr, total):
    for j in range(8):
        row = pl.multiple_of(order[j] * PIECE, PIECE)
        xr[j * PIECE : (j + 1) * PIECE] = x[pl.ds(row, PIECE)]
        cr[j * PIECE : (j + 1) * PIECE] = cot[pl.ds(row, PIECE)]
    total[...] = jnp.sum(cr[:PIECE].astype(F32), axis=0, keepdims=True)


def sequence_body(order, near, far, out):
    for j in range(8):
        row = pl.multiple_of(order[j] * PIECE, PIECE)
        src = near if j < 4 else far
        k = j % 4
        out[pl.ds(row, PIECE)] = src[k * PIECE : (k + 1) * PIECE].astype(out.dtype)


def per_device(
    block_in, qkv_weight, proj_weight, fc1_weight, fc2_weight,
    qv_bias, fc1_bias, norm_gains, row_biases, cotangent,
):
    t = lax.axis_index(T)
    y, c = t // 2, t % 2
    ctx = lax.axis_index("context")
    place = jnp.stack([y, c, ctx]).astype(jnp.int32)
    slope = jnp.exp2(-8.0 * (2 * t + 1 + jnp.arange(2)).astype(F32) / HEADS)
    j = jnp.arange(8)
    order = (2 * ((y - j % 4) % 4) + (c + j // 4) % 2).astype(jnp.int32)
    half = (HALF, D)
    qs, kvs, hs, js = (ROWS, 128), (ROWS, 256), (ROWS, 512), (ROWS, 384)

    (first,) = from_hbm(
        pack_first_body, "pack_first", [qkv_weight, proj_weight, norm_gains, row_biases],
        [sds((16, 72, 512), BF)],
    )
    first, fc1_weight = tie(first, fc1_weight)
    first_all = lax.all_to_all(first, W, 0, 0)
    second_part, third_part = from_hbm(
        pack_rest_body, "pack_rest", [qkv_weight, proj_weight, fc1_weight, fc2_weight],
        [sds((64, 1536), BF), sds((64, 1152), BF)],
    )
    second_all = lax.all_gather(second_part, W, axis=0, tiled=True)
    third_all = lax.all_gather(third_part, W, axis=0, tiled=True)
    table = (
        first_all[:, 64:70, :128].reshape(16, 12, 64).transpose(1, 0, 2).reshape(12, D).astype(F32)
    )
    tab = (table, (12, D), None)
    whole_first = (first_all, (16, 72, 512), None)
    qv = qv_bias.astype(F32).reshape(2, 2, 2, HD).transpose(0, 2, 1, 3)
    zero = jnp.zeros((2, 1, 2, HD), F32)
    joined_bias = jnp.concatenate([qv[:, :1], zero, qv[:, 1:]], axis=1).reshape(2, 1, 384)
    up_bias = fc1_bias.astype(F32).reshape(2, 1, 512)

    x, cot, b13 = call(
        relative_body, "to_relative",
        [(order, None, None), (block_in.reshape(ROWS, D), (ROWS, D), None), (cotangent.reshape(ROWS, D), (ROWS, D), None)],
        [sds((ROWS, D), BF), sds((ROWS, D), BF), sds((1, D), F32)],
    )

    saved = []
    stream = x
    qkv_of = (whole_first, (second_all, (D, 384), (0, 3)))
    proj_of = (whole_first, (third_all, (D, 128), (0, 8)))
    fc1_of = [(m, (D, 512), (0, 0)) for m in (second_all, third_all)]
    fc2_of = [(m, (D, 512), (0, 1)) for m in (second_all, third_all)]

    where = [(place, None, None), (slope, None, None)]
    for l in range(2):
        bias = (joined_bias[l], (1, 384), None)
        if l == 0:
            na, nb, kv = call(
                kv_first_body, "kv_first",
                [(x, half, (0, 0)), (x, half, (1, 0)), whole_first, tab, bias],
                [sds(half, BF), sds(half, BF), sds(kvs, BF)],
            )
        else:
            na, nb = gather_rows(normed)
            (kv,) = call(
                kv_body, "kv", [(na, half, None), (nb, half, None), qkv_of[l], bias], [sds(kvs, BF)]
            )
        kvo = lax.ppermute(kv, "context", [(0, 1)])
        (q,) = call(
            q_body, "q", [(na, half, None), (nb, half, None), qkv_of[l], bias], [sds(qs, BF)]
        )
        (own,) = call(
            attend_own_body, "attend_own", where + [(q, qs, None), (kv, kvs, None)], [sds(js, F32)]
        )
        att, lse, pa, pb = call(
            attend_body, "attend",
            where + [(q, qs, None), (kvo, kvs, None), proj_of[l]] + [(own, js, None)],
            [sds(qs, BF), sds(qs, F32), sds(half, BF), sds(half, BF)],
        )
        middle, second = norm_fwd(
            sum_pieces(pa, pb), stream, table, (l, 1), ((l, 1), (l, 2))
        )
        sa, sb = gather_rows(second)
        act, dgel, pa, pb = call(
            ffn_body, "ffn",
            [(sa, half, None), (sb, half, None), fc1_of[l], fc2_of[l], (up_bias[l], (1, 512), None)],
            [sds(hs, BF), sds(hs, BF), sds(half, BF), sds(half, BF)],
        )
        saved.append((stream, na, nb, q, kv, kvo, att, lse, middle, sa, sb, act, dgel))
        if l == 0:
            stream, normed = norm_fwd(
                sum_pieces(pa, pb), middle, table, (0, 3), ((1, 0), (1, 0))
            )
    out_own = out_rows(sum_pieces(pa, pb), middle, table)

    grad = cot
    ea = (cot, half, (0, 0))
    eb = (cot, half, (1, 0))
    for l in (1, 0):
        stream, na, nb, q, kv, kvo, att, lse, middle, sa, sb, act, dgel = saved[l]
        hg, up_sum, pa, pb = call(
            ffn_back_body, "ffn_back",
            [ea, eb, fc1_of[l], fc2_of[l], (dgel, hs, None)],
            [sds(hs, BF), sds((1, 512), F32), sds(half, BF), sds(half, BF)],
        )
        pieces = sum_pieces(pa, pb)
        ffn_ops = [ea, eb, (act, hs, None), (sa, half, None), (sb, half, None), (hg, hs, None)]
        if l == 1:
            pieces, out_own = tie(pieces, out_own)
        else:
            (ffn_grad,) = call(ffn_weights_body, "ffn_weights", ffn_ops, [sds((D, D), BF)])
            ffn_pieces = lax.all_to_all(ffn_grad.reshape(16, 64, D), W, 0, 0)
        mid, mid_low, s2 = norm_bwd(pieces, middle, grad, table, (l, 1))
        ma, mb = gather_rows(mid_low)
        do, dq, dkvo = call(
            back_earlier_body, "back_earlier",
            where
            + [(ma, half, None), (mb, half, None), proj_of[l], (q, qs, None), (kvo, kvs, None), (lse, qs, None), (att, qs, None)],
            [sds(qs, BF), sds(qs, F32), sds(kvs, BF)],
        )
        got = lax.ppermute(dkvo, "context", [(1, 0)])
        (part,) = call(
            back_own_body, "back_own",
            where
            + [(do, qs, None), (q, qs, None), (kv, kvs, None), (lse, qs, None), (att, qs, None), (dq, qs, None)],
            [sds(js, BF)],
        )
        if l == 1:
            part, out_own = tie(part, out_own)
            oa, ob = gather_rows(out_own)
        else:
            part, oa = tie(part, oa)
            (block_out,) = call(
                sequence_body, "to_sequence",
                [(order, None, None), (oa, half, None), (ob, half, None)],
                [sds((ROWS, D), BF)],
            )
            got, block_out, ffn_pieces = tie(got, block_out, ffn_pieces)
        joined, qv_sum, pa, pb = call(
            qkv_back_body, "qkv_back",
            [(part, js, None), (got, kvs, None), qkv_of[l]],
            [sds(js, BF), sds((1, 384), F32), sds(half, BF), sds(half, BF)],
        )
        pieces = sum_pieces(pa, pb)
        attn_ops = [(na, half, None), (nb, half, None), (joined, js, None), (ma, half, None), (mb, half, None), (att, qs, None)]
        if l == 1:
            (weights_grad,) = call(
                layer_weights_body, "layer_weights", ffn_ops + attn_ops, [sds((D, 1536), BF)]
            )
            pieces, oa, weights_grad = tie(pieces, oa, weights_grad)
            owned1 = lax.psum_scatter(weights_grad, W, scatter_dimension=0, tiled=True)
            up1, qv1, s21 = up_sum, qv_sum, s2
            grad, low, s11 = norm_bwd(pieces, stream, mid, table, (1, 0))
            near, far = gather_rows(low)
            ea, eb = (near, half, None), (far, half, None)
        else:
            three, one = (3, D), (1, D)
            (packed,) = call(
                last_pack_body, "last_pack",
                attn_ops
                + [(pa, half, None), (pb, half, None), (x, half, (0, 0)), (x, half, (1, 0))]
                + [(s21, three, None), (s11, three, None), (s2, three, None), (b13, one, None)]
                + [(up_sum, (1, 512), None), (up1, (1, 512), None), (qv_sum, (1, 384), None), (qv1, (1, 384), None)],
                [sds((16, 80, 512), BF)],
            )
            mixed = lax.all_to_all(packed, W, 0, 0)
            _, low, _ = norm_bwd(pieces, stream, mid, table, (0, 0))
            near, far = gather_rows(low)
            near, ffn_pieces = tie(near, ffn_pieces)
            fc1_grad, fc2_grad = call(
                finish_ffn_body, "finish_ffn",
                [(ffn_pieces, (16, 64, D), None), (owned1, (64, D), (0, 0))],
                [sds((2, 64, 512), F32), sds((2, 64, 512), F32)],
            )
            near, fc1_grad, fc2_grad = tie(near, fc1_grad, fc2_grad)
            (input_grad,) = call(
                sequence_body, "to_sequence",
                [(order, None, None), (near, half, None), (far, half, None)],
                [sds((ROWS, D), F32)],
            )
    odd = ctx.astype(jnp.int32).reshape(1)
    small = (12, 64)
    (tail,) = call(
        finish_columns_body, "finish_columns",
        [(odd, None, None), (mixed, (16, 80, 512), None)],
        [sds(small, F32)],
    )
    tail = tail + core_swap(tail)
    tails = [tail] + [along_y(tail, step) for step in (1, 2, 3)]
    qkv_grad, proj_grad, qv_grad, up_grad = call(
        finish_body, "finish",
        [(mixed, (16, 80, 512), None), (owned1, (64, 512), (0, 2))],
        [sds((2, 64, 384), F32), sds((2, 64, 128), F32), sds((2, 256), F32), sds((2, 512), F32)],
    )
    tails, input_grad, qkv_grad = tie(tails, input_grad, qkv_grad)
    gains_grad, biases_grad = call(
        finish_rows_body, "finish_rows",
        [(v, small, None) for v in tails],
        [sds((2, 2, 64), F32), sds((2, 4, 64), F32)],
    )
    return (
        block_out[None], input_grad[None], qkv_grad, proj_grad, fc1_grad, fc2_grad,
        qv_grad, up_grad, gains_grad, biases_grad,
    )


def solution(mesh):
    return jax.shard_map(
        per_device,
        mesh=mesh,
        in_specs=(
            P("shard", "context", None),
            P(None, W, T),
            P(None, W, T),
            P(None, W, T),
            P(None, W, T),
            P(None, T),
            P(None, T),
            P(None, None, W),
            P(None, None, W),
            P("shard", "context", None),
        ),
        out_specs=(
            P("shard", "context", None),
            P("shard", "context", None),
            P(None, W, T),
            P(None, W, T),
            P(None, W, T),
            P(None, W, T),
            P(None, T),
            P(None, T),
            P(None, None, W),
            P(None, None, W),
        ),
        check_vma=False,
    )
```

```python
import jax
import jax.numpy as jnp
from jax import lax
from jax.experimental import pallas as pl
from jax.experimental.pallas import tpu as pltpu
from jax.sharding import PartitionSpec as P

HEADS = 16
HD = 64
NORM_EPS = 1e-05
GELU_SCALE = 0.7978845608028654
GELU_CUBE = 0.044715
F32 = jnp.float32
BF = jnp.bfloat16
W = ("shard", "context")
T = "tensor"
ROWS = 512
HALF = 256
PIECE = 64
D = 1024
NEG = -1e30
ROOM = {
    "kv_first": 10, "kv": 8, "q": 8, "attend_own": 12, "attend": 12, "ffn": 14, "ffn_back": 12,
    "back_earlier": 14, "back_own": 12, "qkv_back": 10, "ffn_weights": 14, "layer_weights": 20,
    "last_pack": 16, "to_relative": 8, "to_sequence": 8, "finish_ffn": 8,
}


def spec(shape, index=None):
    place = tuple(index) if index is not None else (0,) * len(shape)
    return pl.BlockSpec(shape, lambda i: place)


def smem():
    return pl.BlockSpec(memory_space=pltpu.SMEM)


def call(body, name, operands, outs):
    in_specs, args = [], []
    for array, shape, index in operands:
        in_specs.append(smem() if shape is None else spec(shape, index))
        args.append(array)
    return pl.pallas_call(
        body,
        grid=(1,),
        in_specs=in_specs,
        out_specs=[spec(o.shape) for o in outs],
        out_shape=outs,
        compiler_params=pltpu.CompilerParams(vmem_limit_bytes=ROOM.get(name, 6) << 20),
        name=name,
    )(*args)


def sds(shape, dtype):
    return jax.ShapeDtypeStruct(shape, dtype)


def mm(a, b):
    return lax.dot_general(a, b, (((1,), (0,)), ((), ())), preferred_element_type=F32)


def mm_nt(a, b):
    return lax.dot_general(a, b, (((1,), (1,)), ((), ())), preferred_element_type=F32)


def mm_tn(a, b):
    return lax.dot_general(a, b, (((0,), (0,)), ((), ())), preferred_element_type=F32)


def core_swap(v):
    return lax.ppermute(v, T, [(i, i ^ 1) for i in range(8)])


def along_y(v, step):
    return lax.ppermute(
        v, T, [(2 * y + c, 2 * ((y + step) % 4) + c) for y in range(4) for c in range(2)]
    )


def add_body(pa, got, h0, h1, h2, h3):
    both = pa[...].astype(F32) + got[...].astype(F32)
    h0[...] = both[:PIECE]
    h1[...] = both[PIECE : 2 * PIECE].astype(BF)
    h2[...] = both[2 * PIECE : 3 * PIECE].astype(BF)
    h3[...] = both[3 * PIECE :].astype(BF)


def tie(*values):
    return lax.optimization_barrier(values)


def chip_sums(keep, send):
    got = core_swap(send)
    return call(
        add_body,
        "pair_add",
        [(keep, (HALF, D), None), (got, (HALF, D), None)],
        [sds((PIECE, D), F32)] + [sds((PIECE, D), BF)] * 3,
    )


def spread(sums):
    h0, h1, h2, h3 = sums
    r2 = along_y(h2, -2)
    r1 = along_y(h1, -1)
    r3 = along_y(h3, -3)
    return h0, r1, r2, r3


def sum_pieces(keep, send):
    return spread(chip_sums(keep, send))


def gather_near(own):
    r2 = along_y(own, 2)
    r1 = along_y(own, 1)
    r3 = along_y(own, 3)
    return jnp.concatenate([own, r1, r2, r3], axis=0)


def gather_rows(own):
    near = gather_near(own)
    return near, core_swap(near)


def norm_parts(v):
    mean = jnp.mean(v, axis=-1, keepdims=True)
    centred = v - mean
    var = jnp.mean(centred * centred, axis=-1, keepdims=True)
    s = lax.rsqrt(var + NORM_EPS)
    return centred * s, s


def gain_row(table, l, i):
    at = 2 * l + i
    return table[at : at + 1]


def bias_row(table, l, i):
    at = 4 + 4 * l + i
    return table[at : at + 1]


def norm_fwd(pieces, resid, table, bias_at, next_at):
    def body(h0, r1, r2, r3, resid_ref, rows, stream, normed):
        v = (
            h0[...] + r1[...].astype(F32) + r2[...].astype(F32) + r3[...].astype(F32)
        ) + resid_ref[...].astype(F32) + bias_row(rows, *bias_at)
        stream[...] = v
        xhat, _ = norm_parts(v)
        gain, shift = next_at
        normed[...] = (xhat * gain_row(rows, *gain) + bias_row(rows, *shift)).astype(BF)

    b = (PIECE, D)
    return call(
        body,
        "norm_fwd",
        [(p, b, None) for p in (*pieces, resid)] + [(table, (12, D), None)],
        [sds(b, F32), sds(b, BF)],
    )


def out_rows(pieces, resid, table):
    def body(h0, r1, r2, r3, resid_ref, rows, out):
        out[...] = (
            (h0[...] + r1[...].astype(F32) + r2[...].astype(F32) + r3[...].astype(F32))
            + resid_ref[...]
            + bias_row(rows, 1, 3)
        ).astype(BF)

    b = (PIECE, D)
    return call(
        body,
        "out_rows",
        [(p, b, None) for p in (*pieces, resid)] + [(table, (12, D), None)],
        [sds(b, BF)],
    )[0]


def norm_bwd(pieces, stream, grad, table, gain_at):
    def body(h0, r1, r2, r3, stream_ref, grad_ref, rows, out, low, sums):
        g = h0[...] + r1[...].astype(F32) + r2[...].astype(F32) + r3[...].astype(F32)
        xhat, s = norm_parts(stream_ref[...].astype(F32))
        gx = g * xhat
        c = g * gain_row(rows, *gain_at)
        cx = c * xhat
        e = grad_ref[...].astype(F32) + s * (
            c
            - jnp.mean(c, axis=-1, keepdims=True)
            - xhat * jnp.mean(cx, axis=-1, keepdims=True)
        )
        out[...] = e
        low[...] = e.astype(BF)
        sums[0:1] = jnp.sum(gx, axis=0, keepdims=True)
        sums[1:2] = jnp.sum(g, axis=0, keepdims=True)
        sums[2:3] = jnp.sum(e, axis=0, keepdims=True)

    b = (PIECE, D)
    return call(
        body,
        "norm_bwd",
        [(p, b, None) for p in (*pieces, stream, grad)] + [(table, (12, D), None)],
        [sds(b, F32), sds(b, BF), sds((3, D), F32)],
    )


def kv_first_body(xa, xb, first, rows, bias, na, nb, kv):
    w = qkv_matrix(first)[:, 128:]
    for x, n, at in ((xa, na, 0), (xb, nb, HALF)):
        xhat, _ = norm_parts(x[...].astype(F32))
        normed = (xhat * gain_row(rows, 0, 0) + bias_row(rows, 0, 0)).astype(BF)
        n[...] = normed
        kv[at : at + HALF] = (mm(normed, w) + bias[:, 128:]).astype(BF)


def kv_body(na, nb, w, bias, kv):
    for n, at in ((na, 0), (nb, HALF)):
        kv[at : at + HALF] = (mm(n[...], w[:, 128:]) + bias[:, 128:]).astype(BF)


def q_body(na, nb, w, bias, q):
    m = qkv_matrix(w)[:, :128]
    for n, at in ((na, 0), (nb, HALF)):
        q[at : at + HALF] = (mm(n[...], m) + bias[:, :128]).astype(BF)


def proj_matrix(ref):
    return ref[:, :64, 384:].reshape(D, 128) if len(ref.shape) == 3 else ref[...]


def qkv_matrix(ref):
    return ref[:, :64, :384].reshape(D, 384) if len(ref.shape) == 3 else ref[...]


def places(place, shape, axis):
    r = lax.broadcasted_iota(jnp.int32, shape, axis)
    y, c = place[0], place[1]
    return ((y - ((r >> 6) & 3)) & 3) * 128 + ((c + (r >> 8)) & 1) * 64 + (r & 63)


def own_scores(place, slope, h, qh, kh, mask):
    pos = places(place, (1, ROWS), 1).astype(F32)
    return jnp.where(mask, mm_nt(qh, kh) * 0.125 + slope[h] * pos, NEG)


def earlier_scores(place, slope, h, qh, kh):
    pos = places(place, (1, ROWS), 1).astype(F32)
    off = jnp.where(place[2] == 1, 0.0, NEG)
    return mm_nt(qh, kh) * 0.125 + (slope[h] * (pos - 512.0) + off)


def own_mask(place):
    return places(place, (ROWS, 1), 0) >= places(place, (1, ROWS), 1)


def attend_own_body(place, slope, q, kv, own):
    mask = own_mask(place)
    for h in range(2):
        lo, hi = h * HD, (h + 1) * HD
        s = own_scores(place, slope, h, q[:, lo:hi], kv[:, lo:hi], mask)
        m = jnp.max(s, axis=-1, keepdims=True)
        p = jnp.exp(s - m)
        own[:, lo:hi] = mm(p.astype(BF), kv[:, 128 + lo : 128 + hi])
        own[:, 128 + lo : 128 + hi] = jnp.broadcast_to(m, (ROWS, HD))
        own[:, 256 + lo : 256 + hi] = jnp.broadcast_to(jnp.sum(p, axis=-1, keepdims=True), (ROWS, HD))


def attend_body(place, slope, q, kvo, pw, own, att, lse, pa, pb):
    outs, logs = [], []
    for h in range(2):
        lo, hi = h * HD, (h + 1) * HD
        s = earlier_scores(place, slope, h, q[:, lo:hi], kvo[:, lo:hi])
        m = own[:, 128 + lo : 129 + lo]
        top = jnp.maximum(m, jnp.max(s, axis=-1, keepdims=True))
        p = jnp.exp(s - top)
        scale = jnp.exp(m - top)
        total = own[:, 256 + lo : 257 + lo] * scale + jnp.sum(p, axis=-1, keepdims=True)
        o = own[:, lo:hi] * scale + mm(p.astype(BF), kvo[:, 128 + lo : 128 + hi])
        outs.append(o / total)
        logs.append(jnp.broadcast_to(top + jnp.log(total), (ROWS, HD)))
    attended = jnp.concatenate(outs, axis=1).astype(BF)
    att[...] = attended
    lse[...] = jnp.concatenate(logs, axis=1)
    w = proj_matrix(pw)
    pa[...] = mm_nt(attended[:HALF], w).astype(BF)
    pb[...] = mm_nt(attended[HALF:], w).astype(BF)


def score_grads(p, doh, vh, atth):
    delta = jnp.sum(doh.astype(F32) * atth.astype(F32), axis=-1, keepdims=True)
    return (p * (mm_nt(doh, vh) - delta)).astype(BF)


def back_earlier_body(place, slope, ma, mb, pw, q, kvo, lse, att, do_ref, dq, dkvo):
    w = proj_matrix(pw)
    do = jnp.concatenate([mm(ma[...], w), mm(mb[...], w)], axis=0).astype(BF)
    do_ref[...] = do
    dqs, dks, dvs = [], [], []
    for h in range(2):
        lo, hi = h * HD, (h + 1) * HD
        qh, kh, vh, doh = q[:, lo:hi], kvo[:, lo:hi], kvo[:, 128 + lo : 128 + hi], do[:, lo:hi]
        p = jnp.exp(earlier_scores(place, slope, h, qh, kh) - lse[:, lo : lo + 1])
        d = score_grads(p, doh, vh, att[:, lo:hi])
        dqs.append(mm(d, kh) * 0.125)
        dks.append(mm_tn(d, qh) * 0.125)
        dvs.append(mm_tn(p.astype(BF), doh))
    dq[...] = jnp.concatenate(dqs, axis=1)
    dkvo[...] = jnp.concatenate(dks + dvs, axis=1).astype(BF)


def back_own_body(place, slope, do, q, kv, lse, att, dq_part, part):
    mask = own_mask(place)
    dqs, dks, dvs = [], [], []
    for h in range(2):
        lo, hi = h * HD, (h + 1) * HD
        qh, kh, vh, doh = q[:, lo:hi], kv[:, lo:hi], kv[:, 128 + lo : 128 + hi], do[:, lo:hi]
        p = jnp.exp(own_scores(place, slope, h, qh, kh, mask) - lse[:, lo : lo + 1])
        d = score_grads(p, doh, vh, att[:, lo:hi])
        dqs.append(mm(d, kh) * 0.125)
        dks.append(mm_tn(d, qh) * 0.125)
        dvs.append(mm_tn(p.astype(BF), doh))
    part[:, :128] = (dq_part[...] + jnp.concatenate(dqs, axis=1)).astype(BF)
    part[:, 128:] = jnp.concatenate(dks + dvs, axis=1).astype(BF)


def ffn_body(na, nb, w1, w2, bias, act, dgel, pa, pb):
    for n, p, at in ((na, pa, 0), (nb, pb, HALF)):
        v = mm(n[...], w1[...]) + bias[...]
        v2 = v * v
        th = jnp.tanh(GELU_SCALE * (v + GELU_CUBE * (v2 * v)))
        one = 0.5 + 0.5 * th
        a = (v * one).astype(BF)
        act[at : at + HALF] = a
        dgel[at : at + HALF] = (
            one
            + (0.5 * GELU_SCALE) * v * (1.0 - th * th) * (1.0 + (3.0 * GELU_CUBE) * v2)
        ).astype(BF)
        p[...] = mm_nt(a, w2[...]).astype(BF)


def ffn_back_body(ea, eb, w1, w2, dgel, hg, sums, pa, pb):
    total = jnp.zeros((1, 512), F32)
    for e, p, at in ((ea, pa, 0), (eb, pb, HALF)):
        g = (mm(e[...], w2[...]) * dgel[at : at + HALF].astype(F32)).astype(BF)
        hg[at : at + HALF] = g
        total += jnp.sum(g.astype(F32), axis=0, keepdims=True)
        p[...] = mm_nt(g, w1[...]).astype(BF)
    sums[...] = total


def ffn_weights_body(ea, eb, act, na, nb, hg, out):
    out[:, :512] = (mm_tn(na[...], hg[:HALF]) + mm_tn(nb[...], hg[HALF:])).astype(BF)
    out[:, 512:] = (mm_tn(ea[...], act[:HALF]) + mm_tn(eb[...], act[HALF:])).astype(BF)


def attn_weights_body(na, nb, joined, ma, mb, att, out):
    out[:, :384] = (
        mm_tn(na[...], joined[:HALF]) + mm_tn(nb[...], joined[HALF:])
    ).astype(BF)
    out[:, 384:] = (mm_tn(ma[...], att[:HALF]) + mm_tn(mb[...], att[HALF:])).astype(BF)


def layer_weights_body(ea, eb, act, sa, sb, hg, na, nb, joined, ma, mb, att, out):
    ffn_weights_body(ea, eb, act, sa, sb, hg, out.at[:, :1024])
    attn_weights_body(na, nb, joined, ma, mb, att, out.at[:, 1024:])


def two_halves(v):
    high = v.astype(BF)
    return high, (v - high.astype(F32)).astype(BF)


def last_pack_body(
    na, nb, joined, ma, mb, att, pa, pb, xa, xb, s21, s11, s20, b13,
    up0, up1, qv0, qv1, out,
):
    g = (mm_tn(na[...], joined[:HALF]) + mm_tn(nb[...], joined[HALF:])).astype(BF)
    out[:, :64, :384] = g.reshape(16, 64, 384)
    g = (mm_tn(ma[...], att[:HALF]) + mm_tn(mb[...], att[HALF:])).astype(BF)
    out[:, :64, 384:] = g.reshape(16, 64, 128)
    gain = jnp.zeros((1, D), F32)
    shift = jnp.zeros((1, D), F32)
    for p, x in ((pa, xa), (pb, xb)):
        g = p[...].astype(F32)
        xhat, _ = norm_parts(x[...].astype(F32))
        gain += jnp.sum(g * xhat, axis=0, keepdims=True)
        shift += jnp.sum(g, axis=0, keepdims=True)
    columns = jnp.concatenate(
        [
            gain, s20[0:1], s11[0:1], s21[0:1],
            shift, s20[2:3], s20[1:2], s11[2:3], s11[1:2], s21[2:3], s21[1:2], b13[...],
        ]
    ).astype(BF)
    q0, q0l = two_halves(qv0[...])
    q1, q1l = two_halves(qv1[...])
    u0, u0l = two_halves(up0[...])
    u1, u1l = two_halves(up1[...])
    none = jnp.zeros((1, 384), BF)
    lines = jnp.concatenate(
        [
            q0, q1, q0l, q1l,
            u0[:, :384], u1[:, :384], u0l[:, :384], u1l[:, :384],
            jnp.concatenate([u0[:, 384:], u1[:, 384:], none[:, :128]], axis=1),
            jnp.concatenate([u0l[:, 384:], u1l[:, 384:], none[:, :128]], axis=1),
            none, none,
        ]
    )
    for w in range(16):
        at = 128 * (w // 2)
        tail = jnp.concatenate([columns[:, at : at + 128], lines], axis=1)
        out[w, 64:80] = jnp.concatenate([tail, jnp.zeros((4, 512), BF)])


def qkv_back_body(part, got, w, joined, sums, pa, pb):
    both = (part[:, 128:].astype(F32) + got[...].astype(F32)).astype(BF)
    j = jnp.concatenate([part[:, :128], both], axis=1)
    joined[...] = j
    sums[...] = jnp.sum(j.astype(F32), axis=0, keepdims=True)
    m = qkv_matrix(w)
    pa[...] = mm_nt(j[:HALF], m).astype(BF)
    pb[...] = mm_nt(j[HALF:], m).astype(BF)


def by_kind(m):
    parts = [m[:, i * HD : (i + 1) * HD] for i in range(6)]
    return jnp.concatenate([parts[i] for i in (0, 3, 1, 4, 2, 5)], axis=1)


def by_head(m):
    parts = [m[:, i * HD : (i + 1) * HD] for i in range(6)]
    return jnp.concatenate([parts[i] for i in (0, 2, 4, 1, 3, 5)], axis=1)


def from_hbm(body, name, arrays, outs):
    count = len(arrays)

    def kernel(*refs):
        given, made = refs[:count], refs[count : count + len(outs)]
        held, sems = refs[count + len(outs) : -1], refs[-1]
        copies = [
            pltpu.make_async_copy(src, dst, sems.at[i])
            for i, (src, dst) in enumerate(zip(given, held))
        ]
        for copy in copies:
            copy.start()
        for copy in copies:
            copy.wait()
        body(*held, *made)

    return pl.pallas_call(
        kernel,
        in_specs=[pl.BlockSpec(memory_space=pltpu.HBM) for _ in arrays],
        out_specs=[pl.BlockSpec(memory_space=pltpu.VMEM) for _ in outs],
        out_shape=outs,
        scratch_shapes=[pltpu.VMEM(a.shape, a.dtype) for a in arrays]
        + [pltpu.SemaphoreType.DMA((count,))],
        compiler_params=pltpu.CompilerParams(vmem_limit_bytes=ROOM.get(name, 6) << 20),
        name=name,
    )(*arrays)


def pack_first_body(qkv, proj, gains, biases, first):
    small = [gains[l, i : i + 1] for l in range(2) for i in range(2)]
    small += [biases[l, i : i + 1] for l in range(2) for i in range(4)]
    lines = jnp.concatenate(
        [jnp.concatenate([small[2 * i], small[2 * i + 1]], axis=1) for i in range(6)]
        + [jnp.zeros((2, 128), BF)]
    )
    own = jnp.concatenate(
        [
            jnp.concatenate([by_kind(qkv[0]), proj[0]], axis=1),
            jnp.concatenate([lines, jnp.zeros((8, 384), BF)], axis=1),
        ]
    )
    for w in range(16):
        first[w] = own


def pack_rest_body(qkv, proj, fc1, fc2, second, third):
    second[:, :512] = fc1[0]
    second[:, 512:1024] = fc2[0]
    second[:, 1024:1152] = jnp.zeros((64, 128), BF)
    second[:, 1152:] = by_kind(qkv[1])
    third[:, :512] = fc1[1]
    third[:, 512:1024] = fc2[1]
    third[:, 1024:] = proj[1]


def sum16(ref, *at):
    total = ref[(0, *at)].astype(F32)
    for w in range(1, 16):
        total += ref[(w, *at)].astype(F32)
    return total


def finish_ffn_body(f0, f1, fc1, fc2):
    for l, total in enumerate((sum16(f0), f1[...].astype(F32))):
        fc1[l] = total[:, :512]
        fc2[l] = total[:, 512:]


def finish_columns_body(odd, mixed, columns):
    own = mixed[0, 64:80, :128].astype(F32)
    for w in range(1, 16):
        own += mixed[w, 64:80, :128].astype(F32)
    columns[...] = jnp.where(odd[0] == 1, own[:12, 64:], own[:12, :64])


def finish_body(mixed, attn1, qkv, proj, qv, up):
    total = sum16(mixed)
    for l, m in enumerate((total[:64], attn1[...].astype(F32))):
        qkv[l] = by_head(m[:, :384])
        proj[l] = m[:, 384:]
    own = total[64:76]
    for l in range(2):
        line = own[l : l + 1, 128:] + own[2 + l : 3 + l, 128:]
        parts = [line[:, i * HD : (i + 1) * HD] for i in (0, 4, 1, 5)]
        qv[l : l + 1] = jnp.concatenate(parts, axis=1)
        near = own[4 + l : 5 + l, 128:] + own[6 + l : 7 + l, 128:]
        at = 128 + 128 * l
        up[l : l + 1] = jnp.concatenate(
            [near, own[8:9, at : at + 128] + own[9:10, at : at + 128]], axis=1
        )


def finish_rows_body(t0, t1, t2, t3, gains, biases):
    total = (t0[...] + t1[...]) + (t2[...] + t3[...])
    for l in range(2):
        gains[l] = total[2 * l : 2 * l + 2]
        biases[l] = total[4 + 4 * l : 8 + 4 * l]


def relative_body(order, x, cot, xr, cr, total):
    for j in range(8):
        row = pl.multiple_of(order[j] * PIECE, PIECE)
        xr[j * PIECE : (j + 1) * PIECE] = x[pl.ds(row, PIECE)]
        cr[j * PIECE : (j + 1) * PIECE] = cot[pl.ds(row, PIECE)]
    total[...] = jnp.sum(cr[:PIECE].astype(F32), axis=0, keepdims=True)


def sequence_body(order, near, far, out):
    for j in range(8):
        row = pl.multiple_of(order[j] * PIECE, PIECE)
        src = near if j < 4 else far
        k = j % 4
        out[pl.ds(row, PIECE)] = src[k * PIECE : (k + 1) * PIECE].astype(out.dtype)


def per_device(
    block_in, qkv_weight, proj_weight, fc1_weight, fc2_weight,
    qv_bias, fc1_bias, norm_gains, row_biases, cotangent,
):
    t = lax.axis_index(T)
    y, c = t // 2, t % 2
    ctx = lax.axis_index("context")
    place = jnp.stack([y, c, ctx]).astype(jnp.int32)
    slope = jnp.exp2(-8.0 * (2 * t + 1 + jnp.arange(2)).astype(F32) / HEADS)
    j = jnp.arange(8)
    order = (2 * ((y - j % 4) % 4) + (c + j // 4) % 2).astype(jnp.int32)
    half = (HALF, D)
    qs, kvs, hs, js = (ROWS, 128), (ROWS, 256), (ROWS, 512), (ROWS, 384)

    (first,) = from_hbm(
        pack_first_body, "pack_first", [qkv_weight, proj_weight, norm_gains, row_biases],
        [sds((16, 72, 512), BF)],
    )
    first, fc1_weight = tie(first, fc1_weight)
    first_all = lax.all_to_all(first, W, 0, 0)
    second_part, third_part = from_hbm(
        pack_rest_body, "pack_rest", [qkv_weight, proj_weight, fc1_weight, fc2_weight],
        [sds((64, 1536), BF), sds((64, 1152), BF)],
    )
    second_all = lax.all_gather(second_part, W, axis=0, tiled=True)
    third_all = lax.all_gather(third_part, W, axis=0, tiled=True)
    table = (
        first_all[:, 64:70, :128].reshape(16, 12, 64).transpose(1, 0, 2).reshape(12, D).astype(F32)
    )
    tab = (table, (12, D), None)
    whole_first = (first_all, (16, 72, 512), None)
    qv = qv_bias.astype(F32).reshape(2, 2, 2, HD).transpose(0, 2, 1, 3)
    zero = jnp.zeros((2, 1, 2, HD), F32)
    joined_bias = jnp.concatenate([qv[:, :1], zero, qv[:, 1:]], axis=1).reshape(2, 1, 384)
    up_bias = fc1_bias.astype(F32).reshape(2, 1, 512)

    x, cot, b13 = call(
        relative_body, "to_relative",
        [(order, None, None), (block_in.reshape(ROWS, D), (ROWS, D), None), (cotangent.reshape(ROWS, D), (ROWS, D), None)],
        [sds((ROWS, D), BF), sds((ROWS, D), BF), sds((1, D), F32)],
    )

    saved = []
    stream = x
    qkv_of = (whole_first, (second_all, (D, 384), (0, 3)))
    proj_of = (whole_first, (third_all, (D, 128), (0, 8)))
    fc1_of = [(m, (D, 512), (0, 0)) for m in (second_all, third_all)]
    fc2_of = [(m, (D, 512), (0, 1)) for m in (second_all, third_all)]

    where = [(place, None, None), (slope, None, None)]
    for l in range(2):
        bias = (joined_bias[l], (1, 384), None)
        if l == 0:
            na, nb, kv = call(
                kv_first_body, "kv_first",
                [(x, half, (0, 0)), (x, half, (1, 0)), whole_first, tab, bias],
                [sds(half, BF), sds(half, BF), sds(kvs, BF)],
            )
        else:
            na, nb = gather_rows(normed)
            (kv,) = call(
                kv_body, "kv", [(na, half, None), (nb, half, None), qkv_of[l], bias], [sds(kvs, BF)]
            )
        kvo = lax.ppermute(kv, "context", [(0, 1)])
        (q,) = call(
            q_body, "q", [(na, half, None), (nb, half, None), qkv_of[l], bias], [sds(qs, BF)]
        )
        (own,) = call(
            attend_own_body, "attend_own", where + [(q, qs, None), (kv, kvs, None)], [sds(js, F32)]
        )
        att, lse, pa, pb = call(
            attend_body, "attend",
            where + [(q, qs, None), (kvo, kvs, None), proj_of[l]] + [(own, js, None)],
            [sds(qs, BF), sds(qs, F32), sds(half, BF), sds(half, BF)],
        )
        middle, second = norm_fwd(
            sum_pieces(pa, pb), stream, table, (l, 1), ((l, 1), (l, 2))
        )
        sa, sb = gather_rows(second)
        act, dgel, pa, pb = call(
            ffn_body, "ffn",
            [(sa, half, None), (sb, half, None), fc1_of[l], fc2_of[l], (up_bias[l], (1, 512), None)],
            [sds(hs, BF), sds(hs, BF), sds(half, BF), sds(half, BF)],
        )
        saved.append((stream, na, nb, q, kv, kvo, att, lse, middle, sa, sb, act, dgel))
        if l == 0:
            stream, normed = norm_fwd(
                sum_pieces(pa, pb), middle, table, (0, 3), ((1, 0), (1, 0))
            )
    out_own = out_rows(sum_pieces(pa, pb), middle, table)

    grad = cot
    ea = (cot, half, (0, 0))
    eb = (cot, half, (1, 0))
    for l in (1, 0):
        stream, na, nb, q, kv, kvo, att, lse, middle, sa, sb, act, dgel = saved[l]
        hg, up_sum, pa, pb = call(
            ffn_back_body, "ffn_back",
            [ea, eb, fc1_of[l], fc2_of[l], (dgel, hs, None)],
            [sds(hs, BF), sds((1, 512), F32), sds(half, BF), sds(half, BF)],
        )
        pieces = sum_pieces(pa, pb)
        ffn_ops = [ea, eb, (act, hs, None), (sa, half, None), (sb, half, None), (hg, hs, None)]
        if l == 1:
            pieces, out_own = tie(pieces, out_own)
        else:
            (ffn_grad,) = call(ffn_weights_body, "ffn_weights", ffn_ops, [sds((D, D), BF)])
            ffn_pieces = lax.all_to_all(ffn_grad.reshape(16, 64, D), W, 0, 0)
        mid, mid_low, s2 = norm_bwd(pieces, middle, grad, table, (l, 1))
        ma, mb = gather_rows(mid_low)
        do, dq, dkvo = call(
            back_earlier_body, "back_earlier",
            where
            + [(ma, half, None), (mb, half, None), proj_of[l], (q, qs, None), (kvo, kvs, None), (lse, qs, None), (att, qs, None)],
            [sds(qs, BF), sds(qs, F32), sds(kvs, BF)],
        )
        got = lax.ppermute(dkvo, "context", [(1, 0)])
        (part,) = call(
            back_own_body, "back_own",
            where
            + [(do, qs, None), (q, qs, None), (kv, kvs, None), (lse, qs, None), (att, qs, None), (dq, qs, None)],
            [sds(js, BF)],
        )
        if l == 1:
            part, out_own = tie(part, out_own)
            oa, ob = gather_rows(out_own)
        else:
            part, oa = tie(part, oa)
            (block_out,) = call(
                sequence_body, "to_sequence",
                [(order, None, None), (oa, half, None), (ob, half, None)],
                [sds((ROWS, D), BF)],
            )
            got, block_out, ffn_pieces = tie(got, block_out, ffn_pieces)
        joined, qv_sum, pa, pb = call(
            qkv_back_body, "qkv_back",
            [(part, js, None), (got, kvs, None), qkv_of[l]],
            [sds(js, BF), sds((1, 384), F32), sds(half, BF), sds(half, BF)],
        )
        pieces = sum_pieces(pa, pb)
        attn_ops = [(na, half, None), (nb, half, None), (joined, js, None), (ma, half, None), (mb, half, None), (att, qs, None)]
        if l == 1:
            (weights_grad,) = call(
                layer_weights_body, "layer_weights", ffn_ops + attn_ops, [sds((D, 1536), BF)]
            )
            pieces, oa, weights_grad = tie(pieces, oa, weights_grad)
            owned1 = lax.psum_scatter(weights_grad, W, scatter_dimension=0, tiled=True)
            up1, qv1, s21 = up_sum, qv_sum, s2
            grad, low, s11 = norm_bwd(pieces, stream, mid, table, (1, 0))
            near, far = gather_rows(low)
            ea, eb = (near, half, None), (far, half, None)
        else:
            three, one = (3, D), (1, D)
            (packed,) = call(
                last_pack_body, "last_pack",
                attn_ops
                + [(pa, half, None), (pb, half, None), (x, half, (0, 0)), (x, half, (1, 0))]
                + [(s21, three, None), (s11, three, None), (s2, three, None), (b13, one, None)]
                + [(up_sum, (1, 512), None), (up1, (1, 512), None), (qv_sum, (1, 384), None), (qv1, (1, 384), None)],
                [sds((16, 80, 512), BF)],
            )
            mixed = lax.all_to_all(packed, W, 0, 0)
            _, low, _ = norm_bwd(pieces, stream, mid, table, (0, 0))
            near = gather_near(low)
            fc1_grad, fc2_grad = call(
                finish_ffn_body, "finish_ffn",
                [(ffn_pieces, (16, 64, D), None), (owned1, (64, D), (0, 0))],
                [sds((2, 64, 512), F32), sds((2, 64, 512), F32)],
            )
            near, fc1_grad, fc2_grad = tie(near, fc1_grad, fc2_grad)
            far = core_swap(near)
            (input_grad,) = call(
                sequence_body, "to_sequence",
                [(order, None, None), (near, half, None), (far, half, None)],
                [sds((ROWS, D), F32)],
            )
    odd = ctx.astype(jnp.int32).reshape(1)
    small = (12, 64)
    (tail,) = call(
        finish_columns_body, "finish_columns",
        [(odd, None, None), (mixed, (16, 80, 512), None)],
        [sds(small, F32)],
    )
    tail = tail + core_swap(tail)
    tails = [tail] + [along_y(tail, step) for step in (1, 2, 3)]
    qkv_grad, proj_grad, qv_grad, up_grad = call(
        finish_body, "finish",
        [(mixed, (16, 80, 512), None), (owned1, (64, 512), (0, 2))],
        [sds((2, 64, 384), F32), sds((2, 64, 128), F32), sds((2, 256), F32), sds((2, 512), F32)],
    )
    tails, input_grad, qkv_grad = tie(tails, input_grad, qkv_grad)
    gains_grad, biases_grad = call(
        finish_rows_body, "finish_rows",
        [(v, small, None) for v in tails],
        [sds((2, 2, 64), F32), sds((2, 4, 64), F32)],
    )
    return (
        block_out[None], input_grad[None], qkv_grad, proj_grad, fc1_grad, fc2_grad,
        qv_grad, up_grad, gains_grad, biases_grad,
    )


def solution(mesh):
    return jax.shard_map(
        per_device,
        mesh=mesh,
        in_specs=(
            P("shard", "context", None),
            P(None, W, T),
            P(None, W, T),
            P(None, W, T),
            P(None, W, T),
            P(None, T),
            P(None, T),
            P(None, None, W),
            P(None, None, W),
            P("shard", "context", None),
        ),
        out_specs=(
            P("shard", "context", None),
            P("shard", "context", None),
            P(None, W, T),
            P(None, W, T),
            P(None, W, T),
            P(None, W, T),
            P(None, T),
            P(None, T),
            P(None, None, W),
            P(None, None, W),
        ),
        check_vma=False,
    )
```
